32 devices in a mesh: dp: 4 (over x, y), tp: 8 (over z, core).
Axes of the slice: x: 2, y: 2, z: 4, core: 2. Of those that a mesh axis runs over, the one named last changes fastest.
Arguments:
- hidden: bfloat16 [2048, 2048], P(('dp', 'tp')), parts along dimension 0
- cache_lat: bfloat16 [2048, 512, 512], P(('dp', 'tp')), parts along dimension 0
- cache_rope: bfloat16 [2048, 512, 64], P(('dp', 'tp')), parts along dimension 0
- seq_lens: int32 [2048], P(('dp', 'tp')), parts along dimension 0
- attn_norm: bfloat16 [2048], replicated
- w_query: bfloat16 [2048, 3072], replicated
- w_kv_down: bfloat16 [2048, 576], replicated
- kv_norm: bfloat16 [512], replicated
- w_key_up: bfloat16 [512, 2048], replicated
- w_val_up: bfloat16 [512, 2048], replicated
- w_out: bfloat16 [2048, 2048], replicated
- mlp_norm: bfloat16 [2048], replicated
- w_gate: bfloat16 [2048, 10944], P(None, 'tp')
- w_up: bfloat16 [2048, 10944], P(None, 'tp')
- w_down: bfloat16 [10944, 2048], P('tp')
Outputs:
- output 1: bfloat16 [2048, 2048], P(('dp', 'tp')), parts along dimension 0
- output 2: bfloat16 [2048, 512], P(('dp', 'tp')), parts along dimension 0
- output 3: bfloat16 [2048, 64], P(('dp', 'tp')), parts along dimension 0
There are 4 independent parts. The reference program is written for one: setup_inputs(seed, part) draws one part's arguments, and reference() takes and returns one part's arrays. A program takes and returns all parts, laid end to end along the dimension named above; an argument that names none is the same for every part.
All inputs are finite; a program needn't handle non-finite values.
Results may differ from the reference program's by a relative error of at most 0.0106894.
Values are sent between devices in bfloat16 or wider.
A program may use at most 1 GiB of HBM per device.

```python
import jax
import jax.numpy as jnp
from jax import lax

HIDDEN = 2048
NUM_HEADS = 16
FFN_DIM = 10944
CACHE_LEN = 512
BATCH = 512
KV_LORA = 512
ROPE_DIM = 64
NOPE_DIM = 128
VAL_DIM = 128
EPS = 1e-6
ROPE_BASE = 10000.0
SCALE = (NOPE_DIM + ROPE_DIM) ** -0.5


def setup_inputs(seed: int = 0, part: int = 0) -> dict:
    part_key = jax.random.fold_in(jax.random.key(seed), part)
    part_keys = jax.random.split(part_key, 7)
    shared_keys = jax.random.split(jax.random.key(seed + 1), 11)
    hidden = jax.random.normal(part_keys[0], (BATCH, HIDDEN), jnp.float32).astype(jnp.bfloat16)
    seq_lens = jax.random.randint(part_keys[1], (BATCH,), 0, CACHE_LEN, jnp.int32)
    seq_lens = seq_lens.at[0].set(CACHE_LEN - 1).at[1].set(0)
    slot_scale = jnp.where(jnp.arange(CACHE_LEN)[None, :] < seq_lens[:, None], 1.0, 2.0)[:, :, None]
    slot_gain = jax.random.normal(part_keys[2], (BATCH, CACHE_LEN, 1), jnp.float32)
    lat_dir = jax.random.normal(part_keys[3], (BATCH, 1, KV_LORA), jnp.float32)
    rope_dir = jax.random.normal(part_keys[4], (BATCH, 1, ROPE_DIM), jnp.float32)
    lat_noise = 0.5 * jax.random.normal(part_keys[5], (BATCH, CACHE_LEN, KV_LORA), jnp.float32)
    rope_noise = 0.5 * jax.random.normal(part_keys[6], (BATCH, CACHE_LEN, ROPE_DIM), jnp.float32)
    cache_lat = (slot_scale * (slot_gain * lat_dir + lat_noise)).astype(jnp.bfloat16)
    cache_rope = (slot_scale * (slot_gain * rope_dir + rope_noise)).astype(jnp.bfloat16)

    def norm_gain(rand_key, width):
        return (1.0 + 0.3 * jax.random.normal(rand_key, (width,), jnp.float32)).astype(jnp.bfloat16)

    def weight(rand_key, dims, fan_in):
        return (jax.random.normal(rand_key, dims, jnp.float32) * fan_in ** -0.5).astype(jnp.bfloat16)

    return {
        'hidden': hidden,
        'cache_lat': cache_lat,
        'cache_rope': cache_rope,
        'seq_lens': seq_lens,
        'attn_norm': norm_gain(shared_keys[0], HIDDEN),
        'w_query': weight(shared_keys[1], (HIDDEN, NUM_HEADS * (NOPE_DIM + ROPE_DIM)), HIDDEN),
        'w_kv_down': weight(shared_keys[2], (HIDDEN, KV_LORA + ROPE_DIM), HIDDEN),
        'kv_norm': norm_gain(shared_keys[3], KV_LORA),
        'w_key_up': weight(shared_keys[4], (KV_LORA, NUM_HEADS * NOPE_DIM), NOPE_DIM),
        'w_val_up': weight(shared_keys[5], (KV_LORA, NUM_HEADS * VAL_DIM), KV_LORA),
        'w_out': weight(shared_keys[6], (NUM_HEADS * VAL_DIM, HIDDEN), NUM_HEADS * VAL_DIM),
        'mlp_norm': norm_gain(shared_keys[7], HIDDEN),
        'w_gate': weight(shared_keys[8], (HIDDEN, FFN_DIM), HIDDEN),
        'w_up': weight(shared_keys[9], (HIDDEN, FFN_DIM), HIDDEN),
        'w_down': weight(shared_keys[10], (FFN_DIM, HIDDEN), FFN_DIM),
    }


def rms_norm(vals, gain):
    vals32 = vals.astype(jnp.float32)
    inv_rms = lax.rsqrt(jnp.mean(vals32 * vals32, axis=-1, keepdims=True) + EPS)
    return (vals32 * inv_rms * gain.astype(jnp.float32)).astype(jnp.bfloat16)


def rotate(vals, cos_tab, sin_tab):
    half = vals.shape[-1] // 2
    first = vals[..., :half]
    second = vals[..., half:]
    return jnp.concatenate([first * cos_tab - second * sin_tab, second * cos_tab + first * sin_tab], axis=-1)


def rope_tables(seq_lens):
    inv_freq = ROPE_BASE ** (-jnp.arange(0, ROPE_DIM, 2, dtype=jnp.float32) / ROPE_DIM)
    angles = seq_lens.astype(jnp.float32)[:, None] * inv_freq[None, :]
    return jnp.cos(angles), jnp.sin(angles)


def attend_one(packed):
    q_lat, q_rot, lat_rows, rope_rows, length, lat_new, rope_new = packed
    scores = (jnp.dot(q_lat, lat_rows.T, preferred_element_type=jnp.float32) + jnp.dot(q_rot, rope_rows.T, preferred_element_type=jnp.float32)) * SCALE
    score_new = (jnp.dot(q_lat, lat_new, preferred_element_type=jnp.float32) + jnp.dot(q_rot, rope_new, preferred_element_type=jnp.float32)) * SCALE
    valid = jnp.arange(CACHE_LEN) < length
    scores = jnp.where(valid[None, :], scores, -jnp.inf)
    top = jnp.maximum(jnp.max(scores, axis=-1), score_new)
    expo = jnp.exp(scores - top[:, None])
    expo_new = jnp.exp(score_new - top)
    denom = jnp.sum(expo, axis=-1) + expo_new
    probs = (expo / denom[:, None]).astype(jnp.bfloat16)
    prob_new = (expo_new / denom).astype(jnp.bfloat16)
    lat_sum = jnp.dot(probs, lat_rows, preferred_element_type=jnp.float32) + prob_new.astype(jnp.float32)[:, None] * lat_new.astype(jnp.float32)[None, :]
    return lat_sum.astype(jnp.bfloat16)


def reference(hidden, cache_lat, cache_rope, seq_lens, attn_norm, w_query, w_kv_down, kv_norm, w_key_up, w_val_up, w_out, mlp_norm, w_gate, w_up, w_down):
    normed = rms_norm(hidden, attn_norm)
    query = jnp.dot(normed, w_query, preferred_element_type=jnp.float32).astype(jnp.bfloat16).reshape(BATCH, NUM_HEADS, NOPE_DIM + ROPE_DIM)
    kv_proj = jnp.dot(normed, w_kv_down, preferred_element_type=jnp.float32).astype(jnp.bfloat16)
    lat_new = rms_norm(kv_proj[:, :KV_LORA], kv_norm)
    cos_tab, sin_tab = rope_tables(seq_lens)
    rope_new = rotate(kv_proj[:, KV_LORA:].astype(jnp.float32), cos_tab, sin_tab).astype(jnp.bfloat16)
    q_rot = rotate(query[:, :, NOPE_DIM:].astype(jnp.float32), cos_tab[:, None, :], sin_tab[:, None, :]).astype(jnp.bfloat16)
    key_up = w_key_up.reshape(KV_LORA, NUM_HEADS, NOPE_DIM).astype(jnp.float32)
    q_lat = jnp.einsum('bhn,khn->bhk', query[:, :, :NOPE_DIM].astype(jnp.float32), key_up).astype(jnp.bfloat16)
    lat_out = lax.map(attend_one, (q_lat, q_rot, cache_lat, cache_rope, seq_lens, lat_new, rope_new))
    val_up = w_val_up.reshape(KV_LORA, NUM_HEADS, VAL_DIM).astype(jnp.float32)
    head_out = jnp.einsum('bhk,khv->bhv', lat_out.astype(jnp.float32), val_up).astype(jnp.bfloat16).reshape(BATCH, NUM_HEADS * VAL_DIM)
    attn_out = jnp.dot(head_out, w_out, preferred_element_type=jnp.float32)
    resid = (hidden.astype(jnp.float32) + attn_out).astype(jnp.bfloat16)
    mlp_in = rms_norm(resid, mlp_norm)
    gate_proj = jnp.dot(mlp_in, w_gate, preferred_element_type=jnp.float32)
    up_proj = jnp.dot(mlp_in, w_up, preferred_element_type=jnp.float32)
    act = (jax.nn.silu(gate_proj) * up_proj).astype(jnp.bfloat16)
    mlp_out = jnp.dot(act, w_down, preferred_element_type=jnp.float32)
    out_hidden = (resid.astype(jnp.float32) + mlp_out).astype(jnp.bfloat16)
    return (out_hidden, lat_new, rope_new)
```

```python
import jax
import jax.numpy as jnp
from jax import lax
from jax.experimental import pallas as pl
from jax.experimental.pallas import tpu as pltpu
from jax.sharding import PartitionSpec as P

EPS = 1e-6
ROPE_BASE = 10000.0
value_a7 = 512
ROPE_DIM = 64
NOPE_DIM = 128
SCALE = (NOPE_DIM + ROPE_DIM) ** -0.5


def rms_norm(vals, gain):
    vals32 = vals.astype(jnp.float32)
    inv_rms = lax.rsqrt(jnp.mean(vals32 * vals32, axis=-1, keepdims=True) + EPS)
    return (vals32 * inv_rms * gain.astype(jnp.float32)).astype(jnp.bfloat16)


def rotate(vals, cos_tab, sin_tab):
    half = vals.shape[-1] // 2
    first = vals[..., :half]
    second = vals[..., half:]
    return jnp.concatenate([first * cos_tab - second * sin_tab, second * cos_tab + first * sin_tab], axis=-1)


def rope_tables(seq_lens):
    inv_freq = ROPE_BASE ** (-jnp.arange(0, ROPE_DIM, 2, dtype=jnp.float32) / ROPE_DIM)
    angles = seq_lens.astype(jnp.float32)[:, None] * inv_freq[None, :]
    return jnp.cos(angles), jnp.sin(angles)


def attention_block(hidden, cache_lat, cache_rope, seq_lens, attn_norm, w_query, w_kv_down, kv_norm, w_key_up, w_val_up, w_out):
    rows = hidden.shape[0]
    heads = w_key_up.shape[1] // NOPE_DIM
    normed = rms_norm(hidden, attn_norm)
    query = jnp.dot(normed, w_query, preferred_element_type=jnp.float32).astype(jnp.bfloat16).reshape(rows, heads, NOPE_DIM + ROPE_DIM)
    kv_proj = jnp.dot(normed, w_kv_down, preferred_element_type=jnp.float32).astype(jnp.bfloat16)
    lat_new = rms_norm(kv_proj[:, :value_a7], kv_norm)
    cos_tab, sin_tab = rope_tables(seq_lens)
    rope_new = rotate(kv_proj[:, value_a7:].astype(jnp.float32), cos_tab, sin_tab).astype(jnp.bfloat16)
    q_rot = rotate(query[:, :, NOPE_DIM:].astype(jnp.float32), cos_tab[:, None, :], sin_tab[:, None, :]).astype(jnp.bfloat16)
    key_up = w_key_up.reshape(value_a7, heads, NOPE_DIM)
    q_lat = jnp.einsum('bhn,khn->bhk', query[:, :, :NOPE_DIM], key_up, preferred_element_type=jnp.float32).astype(jnp.bfloat16)
    scores = (jnp.einsum('bhk,bsk->bhs', q_lat, cache_lat, preferred_element_type=jnp.float32) + jnp.einsum('bhr,bsr->bhs', q_rot, cache_rope, preferred_element_type=jnp.float32)) * SCALE
    score_new = (jnp.einsum('bhk,bk->bh', q_lat, lat_new, preferred_element_type=jnp.float32) + jnp.einsum('bhr,br->bh', q_rot, rope_new, preferred_element_type=jnp.float32)) * SCALE
    slots = cache_lat.shape[1]
    valid = jnp.arange(slots)[None, None, :] < seq_lens[:, None, None]
    scores = jnp.where(valid, scores, -jnp.inf)
    top = jnp.maximum(jnp.max(scores, axis=-1), score_new)
    expo = jnp.exp(scores - top[..., None])
    expo_new = jnp.exp(score_new - top)
    denom = jnp.sum(expo, axis=-1) + expo_new
    probs = (expo / denom[..., None]).astype(jnp.bfloat16)
    prob_new = (expo_new / denom).astype(jnp.bfloat16)
    lat_sum = jnp.einsum('bhs,bsk->bhk', probs, cache_lat, preferred_element_type=jnp.float32) + prob_new.astype(jnp.float32)[..., None] * lat_new.astype(jnp.float32)[:, None, :]
    lat_out = lat_sum.astype(jnp.bfloat16)
    val_up = w_val_up.reshape(value_a7, heads, -1)
    head_out = jnp.einsum('bhk,khv->bhv', lat_out, val_up, preferred_element_type=jnp.float32).astype(jnp.bfloat16).reshape(rows, -1)
    attn_out = jnp.dot(head_out, w_out, preferred_element_type=jnp.float32)
    resid = (hidden.astype(jnp.float32) + attn_out).astype(jnp.bfloat16)
    return resid, lat_new, rope_new


MESH = pl.DeviceIdType.MESH
NSUB = 2
NRS = 4
STRIP = 256


def mlp_kernel(g_ref, resid_ref, wg_hbm, wu_hbm, wd_hbm, out_ref,
               g_all, wg, wu, wd, act, pown, psend, precv, rsend, rrecv_e, rrecv_m,
               w_sem, ag_recv, ag_recv_d, ag_send_e, ag_send_m, ag_send_d,
               rd_recv, rd_send, rs_recv_e, rs_recv_m, rs_send):
    ffn = wg.shape[0]
    rows, width = g_ref.shape
    sub = rows // NSUB
    rsub = rows // NRS
    me = lax.axis_index('tp')
    z = lax.div(me, 2)
    c = lax.rem(me, 2)
    upper = z >= 2
    is_end = jnp.logical_or(z == 0, z == 3)
    is_int = jnp.logical_not(is_end)

    def mir(k):
        return jnp.where(upper, k, 3 - k)

    partner = 2 * z + (1 - c)
    dev_e = jnp.where(is_end, me, 2 * mir(3) + c)
    dev_m = 2 * jnp.where(is_end, mir(2), mir(1)) + c

    w_copies = []
    for idx, (src, dst) in enumerate(((wg_hbm, wg), (wu_hbm, wu), (wd_hbm, wd))):
        copy = pltpu.make_async_copy(src, dst, w_sem.at[idx])
        copy.start()
        w_copies.append(copy)

    barrier = pltpu.get_barrier_semaphore()
    pl.semaphore_signal(barrier, inc=1, device_id={'tp': partner}, device_id_type=MESH)
    pl.semaphore_signal(barrier, inc=1, device_id={'tp': dev_m}, device_id_type=MESH)

    @pl.when(is_int)
    def _():
        pl.semaphore_signal(barrier, inc=1, device_id={'tp': dev_e}, device_id_type=MESH)
        pl.semaphore_wait(barrier, 3)

    @pl.when(is_end)
    def _():
        pl.semaphore_wait(barrier, 2)

    def remote(src, dst, send_sem, recv_sem, dev):
        return pltpu.make_async_remote_copy(src_ref=src, dst_ref=dst, send_sem=send_sem, recv_sem=recv_sem, device_id={'tp': dev}, device_id_type=MESH)

    def ag_copy(src, chip, k, send_sem, dev):
        return remote(src, g_all.at[chip, 0, pl.ds(k * sub, sub)], send_sem.at[chip, k], ag_recv.at[chip, k], dev)

    def ag_d2d(src, chip, k):
        return remote(src, g_all.at[chip, 1, pl.ds(k * sub, sub)], ag_send_d.at[chip, k], ag_recv_d.at[chip, k], partner)

    for k in range(NSUB):
        piece = g_ref.at[pl.ds(k * sub, sub)]
        ag_copy(piece, z, k, ag_send_m, dev_m).start()

        @pl.when(is_int)
        def _():
            ag_copy(piece, z, k, ag_send_e, dev_e).start()

        ag_d2d(piece, z, k).start()
    g_all[z, 0] = g_ref[...]

    def landed(chip, k):
        return g_all.at[chip, 0, pl.ds(k * sub, sub)]

    def arrive(chip, k, send_sem, dev):
        src = landed(chip, k)
        ag_copy(src, chip, k, ag_send_d, dev_m).wait_recv()
        if dev is not None:
            ag_copy(src, chip, k, send_sem, dev).start()
        ag_d2d(src, chip, k).start()

    def both(chip):
        for k in range(NSUB):
            ag_d2d(landed(chip, k), chip, k).wait_recv()

    def rd_copy(chip):
        return remote(psend.at[chip], precv.at[chip], rd_send.at[chip], rd_recv.at[chip], partner)

    def rs_copy(chip, k, dst, recv_sem, dev):
        span = pl.ds(k * rsub, rsub)
        return remote(rsend.at[chip, span], dst.at[chip, span], rs_send.at[chip, k], recv_sem.at[chip, k], dev)

    def rs_base(chip, k):
        span = pl.ds(k * rsub, rsub)
        return pown[chip, span] + precv[chip, span].astype(jnp.float32)

    def end_send(chip):
        rd_copy(chip).wait_recv()
        for k in range(NRS):
            rsend[chip, pl.ds(k * rsub, rsub)] = rs_base(chip, k).astype(jnp.bfloat16)
            rs_copy(chip, k, rrecv_e, rs_recv_e, dev_m).start()

    def hook(step, strip):
        def at(role, want_step, want_strip, fn):
            pl.when(jnp.logical_and(role, jnp.logical_and(step == want_step, strip == want_strip)))(fn)

        def int_a():
            arrive(mir(3), 1, ag_send_m, dev_m)
            arrive(mir(1), 1, ag_send_e, dev_e)

        at(is_int, 0, 2, int_a)
        at(is_int, 1, 2, lambda: arrive(mir(0), 0, ag_send_e, dev_e))
        at(is_int, 2, 1, lambda: arrive(mir(0), 1, ag_send_e, dev_e))
        at(is_end, 0, 2, lambda: arrive(mir(2), 0, None, None))
        at(is_end, 1, 2, lambda: arrive(mir(1), 0, None, None))
        at(is_end, 2, 0, lambda: end_send(mir(2)))
        at(is_end, 2, 2, lambda: arrive(mir(0), 0, None, None))
        at(is_end, 3, 0, lambda: end_send(mir(1)))

    def swiglu(lhs, at, count):
        gate = lax.dot_general(lhs, wg[pl.ds(at, count)], (((1,), (1,)), ((), ())), preferred_element_type=jnp.float32)
        up = lax.dot_general(lhs, wu[pl.ds(at, count)], (((1,), (1,)), ((), ())), preferred_element_type=jnp.float32)
        return (gate / (1.0 + jnp.exp(-gate)) * up).astype(jnp.bfloat16)

    whole = ffn // STRIP
    rest = ffn - whole * STRIP

    def one_step(step, carry):
        third = jnp.where(is_end, mir(1), mir(1))
        chip = jnp.where(step == 0, z, jnp.where(step == 1, jnp.where(is_end, mir(2), mir(3)), jnp.where(step == 2, third, mir(0))))

        @pl.when(jnp.logical_and(step == 0, is_int))
        def _():
            arrive(mir(3), 0, ag_send_m, dev_m)
            arrive(mir(1), 0, ag_send_e, dev_e)

        @pl.when(jnp.logical_and(step == 2, is_end))
        def _():
            arrive(mir(1), 1, None, None)

        @pl.when(jnp.logical_and(step == 3, is_end))
        def _():
            arrive(mir(0), 1, None, None)

        both(chip)

        @pl.when(step == 0)
        def _():
            w_copies[0].wait()
            w_copies[1].wait()

        def one_strip(strip, carry):
            at = pl.multiple_of(strip * STRIP, STRIP)
            act[:, pl.ds(at, STRIP)] = swiglu(g_all[chip].reshape(2 * rows, width), at, STRIP)
            hook(step, strip)
            return carry

        lax.fori_loop(0, whole, one_strip, 0)
        act[:, whole * STRIP:] = swiglu(g_all[chip].reshape(2 * rows, width), whole * STRIP, rest)

        @pl.when(jnp.logical_and(step == 0, is_end))
        def _():
            arrive(mir(2), 1, None, None)

        @pl.when(step == 0)
        def _():
            w_copies[2].wait()

        def one_col(col, carry):
            span = pl.ds(pl.multiple_of(col * STRIP, STRIP), STRIP)
            part = jnp.dot(act[...], wd[:, span], preferred_element_type=jnp.float32)
            pown[chip, :, span] = part[:rows]
            psend[chip, :, span] = part[rows:].astype(jnp.bfloat16)
            return carry

        lax.fori_loop(0, width // STRIP, one_col, 0)
        rd_copy(chip).start()
        return carry

    lax.fori_loop(0, 4, one_step, 0)

    @pl.when(is_end)
    def _():
        end_send(mir(0))
        rd_copy(z).wait_recv()
        base = pown[z] + precv[z].astype(jnp.float32) + resid_ref[...].astype(jnp.float32)
        pown[z] = base
        for k in range(NRS):
            span = pl.ds(k * rsub, rsub)
            rs_copy(z, k, rrecv_m, rs_recv_m, dev_m).wait_recv()
            out_ref[span] = (pown[z, span] + rrecv_m[z, span].astype(jnp.float32)).astype(jnp.bfloat16)

    @pl.when(is_int)
    def _():
        def pass_on(chip, dst_in, sem_in, dst_out, sem_out, dev):
            rd_copy(chip).wait_recv()
            for k in range(NRS):
                span = pl.ds(k * rsub, rsub)
                rs_copy(chip, k, dst_in, sem_in, dev_m).wait_recv()
                rsend[chip, span] = (rs_base(chip, k) + dst_in[chip, span].astype(jnp.float32)).astype(jnp.bfloat16)
                rs_copy(chip, k, dst_out, sem_out, dev).start()

        def own_send(chip):
            pass_on(chip, rrecv_e, rs_recv_e, rrecv_m, rs_recv_m, dev_m)

        own_send(mir(1))
        rd_copy(z).wait_recv()
        for k in range(NRS):
            rs_copy(z, k, rrecv_e, rs_recv_e, dev_m).wait_recv()
        pown[z] = pown[z] + precv[z].astype(jnp.float32) + resid_ref[...].astype(jnp.float32) + rrecv_e[z].astype(jnp.float32)
        own_send(mir(0))
        for k in range(NRS):
            span = pl.ds(k * rsub, rsub)
            rs_copy(z, k, rrecv_m, rs_recv_m, dev_m).wait_recv()
            out_ref[span] = (pown[z, span] + rrecv_m[z, span].astype(jnp.float32)).astype(jnp.bfloat16)
        pass_on(mir(3), rrecv_m, rs_recv_m, rrecv_m, rs_recv_m, dev_e)

    for k in range(NSUB):
        for chip in range(4):
            ag_d2d(landed(chip, k), chip, k).wait_send()
        ag_copy(landed(z, k), z, k, ag_send_m, dev_m).wait_send()

        @pl.when(is_int)
        def _():
            ag_copy(landed(z, k), z, k, ag_send_e, dev_e).wait_send()
            ag_copy(landed(mir(3), k), mir(3), k, ag_send_m, dev_m).wait_send()
            ag_copy(landed(mir(1), k), mir(1), k, ag_send_e, dev_e).wait_send()
            ag_copy(landed(mir(0), k), mir(0), k, ag_send_e, dev_e).wait_send()

    for chip in range(4):
        rd_copy(chip).wait_send()

        @pl.when(chip != z)
        def _():
            for k in range(NRS):
                rs_copy(chip, k, rrecv_m, rs_recv_m, dev_m).wait_send()


def mlp_block(mlp_in, resid, w_gate_t, w_up_t, w_down):
    rows, width = mlp_in.shape
    ffn = w_gate_t.shape[0]
    bf16, f32 = jnp.bfloat16, jnp.float32
    vmem = pl.BlockSpec(memory_space=pltpu.VMEM)
    hbm = pl.BlockSpec(memory_space=pl.ANY)
    dma = pltpu.SemaphoreType.DMA
    flops = 3 * 2 * 8 * rows * width * ffn
    return pl.pallas_call(
        mlp_kernel,
        out_shape=jax.ShapeDtypeStruct((rows, width), bf16),
        in_specs=[vmem, vmem, hbm, hbm, hbm],
        out_specs=vmem,
        scratch_shapes=[
            pltpu.VMEM((4, 2, rows, width), bf16),
            pltpu.VMEM((ffn, width), bf16),
            pltpu.VMEM((ffn, width), bf16),
            pltpu.VMEM((ffn, width), bf16),
            pltpu.VMEM((2 * rows, ffn), bf16),
            pltpu.VMEM((4, rows, width), f32),
            pltpu.VMEM((4, rows, width), bf16),
            pltpu.VMEM((4, rows, width), bf16),
            pltpu.VMEM((4, rows, width), bf16),
            pltpu.VMEM((4, rows, width), bf16),
            pltpu.VMEM((4, rows, width), bf16),
            dma((3,)),
            dma((4, NSUB)), dma((4, NSUB)), dma((4, NSUB)), dma((4, NSUB)), dma((4, NSUB)),
            dma((4,)), dma((4,)),
            dma((4, NRS)), dma((4, NRS)), dma((4, NRS)),
        ],
        compiler_params=pltpu.CompilerParams(collective_id=0, has_side_effects=True, vmem_limit_bytes=60 * 1024 * 1024),
        cost_estimate=pl.CostEstimate(flops=flops, bytes_accessed=3 * 2 * ffn * width, transcendentals=8 * rows * ffn),
        name='mlp_exchange',
    )(mlp_in, resid, w_gate_t, w_up_t, w_down)


def solution(mesh):
    rows_spec = P(('dp', 'tp'), None)
    cache_spec = P(('dp', 'tp'), None, None)
    whole = P()
    in_specs = (rows_spec, cache_spec, cache_spec, P(('dp', 'tp')), whole, whole, whole, whole, whole, whole, whole, whole, P(None, 'tp'), P(None, 'tp'), P('tp', None))
    out_specs = (rows_spec, rows_spec, rows_spec)

    def device_step(hidden, cache_lat, cache_rope, seq_lens, attn_norm, w_query, w_kv_down, kv_norm, w_key_up, w_val_up, w_out, mlp_norm, w_gate, w_up, w_down):
        resid, lat_new, rope_new = attention_block(hidden, cache_lat, cache_rope, seq_lens, attn_norm, w_query, w_kv_down, kv_norm, w_key_up, w_val_up, w_out)
        mlp_in = rms_norm(resid, mlp_norm)
        out_hidden = mlp_block(mlp_in, resid, w_gate.T, w_up.T, w_down)
        return out_hidden, lat_new, rope_new

    return jax.shard_map(device_step, mesh=mesh, in_specs=in_specs, out_specs=out_specs, check_vma=False)
```

```python
import math

import jax
import jax.numpy as jnp
from jax import lax
from jax.experimental import pallas as pl
from jax.experimental.pallas import tpu as pltpu
from jax.sharding import PartitionSpec as P

EPS = 1e-6
ROPE_BASE = 10000.0
ROPE_DIM = 64
NOPE_DIM = 128
VAL_DIM = 128
SCALE = (NOPE_DIM + ROPE_DIM) ** -0.5


GROUP = 4
SLOTS = 7
BLOCK = 128
Q_CHUNKS = 4
VMEM_LIMIT = 63 * 1024 * 1024


def attn_kernel(lens_ref, hidden_ref, lens_col, attn_gain, kv_gain, mlp_gain, lat_hbm, rope_hbm, wq_hbm, wkv_hbm, wk_hbm, wv_hbm, wo_hbm,
                resid_ref, mlp_in_ref, lat_new_ref, rope_new_ref,
                keys, rope, wq, wkv, wk, wv, wo, normed, qs, qr, lat_row, rope_row, heads_out, order, key_sem, w_sem):
    f32, bf16 = jnp.float32, jnp.bfloat16
    rows, width = hidden_ref.shape
    rank = wk.shape[0]
    heads = wk.shape[1] // NOPE_DIM
    groups = rows // GROUP
    classes = keys.shape[2] // BLOCK

    chunk = wq.shape[2]
    w_copies = [pltpu.make_async_copy(wkv_hbm, wkv, w_sem.at[0]), pltpu.make_async_copy(wk_hbm, wk, w_sem.at[1])]
    w_copies += [pltpu.make_async_copy(wq_hbm.at[:, pl.ds(j * chunk, chunk)], wq.at[j], w_sem.at[2 + j]) for j in range(Q_CHUNKS)]
    rope_copy = pltpu.make_async_copy(rope_hbm, rope, w_sem.at[2 + Q_CHUNKS])
    late_copies = [pltpu.make_async_copy(wv_hbm, wv, w_sem.at[3 + Q_CHUNKS]), pltpu.make_async_copy(wo_hbm, wo, w_sem.at[4 + Q_CHUNKS])]
    for copy in w_copies:
        copy.start()
    rope_copy.start()

    def kind(b):
        return lax.div(lens_ref[b], BLOCK)

    def count(b, counts):
        k = kind(b)
        return tuple(n + jnp.where(k == i, 1, 0) for i, n in enumerate(counts))

    zero = jnp.int32(0)
    counts = lax.fori_loop(0, rows, count, (zero,) * classes)
    firsts = []
    total = zero
    for i in reversed(range(classes)):
        firsts.append(total)
        total = total + counts[i]
    firsts = tuple(reversed(firsts))

    def place(b, firsts):
        k = kind(b)
        at = firsts[0]
        for i in range(1, classes):
            at = jnp.where(k == i, firsts[i], at)
        order[at] = b
        return tuple(n + jnp.where(k == i, 1, 0) for i, n in enumerate(firsts))

    lax.fori_loop(0, rows, place, firsts)

    def group_copies(g, blocks):
        slot = lax.rem(g, SLOTS)
        return [pltpu.make_async_copy(lat_hbm.at[order[g * GROUP + i], pl.ds(0, blocks * BLOCK)], keys.at[slot, i, pl.ds(0, blocks * BLOCK)], key_sem.at[slot, i]) for i in range(GROUP)]

    def per_class(g, fn):
        k = kind(order[g * GROUP])
        for i in range(classes):
            @pl.when(k == i)
            def _():
                fn(i + 1)

    def start_group(g):
        def start(blocks):
            for copy in group_copies(g, blocks):
                copy.start()

        per_class(g, start)

    def start_first(g, carry):
        start_group(g)
        return carry

    lax.fori_loop(0, SLOTS, start_first, 0)

    vals = hidden_ref[...].astype(f32)
    inv_rms = lax.rsqrt(jnp.mean(vals * vals, axis=-1, keepdims=True) + EPS)
    normed[...] = (vals * inv_rms * attn_gain[...].astype(f32)).astype(bf16)

    lane = lax.broadcasted_iota(jnp.int32, (rows, 2 * ROPE_DIM), 1)
    half = ROPE_DIM // 2
    freq = jnp.exp(lax.rem(lane, half).astype(f32) * (-math.log(ROPE_BASE) / half))
    angles = lens_col[...].astype(f32) * freq
    cos_tab = jnp.cos(angles)
    is_first = lax.rem(lane, ROPE_DIM) < half
    sin_tab = jnp.where(is_first, -jnp.sin(angles), jnp.sin(angles))

    def rotate_pair(pair):
        swapped = jnp.where(is_first, pltpu.roll(pair, 2 * ROPE_DIM - half, 1), pltpu.roll(pair, half, 1))
        return (pair * cos_tab + swapped * sin_tab).astype(bf16).astype(f32)

    w_copies[0].wait()
    kv = lax.dot_general(normed[...], wkv[...], (((1,), (1,)), ((), ())), preferred_element_type=f32).astype(bf16).astype(f32)
    lat = kv[:, :rank]
    inv_lat = lax.rsqrt(jnp.mean(lat * lat, axis=-1, keepdims=True) + EPS)
    lat_new = (lat * inv_lat * kv_gain[...].astype(f32)).astype(bf16)
    lat_new_ref[...] = lat_new
    lat_row[...] = lat_new.astype(f32)
    pe = kv[:, rank:]
    rope_new = rotate_pair(jnp.concatenate([pe, pe], axis=1))
    rope_new_ref[...] = rope_new[:, :ROPE_DIM].astype(bf16)
    rope_row[...] = rope_new

    w_copies[1].wait()
    low = lane < ROPE_DIM

    def put_head(head, nope, pe_rot):
        key_up = wk[:, head * NOPE_DIM:(head + 1) * NOPE_DIM]
        q_lat = lax.dot_general(nope.astype(bf16), key_up, (((1,), (1,)), ((), ())), preferred_element_type=f32).astype(bf16).astype(f32)
        for part in range(rank // 128):
            qs[part, pl.ds(head, rows, stride=heads), :] = q_lat[:, part * 128:(part + 1) * 128]
        qr[pl.ds(head, rows, stride=heads), :] = pe_rot

    for j in range(Q_CHUNKS):
        w_copies[2 + j].wait()
        query = jnp.dot(normed[...], wq[j], preferred_element_type=f32).astype(bf16).astype(f32)
        for pair in range(chunk // 384):
            base = pair * 384
            part_a, part_b, part_c = (query[:, base + 128 * i:base + 128 * (i + 1)] for i in range(3))
            pe_rot = rotate_pair(jnp.where(low, part_b, part_c))
            head = (j * chunk + base) // 192
            put_head(head, part_a, pe_rot)
            put_head(head + 1, jnp.where(low, pltpu.roll(part_b, ROPE_DIM, 1), pltpu.roll(part_c, ROPE_DIM, 1)), pltpu.roll(pe_rot, ROPE_DIM, 1))

    rope_copy.wait()

    def attend(g, blocks):
        slot = lax.rem(g, SLOTS)
        span = blocks * BLOCK
        for copy in group_copies(g, blocks):
            copy.wait()
        scores = []
        picks = [order[g * GROUP + i] for i in range(GROUP)]
        for i, b in enumerate(picks):
            length = lens_ref[b]
            base = pl.multiple_of(lax.div(length, 16) * 16, 16)
            tile = keys[slot, i, pl.ds(base, 16), :].astype(f32)
            sub = lax.broadcasted_iota(jnp.int32, (16, rank), 0)
            keys[slot, i, pl.ds(base, 16), :] = jnp.where(sub == length - base, lat_row[pl.ds(b, 1), :], tile).astype(bf16)
        for i, b in enumerate(picks):
            length = lens_ref[b]
            mine = pl.ds(pl.multiple_of(b * heads, heads), heads)
            q_lat = jnp.concatenate([qs[part, mine, :] for part in range(rank // 128)], axis=1).astype(bf16)
            q_rot = qr[mine, :]
            score = lax.dot_general(q_lat, keys[slot, i, :span], (((1,), (1,)), ((), ())), preferred_element_type=f32)
            near = jnp.dot(q_rot[:, :ROPE_DIM].astype(bf16), rope[b, :, :span], preferred_element_type=f32)
            first = lax.broadcasted_iota(jnp.int32, (heads, 2 * ROPE_DIM), 1) < ROPE_DIM
            new = jnp.sum(jnp.where(first, q_rot * rope_row[pl.ds(b, 1), :], 0.0), axis=1, keepdims=True)
            at = lax.broadcasted_iota(jnp.int32, (heads, span), 1)
            score = (score + jnp.where(at == length, new, near)) * SCALE
            scores.append(jnp.where(at <= length, score, -jnp.inf))
        probs = []
        for score in scores:
            expo = jnp.exp(score - jnp.max(score, axis=1, keepdims=True))
            probs.append((expo / jnp.sum(expo, axis=1, keepdims=True)).astype(bf16))
        for i, b in enumerate(picks):
            mine = pl.ds(pl.multiple_of(b * heads, heads), heads)
            out = jnp.dot(probs[i], keys[slot, i, :span], preferred_element_type=f32)
            for part in range(rank // 128):
                qs[part, mine, :] = out[:, part * 128:(part + 1) * 128]

    def one_group(g, carry):
        per_class(g, lambda blocks: attend(g, blocks))

        @pl.when(g + SLOTS < groups)
        def _():
            start_group(g + SLOTS)

        @pl.when(g == groups - SLOTS - 1)
        def _():
            for copy in late_copies:
                copy.start()

        return carry

    lax.fori_loop(0, groups, one_group, 0)

    late_copies[0].wait()
    for head in range(heads):
        cols = slice(head * VAL_DIM, (head + 1) * VAL_DIM)
        lat_out = jnp.concatenate([qs[part, pl.ds(head, rows, stride=heads), :] for part in range(rank // 128)], axis=1).astype(bf16)
        heads_out[:, cols] = jnp.dot(lat_out, wv[:, cols], preferred_element_type=f32).astype(bf16)
    late_copies[1].wait()
    square = jnp.zeros((rows, 1), f32)
    for n in range(width // 512):
        cols = slice(n * 512, (n + 1) * 512)
        attn_out = jnp.dot(heads_out[...], wo[:, cols], preferred_element_type=f32)
        resid = (hidden_ref[:, cols].astype(f32) + attn_out).astype(bf16)
        resid_ref[:, cols] = resid
        square = square + jnp.sum(resid.astype(f32) * resid.astype(f32), axis=-1, keepdims=True)
    inv_rms = lax.rsqrt(square * (1.0 / width) + EPS)
    mlp_in_ref[...] = (resid_ref[...].astype(f32) * inv_rms * mlp_gain[...].astype(f32)).astype(bf16)


def attention_block(hidden, cache_lat, cache_rope, seq_lens, attn_norm, w_query, w_kv_down, kv_norm, w_key_up, w_val_up, w_out, mlp_norm):
    rows, width = hidden.shape
    slots, rank = cache_lat.shape[1:]
    bf16, f32 = jnp.bfloat16, jnp.float32
    heads = w_key_up.shape[1] // NOPE_DIM
    q_width = w_query.shape[1]
    vmem = pl.BlockSpec(memory_space=pltpu.VMEM)
    hbm = pl.BlockSpec(memory_space=pl.ANY)
    smem = pl.BlockSpec(memory_space=pltpu.SMEM)
    dma = pltpu.SemaphoreType.DMA
    flops = 2 * rows * (width * (q_width + rank + ROPE_DIM + width) + heads * rank * (NOPE_DIM + VAL_DIM) + heads * slots * (2 * rank + ROPE_DIM))
    moved = 2 * (width * (q_width + rank + ROPE_DIM + width) + heads * rank * (NOPE_DIM + VAL_DIM) + rows * slots * (rank + ROPE_DIM))
    return pl.pallas_call(
        attn_kernel,
        out_shape=(
            jax.ShapeDtypeStruct((rows, width), bf16),
            jax.ShapeDtypeStruct((rows, width), bf16),
            jax.ShapeDtypeStruct((rows, rank), bf16),
            jax.ShapeDtypeStruct((rows, ROPE_DIM), bf16),
        ),
        in_specs=[smem] + [vmem] * 5 + [hbm] * 7,
        out_specs=(vmem,) * 4,
        scratch_shapes=[
            pltpu.VMEM((SLOTS, GROUP, slots, rank), bf16),
            pltpu.VMEM((rows, ROPE_DIM, slots), bf16),
            pltpu.VMEM((Q_CHUNKS, width, q_width // Q_CHUNKS), bf16),
            pltpu.VMEM((rank + ROPE_DIM, width), bf16),
            pltpu.VMEM((rank, heads * NOPE_DIM), bf16),
            pltpu.VMEM((rank, heads * VAL_DIM), bf16),
            pltpu.VMEM((heads * VAL_DIM, width), bf16),
            pltpu.VMEM((rows, width), bf16),
            pltpu.VMEM((rank // 128, rows * heads, 128), f32),
            pltpu.VMEM((rows * heads, 2 * ROPE_DIM), f32),
            pltpu.VMEM((rows, rank), f32),
            pltpu.VMEM((rows, 2 * ROPE_DIM), f32),
            pltpu.VMEM((rows, heads * VAL_DIM), bf16),
            pltpu.SMEM((rows,), jnp.int32),
            dma((SLOTS, GROUP)),
            dma((5 + Q_CHUNKS,)),
        ],
        compiler_params=pltpu.CompilerParams(vmem_limit_bytes=VMEM_LIMIT),
        cost_estimate=pl.CostEstimate(flops=flops, bytes_accessed=moved, transcendentals=rows * heads * slots),
        name='latent_attention',
    )(seq_lens, hidden, seq_lens[:, None], attn_norm[None], kv_norm[None], mlp_norm[None], cache_lat, jnp.swapaxes(cache_rope, 1, 2), w_query, w_kv_down.T, w_key_up, w_val_up, w_out)


MESH = pl.DeviceIdType.MESH
NSUB = 2
NRS = 4
STRIP = 256


def mlp_kernel(g_ref, resid_ref, wg_hbm, wu_hbm, wd_hbm, out_ref,
               g_all, wg, wu, wd, act, pown, psend, precv, rsend, rrecv_e, rrecv_m,
               w_sem, ag_recv, ag_recv_d, ag_send_e, ag_send_m, ag_send_d,
               rd_recv, rd_send, rs_recv_e, rs_recv_m, rs_send):
    ffn = wg.shape[0]
    rows, width = g_ref.shape
    sub = rows // NSUB
    rsub = rows // NRS
    me = lax.axis_index('tp')
    z = lax.div(me, 2)
    c = lax.rem(me, 2)
    upper = z >= 2
    is_end = jnp.logical_or(z == 0, z == 3)
    is_int = jnp.logical_not(is_end)

    def mir(k):
        return jnp.where(upper, k, 3 - k)

    partner = 2 * z + (1 - c)
    dev_e = jnp.where(is_end, me, 2 * mir(3) + c)
    dev_m = 2 * jnp.where(is_end, mir(2), mir(1)) + c

    w_copies = []
    for idx, (src, dst) in enumerate(((wg_hbm, wg), (wu_hbm, wu), (wd_hbm, wd))):
        copy = pltpu.make_async_copy(src, dst, w_sem.at[idx])
        copy.start()
        w_copies.append(copy)

    barrier = pltpu.get_barrier_semaphore()
    pl.semaphore_signal(barrier, inc=1, device_id={'tp': partner}, device_id_type=MESH)
    pl.semaphore_signal(barrier, inc=1, device_id={'tp': dev_m}, device_id_type=MESH)

    @pl.when(is_int)
    def _():
        pl.semaphore_signal(barrier, inc=1, device_id={'tp': dev_e}, device_id_type=MESH)
        pl.semaphore_wait(barrier, 3)

    @pl.when(is_end)
    def _():
        pl.semaphore_wait(barrier, 2)

    def remote(src, dst, send_sem, recv_sem, dev):
        return pltpu.make_async_remote_copy(src_ref=src, dst_ref=dst, send_sem=send_sem, recv_sem=recv_sem, device_id={'tp': dev}, device_id_type=MESH)

    def ag_copy(src, chip, k, send_sem, dev):
        return remote(src, g_all.at[chip, 0, pl.ds(k * sub, sub)], send_sem.at[chip, k], ag_recv.at[chip, k], dev)

    def ag_d2d(src, chip, k):
        return remote(src, g_all.at[chip, 1, pl.ds(k * sub, sub)], ag_send_d.at[chip, k], ag_recv_d.at[chip, k], partner)

    for k in range(NSUB):
        piece = g_ref.at[pl.ds(k * sub, sub)]
        ag_copy(piece, z, k, ag_send_m, dev_m).start()

        @pl.when(is_int)
        def _():
            ag_copy(piece, z, k, ag_send_e, dev_e).start()

        ag_d2d(piece, z, k).start()
    g_all[z, 0] = g_ref[...]

    def landed(chip, k):
        return g_all.at[chip, 0, pl.ds(k * sub, sub)]

    def arrive(chip, k, send_sem, dev):
        src = landed(chip, k)
        ag_copy(src, chip, k, ag_send_d, dev_m).wait_recv()
        if dev is not None:
            ag_copy(src, chip, k, send_sem, dev).start()
        ag_d2d(src, chip, k).start()

    def both(chip):
        for k in range(NSUB):
            ag_d2d(landed(chip, k), chip, k).wait_recv()

    def rd_copy(chip):
        return remote(psend.at[chip], precv.at[chip], rd_send.at[chip], rd_recv.at[chip], partner)

    def rs_copy(chip, k, dst, recv_sem, dev):
        span = pl.ds(k * rsub, rsub)
        return remote(rsend.at[chip, span], dst.at[chip, span], rs_send.at[chip, k], recv_sem.at[chip, k], dev)

    def rs_base(chip, k):
        span = pl.ds(k * rsub, rsub)
        return pown[chip, span] + precv[chip, span].astype(jnp.float32)

    def end_send(chip):
        rd_copy(chip).wait_recv()
        for k in range(NRS):
            rsend[chip, pl.ds(k * rsub, rsub)] = rs_base(chip, k).astype(jnp.bfloat16)
            rs_copy(chip, k, rrecv_e, rs_recv_e, dev_m).start()

    def hook(step, strip):
        def at(role, want_step, want_strip, fn):
            pl.when(jnp.logical_and(role, jnp.logical_and(step == want_step, strip == want_strip)))(fn)

        def int_a():
            arrive(mir(3), 1, ag_send_m, dev_m)
            arrive(mir(1), 1, ag_send_e, dev_e)

        at(is_int, 0, 2, int_a)
        at(is_int, 1, 2, lambda: arrive(mir(0), 0, ag_send_e, dev_e))
        at(is_int, 2, 1, lambda: arrive(mir(0), 1, ag_send_e, dev_e))
        at(is_end, 0, 2, lambda: arrive(mir(2), 0, None, None))
        at(is_end, 1, 2, lambda: arrive(mir(1), 0, None, None))
        at(is_end, 2, 0, lambda: end_send(mir(2)))
        at(is_end, 2, 2, lambda: arrive(mir(0), 0, None, None))
        at(is_end, 3, 0, lambda: end_send(mir(1)))

    def swiglu(lhs, at, count):
        gate = lax.dot_general(lhs, wg[pl.ds(at, count)], (((1,), (1,)), ((), ())), preferred_element_type=jnp.float32)
        up = lax.dot_general(lhs, wu[pl.ds(at, count)], (((1,), (1,)), ((), ())), preferred_element_type=jnp.float32)
        return (gate / (1.0 + jnp.exp(-gate)) * up).astype(jnp.bfloat16)

    whole = ffn // STRIP
    rest = ffn - whole * STRIP

    def one_step(step, carry):
        third = jnp.where(is_end, mir(1), mir(1))
        chip = jnp.where(step == 0, z, jnp.where(step == 1, jnp.where(is_end, mir(2), mir(3)), jnp.where(step == 2, third, mir(0))))

        @pl.when(jnp.logical_and(step == 0, is_int))
        def _():
            arrive(mir(3), 0, ag_send_m, dev_m)
            arrive(mir(1), 0, ag_send_e, dev_e)

        @pl.when(jnp.logical_and(step == 2, is_end))
        def _():
            arrive(mir(1), 1, None, None)

        @pl.when(jnp.logical_and(step == 3, is_end))
        def _():
            arrive(mir(0), 1, None, None)

        both(chip)

        @pl.when(step == 0)
        def _():
            w_copies[0].wait()
            w_copies[1].wait()

        def one_strip(strip, carry):
            at = pl.multiple_of(strip * STRIP, STRIP)
            act[:, pl.ds(at, STRIP)] = swiglu(g_all[chip].reshape(2 * rows, width), at, STRIP)
            hook(step, strip)
            return carry

        lax.fori_loop(0, whole, one_strip, 0)
        act[:, whole * STRIP:] = swiglu(g_all[chip].reshape(2 * rows, width), whole * STRIP, rest)

        @pl.when(jnp.logical_and(step == 0, is_end))
        def _():
            arrive(mir(2), 1, None, None)

        @pl.when(step == 0)
        def _():
            w_copies[2].wait()

        def one_col(col, carry):
            span = pl.ds(pl.multiple_of(col * STRIP, STRIP), STRIP)
            part = jnp.dot(act[...], wd[:, span], preferred_element_type=jnp.float32)
            pown[chip, :, span] = part[:rows]
            psend[chip, :, span] = part[rows:].astype(jnp.bfloat16)
            return carry

        lax.fori_loop(0, width // STRIP, one_col, 0)
        rd_copy(chip).start()
        return carry

    lax.fori_loop(0, 4, one_step, 0)

    @pl.when(is_end)
    def _():
        end_send(mir(0))
        rd_copy(z).wait_recv()
        base = pown[z] + precv[z].astype(jnp.float32) + resid_ref[...].astype(jnp.float32)
        pown[z] = base
        for k in range(NRS):
            span = pl.ds(k * rsub, rsub)
            rs_copy(z, k, rrecv_m, rs_recv_m, dev_m).wait_recv()
            out_ref[span] = (pown[z, span] + rrecv_m[z, span].astype(jnp.float32)).astype(jnp.bfloat16)

    @pl.when(is_int)
    def _():
        def pass_on(chip, dst_in, sem_in, dst_out, sem_out, dev):
            rd_copy(chip).wait_recv()
            for k in range(NRS):
                span = pl.ds(k * rsub, rsub)
                rs_copy(chip, k, dst_in, sem_in, dev_m).wait_recv()
                rsend[chip, span] = (rs_base(chip, k) + dst_in[chip, span].astype(jnp.float32)).astype(jnp.bfloat16)
                rs_copy(chip, k, dst_out, sem_out, dev).start()

        def own_send(chip):
            pass_on(chip, rrecv_e, rs_recv_e, rrecv_m, rs_recv_m, dev_m)

        own_send(mir(1))
        rd_copy(z).wait_recv()
        for k in range(NRS):
            rs_copy(z, k, rrecv_e, rs_recv_e, dev_m).wait_recv()
        pown[z] = pown[z] + precv[z].astype(jnp.float32) + resid_ref[...].astype(jnp.float32) + rrecv_e[z].astype(jnp.float32)
        own_send(mir(0))
        for k in range(NRS):
            span = pl.ds(k * rsub, rsub)
            rs_copy(z, k, rrecv_m, rs_recv_m, dev_m).wait_recv()
            out_ref[span] = (pown[z, span] + rrecv_m[z, span].astype(jnp.float32)).astype(jnp.bfloat16)
        pass_on(mir(3), rrecv_m, rs_recv_m, rrecv_m, rs_recv_m, dev_e)

    for k in range(NSUB):
        for chip in range(4):
            ag_d2d(landed(chip, k), chip, k).wait_send()
        ag_copy(landed(z, k), z, k, ag_send_m, dev_m).wait_send()

        @pl.when(is_int)
        def _():
            ag_copy(landed(z, k), z, k, ag_send_e, dev_e).wait_send()
            ag_copy(landed(mir(3), k), mir(3), k, ag_send_m, dev_m).wait_send()
            ag_copy(landed(mir(1), k), mir(1), k, ag_send_e, dev_e).wait_send()
            ag_copy(landed(mir(0), k), mir(0), k, ag_send_e, dev_e).wait_send()

    for chip in range(4):
        rd_copy(chip).wait_send()

        @pl.when(chip != z)
        def _():
            for k in range(NRS):
                rs_copy(chip, k, rrecv_m, rs_recv_m, dev_m).wait_send()


def mlp_block(mlp_in, resid, w_gate_t, w_up_t, w_down):
    rows, width = mlp_in.shape
    ffn = w_gate_t.shape[0]
    bf16, f32 = jnp.bfloat16, jnp.float32
    vmem = pl.BlockSpec(memory_space=pltpu.VMEM)
    hbm = pl.BlockSpec(memory_space=pl.ANY)
    dma = pltpu.SemaphoreType.DMA
    flops = 3 * 2 * 8 * rows * width * ffn
    return pl.pallas_call(
        mlp_kernel,
        out_shape=jax.ShapeDtypeStruct((rows, width), bf16),
        in_specs=[vmem, vmem, hbm, hbm, hbm],
        out_specs=vmem,
        scratch_shapes=[
            pltpu.VMEM((4, 2, rows, width), bf16),
            pltpu.VMEM((ffn, width), bf16),
            pltpu.VMEM((ffn, width), bf16),
            pltpu.VMEM((ffn, width), bf16),
            pltpu.VMEM((2 * rows, ffn), bf16),
            pltpu.VMEM((4, rows, width), f32),
            pltpu.VMEM((4, rows, width), bf16),
            pltpu.VMEM((4, rows, width), bf16),
            pltpu.VMEM((4, rows, width), bf16),
            pltpu.VMEM((4, rows, width), bf16),
            pltpu.VMEM((4, rows, width), bf16),
            dma((3,)),
            dma((4, NSUB)), dma((4, NSUB)), dma((4, NSUB)), dma((4, NSUB)), dma((4, NSUB)),
            dma((4,)), dma((4,)),
            dma((4, NRS)), dma((4, NRS)), dma((4, NRS)),
        ],
        compiler_params=pltpu.CompilerParams(collective_id=0, has_side_effects=True, vmem_limit_bytes=60 * 1024 * 1024),
        cost_estimate=pl.CostEstimate(flops=flops, bytes_accessed=3 * 2 * ffn * width, transcendentals=8 * rows * ffn),
        name='mlp_exchange',
    )(mlp_in, resid, w_gate_t, w_up_t, w_down)


def solution(mesh):
    rows_spec = P(('dp', 'tp'), None)
    cache_spec = P(('dp', 'tp'), None, None)
    whole = P()
    in_specs = (rows_spec, cache_spec, cache_spec, P(('dp', 'tp')), whole, whole, whole, whole, whole, whole, whole, whole, P(None, 'tp'), P(None, 'tp'), P('tp', None))
    out_specs = (rows_spec, rows_spec, rows_spec)

    def device_step(hidden, cache_lat, cache_rope, seq_lens, attn_norm, w_query, w_kv_down, kv_norm, w_key_up, w_val_up, w_out, mlp_norm, w_gate, w_up, w_down):
        resid, mlp_in, lat_new, rope_new = attention_block(hidden, cache_lat, cache_rope, seq_lens, attn_norm, w_query, w_kv_down, kv_norm, w_key_up, w_val_up, w_out, mlp_norm)
        out_hidden = mlp_block(mlp_in, resid, w_gate.T, w_up.T, w_down)
        return out_hidden, lat_new, rope_new

    return jax.shard_map(device_step, mesh=mesh, in_specs=in_specs, out_specs=out_specs, check_vma=False)
```

```python
import math

import jax
import jax.numpy as jnp
from jax import lax
from jax.experimental import pallas as pl
from jax.experimental.pallas import tpu as pltpu
from jax.sharding import PartitionSpec as P

EPS = 1e-6
ROPE_BASE = 10000.0
ROPE_DIM = 64
NOPE_DIM = 128
VAL_DIM = 128
SCALE = (NOPE_DIM + ROPE_DIM) ** -0.5


GROUP = 4
SLOTS = 7
BLOCK = 128
Q_CHUNKS = 4
VMEM_LIMIT = 63 * 1024 * 1024


def attn_kernel(lens_ref, hidden_ref, lens_vec, attn_gain, kv_gain, mlp_gain, lat_hbm, rope_hbm, wq_hbm, wkv_hbm, wk_hbm, wv_hbm, wo_hbm,
                resid_ref, mlp_in_ref, lat_new_ref, rope_new_ref,
                keys, rope, wq, wkv, wk, wv, wo, normed, qs, ol, qr, lat_row, rope_row, heads_out, order, key_sem, w_sem):
    f32, bf16 = jnp.float32, jnp.bfloat16
    rows, width = hidden_ref.shape
    rank = wk.shape[0]
    heads = wk.shape[1] // NOPE_DIM
    groups = rows // GROUP
    classes = keys.shape[2] // BLOCK

    chunk = wq.shape[2]
    w_copies = [pltpu.make_async_copy(wkv_hbm, wkv, w_sem.at[0]), pltpu.make_async_copy(wk_hbm, wk, w_sem.at[1])]
    w_copies += [pltpu.make_async_copy(wq_hbm.at[:, pl.ds(j * chunk, chunk)], wq.at[j], w_sem.at[2 + j]) for j in range(Q_CHUNKS)]
    rope_copy = pltpu.make_async_copy(rope_hbm, rope, w_sem.at[2 + Q_CHUNKS])
    late_copies = [pltpu.make_async_copy(wv_hbm, wv, w_sem.at[3 + Q_CHUNKS])]
    late_copies += [pltpu.make_async_copy(wo_hbm.at[:, pl.ds(n * 512, 512)], wo.at[n], w_sem.at[4 + Q_CHUNKS + n]) for n in range(width // 512)]
    for copy in w_copies[:4]:
        copy.start()

    def kind(b):
        return lax.div(lens_ref[b], BLOCK)

    def count(b, counts):
        k = kind(b)
        return tuple(n + jnp.where(k == i, 1, 0) for i, n in enumerate(counts))

    zero = jnp.int32(0)
    counts = lax.fori_loop(0, rows, count, (zero,) * classes)
    firsts = []
    total = zero
    for i in reversed(range(classes)):
        firsts.append(total)
        total = total + counts[i]
    firsts = tuple(reversed(firsts))

    def place(b, firsts):
        k = kind(b)
        at = firsts[0]
        for i in range(1, classes):
            at = jnp.where(k == i, firsts[i], at)
        order[at] = b
        return tuple(n + jnp.where(k == i, 1, 0) for i, n in enumerate(firsts))

    lax.fori_loop(0, rows, place, firsts)

    def group_copies(g, blocks):
        slot = lax.rem(g, SLOTS)
        return [pltpu.make_async_copy(lat_hbm.at[order[g * GROUP + i], pl.ds(0, blocks * BLOCK)], keys.at[slot, i, pl.ds(0, blocks * BLOCK)], key_sem.at[slot, i]) for i in range(GROUP)]

    def per_class(g, fn):
        k = kind(order[g * GROUP])
        for i in range(classes):
            @pl.when(k == i)
            def _():
                fn(i + 1)

    def start_group(g):
        def start(blocks):
            for copy in group_copies(g, blocks):
                copy.start()

        per_class(g, start)

    def start_first(g, carry):
        start_group(g)
        return carry

    vals = hidden_ref[...].astype(f32)
    inv_rms = lax.rsqrt(jnp.mean(vals * vals, axis=-1, keepdims=True) + EPS)
    normed[...] = (vals * inv_rms * attn_gain[...].astype(f32)[None]).astype(bf16)

    lane = lax.broadcasted_iota(jnp.int32, (rows, 2 * ROPE_DIM), 1)
    half = ROPE_DIM // 2
    freq = jnp.exp(lax.rem(lane, half).astype(f32) * (-math.log(ROPE_BASE) / half))
    square_ids = (rows, rows)
    diagonal = lax.broadcasted_iota(jnp.int32, square_ids, 0) == lax.broadcasted_iota(jnp.int32, square_ids, 1)
    lens = jnp.sum(jnp.where(diagonal, lens_vec[...].astype(f32)[None], 0.0), axis=1, keepdims=True)
    angles = lens * freq
    cos_tab = jnp.cos(angles)
    is_first = lax.rem(lane, ROPE_DIM) < half
    sin_tab = jnp.where(is_first, -jnp.sin(angles), jnp.sin(angles))

    def rotate_pair(pair):
        swapped = jnp.where(is_first, pltpu.roll(pair, 2 * ROPE_DIM - half, 1), pltpu.roll(pair, half, 1))
        return (pair * cos_tab + swapped * sin_tab).astype(bf16).astype(f32)

    w_copies[0].wait()
    for copy in w_copies[4:]:
        copy.start()
    kv = lax.dot_general(normed[...], wkv[...], (((1,), (1,)), ((), ())), preferred_element_type=f32).astype(bf16).astype(f32)
    lat = kv[:, :rank]
    inv_lat = lax.rsqrt(jnp.mean(lat * lat, axis=-1, keepdims=True) + EPS)
    lat_new = (lat * inv_lat * kv_gain[...].astype(f32)[None]).astype(bf16)
    lat_new_ref[...] = lat_new
    lat_row[...] = lat_new.astype(f32)
    pe = kv[:, rank:]
    rope_new = rotate_pair(jnp.concatenate([pe, pe], axis=1))
    rope_new_ref[...] = rope_new[:, :ROPE_DIM].astype(bf16)
    rope_row[...] = rope_new

    w_copies[1].wait()
    low = lane < ROPE_DIM

    def put_head(head, nope, pe_rot):
        key_up = wk[:, head * NOPE_DIM:(head + 1) * NOPE_DIM]
        q_lat = lax.dot_general(nope.astype(bf16), key_up, (((1,), (1,)), ((), ())), preferred_element_type=f32).astype(bf16).astype(f32)
        for part in range(rank // 128):
            qs[part, pl.ds(head, rows, stride=heads), :] = q_lat[:, part * 128:(part + 1) * 128]
        qr[pl.ds(head, rows, stride=heads), :] = pe_rot

    for j in range(Q_CHUNKS):
        w_copies[2 + j].wait()
        if j == 1:
            rope_copy.start()
        first, last = j * SLOTS // Q_CHUNKS, (j + 1) * SLOTS // Q_CHUNKS
        lax.fori_loop(first, last, start_first, 0)
        query = jnp.dot(normed[...], wq[j], preferred_element_type=f32).astype(bf16).astype(f32)
        for pair in range(chunk // 384):
            base = pair * 384
            part_a, part_b, part_c = (query[:, base + 128 * i:base + 128 * (i + 1)] for i in range(3))
            pe_rot = rotate_pair(jnp.where(low, part_b, part_c))
            head = (j * chunk + base) // 192
            put_head(head, part_a, pe_rot)
            put_head(head + 1, jnp.where(low, pltpu.roll(part_b, ROPE_DIM, 1), pltpu.roll(part_c, ROPE_DIM, 1)), pltpu.roll(pe_rot, ROPE_DIM, 1))

    rope_copy.wait()

    def attend(g, blocks):
        slot = lax.rem(g, SLOTS)
        span = blocks * BLOCK
        for copy in group_copies(g, blocks):
            copy.wait()
        scores = []
        picks = [order[g * GROUP + i] for i in range(GROUP)]
        for i, b in enumerate(picks):
            length = lens_ref[b]
            base = pl.multiple_of(lax.div(length, 16) * 16, 16)
            tile = keys[slot, i, pl.ds(base, 16), :].astype(f32)
            sub = lax.broadcasted_iota(jnp.int32, (16, rank), 0)
            keys[slot, i, pl.ds(base, 16), :] = jnp.where(sub == length - base, lat_row[pl.ds(b, 1), :], tile).astype(bf16)
        for i, b in enumerate(picks):
            length = lens_ref[b]
            mine = pl.ds(pl.multiple_of(b * heads, heads), heads)
            q_lat = jnp.concatenate([qs[part, mine, :] for part in range(rank // 128)], axis=1).astype(bf16)
            q_rot = qr[mine, :]
            score = lax.dot_general(q_lat, keys[slot, i, :span], (((1,), (1,)), ((), ())), preferred_element_type=f32)
            near = jnp.dot(q_rot[:, :ROPE_DIM].astype(bf16), rope[b, :, :span], preferred_element_type=f32)
            first = lax.broadcasted_iota(jnp.int32, (heads, 2 * ROPE_DIM), 1) < ROPE_DIM
            new = jnp.sum(jnp.where(first, q_rot * rope_row[pl.ds(b, 1), :], 0.0), axis=1, keepdims=True)
            at = lax.broadcasted_iota(jnp.int32, (heads, span), 1)
            score = (score + jnp.where(at == length, new, near)) * SCALE
            scores.append(jnp.where(at <= length, score, -jnp.inf))
        probs = []
        for score in scores:
            expo = jnp.exp(score - jnp.max(score, axis=1, keepdims=True))
            probs.append((expo / jnp.sum(expo, axis=1, keepdims=True)).astype(bf16))
        for i, b in enumerate(picks):
            out = jnp.dot(probs[i], keys[slot, i, :span], preferred_element_type=f32)
            for part in range(rank // 128):
                ol[part, pl.ds(b, heads, stride=rows), :] = out[:, part * 128:(part + 1) * 128]

    def one_group(g, carry):
        per_class(g, lambda blocks: attend(g, blocks))

        @pl.when(g + SLOTS < groups)
        def _():
            start_group(g + SLOTS)

        @pl.when(g == groups - SLOTS - 2)
        def _():
            for copy in late_copies:
                copy.start()

        return carry

    lax.fori_loop(0, groups, one_group, 0)

    late_copies[0].wait()
    for head in range(heads):
        cols = slice(head * VAL_DIM, (head + 1) * VAL_DIM)
        lat_out = jnp.concatenate([ol[part, head * rows:(head + 1) * rows, :] for part in range(rank // 128)], axis=1).astype(bf16)
        heads_out[:, cols] = jnp.dot(lat_out, wv[:, cols], preferred_element_type=f32).astype(bf16)
    square = jnp.zeros((rows, 1), f32)
    for n in range(width // 512):
        cols = slice(n * 512, (n + 1) * 512)
        late_copies[1 + n].wait()
        attn_out = jnp.dot(heads_out[...], wo[n], preferred_element_type=f32)
        resid = (hidden_ref[:, cols].astype(f32) + attn_out).astype(bf16)
        resid_ref[:, cols] = resid
        square = square + jnp.sum(resid.astype(f32) * resid.astype(f32), axis=-1, keepdims=True)
    inv_rms = lax.rsqrt(square * (1.0 / width) + EPS)
    mlp_in_ref[...] = (resid_ref[...].astype(f32) * inv_rms * mlp_gain[...].astype(f32)[None]).astype(bf16)


def attention_block(hidden, cache_lat, cache_rope, seq_lens, attn_norm, w_query, w_kv_down, kv_norm, w_key_up, w_val_up, w_out, mlp_norm):
    rows, width = hidden.shape
    slots, rank = cache_lat.shape[1:]
    bf16, f32 = jnp.bfloat16, jnp.float32
    heads = w_key_up.shape[1] // NOPE_DIM
    q_width = w_query.shape[1]
    vmem = pl.BlockSpec(memory_space=pltpu.VMEM)
    hbm = pl.BlockSpec(memory_space=pl.ANY)
    smem = pl.BlockSpec(memory_space=pltpu.SMEM)
    dma = pltpu.SemaphoreType.DMA
    flops = 2 * rows * (width * (q_width + rank + ROPE_DIM + width) + heads * rank * (NOPE_DIM + VAL_DIM) + heads * slots * (2 * rank + ROPE_DIM))
    moved = 2 * (width * (q_width + rank + ROPE_DIM + width) + heads * rank * (NOPE_DIM + VAL_DIM) + rows * slots * (rank + ROPE_DIM))
    return pl.pallas_call(
        attn_kernel,
        out_shape=(
            jax.ShapeDtypeStruct((rows, width), bf16),
            jax.ShapeDtypeStruct((rows, width), bf16),
            jax.ShapeDtypeStruct((rows, rank), bf16),
            jax.ShapeDtypeStruct((rows, ROPE_DIM), bf16),
        ),
        in_specs=[smem] + [vmem] * 5 + [hbm] * 7,
        out_specs=(vmem,) * 4,
        scratch_shapes=[
            pltpu.VMEM((SLOTS, GROUP, slots, rank), bf16),
            pltpu.VMEM((rows, ROPE_DIM, slots), bf16),
            pltpu.VMEM((Q_CHUNKS, width, q_width // Q_CHUNKS), bf16),
            pltpu.VMEM((rank + ROPE_DIM, width), bf16),
            pltpu.VMEM((rank, heads * NOPE_DIM), bf16),
            pltpu.VMEM((rank, heads * VAL_DIM), bf16),
            pltpu.VMEM((width // 512, heads * VAL_DIM, 512), bf16),
            pltpu.VMEM((rows, width), bf16),
            pltpu.VMEM((rank // 128, rows * heads, 128), f32),
            pltpu.VMEM((rank // 128, rows * heads, 128), f32),
            pltpu.VMEM((rows * heads, 2 * ROPE_DIM), f32),
            pltpu.VMEM((rows, rank), f32),
            pltpu.VMEM((rows, 2 * ROPE_DIM), f32),
            pltpu.VMEM((rows, heads * VAL_DIM), bf16),
            pltpu.SMEM((rows,), jnp.int32),
            dma((SLOTS, GROUP)),
            dma((4 + Q_CHUNKS + width // 512,)),
        ],
        compiler_params=pltpu.CompilerParams(vmem_limit_bytes=VMEM_LIMIT),
        cost_estimate=pl.CostEstimate(flops=flops, bytes_accessed=moved, transcendentals=rows * heads * slots),
        name='latent_attention',
    )(seq_lens, hidden, seq_lens, attn_norm, kv_norm, mlp_norm, cache_lat, jnp.swapaxes(cache_rope, 1, 2), w_query, w_kv_down.T, w_key_up, w_val_up, w_out)


MESH = pl.DeviceIdType.MESH
NSUB = 2
NRS = 8
STRIP = 256
HALVES = 2


def mlp_kernel(g_ref, resid_ref, wg_hbm, wu_hbm, wd_hbm, out_ref,
               g_all, wg, wu, wd, act, pown, psend, precv, rsend, rrecv_e, rrecv_m,
               w_sem, ag_recv, ag_recv_d, ag_send_e, ag_send_m, ag_send_d,
               rd_recv, rd_send, rs_recv_e, rs_recv_m, rs_send):
    ffn = wg.shape[0]
    rows, width = g_ref.shape
    sub = rows // NSUB
    rsub = rows // NRS
    me = lax.axis_index('tp')
    z = lax.div(me, 2)
    c = lax.rem(me, 2)
    upper = z >= 2
    is_end = jnp.logical_or(z == 0, z == 3)
    is_int = jnp.logical_not(is_end)

    def mir(k):
        return jnp.where(upper, k, 3 - k)

    partner = 2 * z + (1 - c)
    dev_e = jnp.where(is_end, me, 2 * mir(3) + c)
    dev_m = 2 * jnp.where(is_end, mir(2), mir(1)) + c

    w_copies = []
    for idx, (src, dst) in enumerate(((wg_hbm, wg), (wu_hbm, wu), (wd_hbm, wd))):
        copy = pltpu.make_async_copy(src, dst, w_sem.at[idx])
        w_copies.append(copy)
    w_copies[0].start()
    w_copies[1].start()

    barrier = pltpu.get_barrier_semaphore()
    pl.semaphore_signal(barrier, inc=1, device_id={'tp': partner}, device_id_type=MESH)
    pl.semaphore_signal(barrier, inc=1, device_id={'tp': dev_m}, device_id_type=MESH)

    @pl.when(is_int)
    def _():
        pl.semaphore_signal(barrier, inc=1, device_id={'tp': dev_e}, device_id_type=MESH)
        pl.semaphore_wait(barrier, 3)

    @pl.when(is_end)
    def _():
        pl.semaphore_wait(barrier, 2)

    def remote(src, dst, send_sem, recv_sem, dev):
        return pltpu.make_async_remote_copy(src_ref=src, dst_ref=dst, send_sem=send_sem, recv_sem=recv_sem, device_id={'tp': dev}, device_id_type=MESH)

    def ag_copy(src, chip, k, send_sem, dev):
        return remote(src, g_all.at[chip, 0, pl.ds(k * sub, sub)], send_sem.at[chip, k], ag_recv.at[chip, k], dev)

    def ag_d2d(src, chip, k):
        return remote(src, g_all.at[chip, 1, pl.ds(k * sub, sub)], ag_send_d.at[chip, k], ag_recv_d.at[chip, k], partner)

    for k in range(NSUB):
        piece = g_ref.at[pl.ds(k * sub, sub)]
        ag_copy(piece, z, k, ag_send_m, dev_m).start()

        @pl.when(is_int)
        def _():
            ag_copy(piece, z, k, ag_send_e, dev_e).start()

        ag_d2d(piece, z, k).start()
    g_all[z, 0] = g_ref[...]

    def landed(chip, k):
        return g_all.at[chip, 0, pl.ds(k * sub, sub)]

    def arrive(chip, k, send_sem, dev):
        src = landed(chip, k)
        ag_copy(src, chip, k, ag_send_d, dev_m).wait_recv()
        if dev is not None:
            ag_copy(src, chip, k, send_sem, dev).start()
        ag_d2d(src, chip, k).start()

    def both(chip):
        for k in range(NSUB):
            ag_d2d(landed(chip, k), chip, k).wait_recv()

    def rd_copy(chip, part):
        span = pl.ds(pl.multiple_of(part * (width // HALVES), width // HALVES), width // HALVES)
        return remote(psend.at[chip, :, span], precv.at[chip, :, span], rd_send.at[chip, part], rd_recv.at[chip, part], partner)

    def rd_wait(chip):
        for part in range(HALVES):
            rd_copy(chip, part).wait_recv()

    def rs_copy(chip, k, dst, recv_sem, dev):
        span = pl.ds(k * rsub, rsub)
        return remote(rsend.at[chip, span], dst.at[chip, span], rs_send.at[chip, k], recv_sem.at[chip, k], dev)

    def rs_base(chip, k):
        span = pl.ds(k * rsub, rsub)
        return pown[chip, span] + precv[chip, span].astype(jnp.float32)

    def end_send(chip):
        rd_wait(chip)
        for k in range(NRS):
            rsend[chip, pl.ds(k * rsub, rsub)] = rs_base(chip, k).astype(jnp.bfloat16)
            rs_copy(chip, k, rrecv_e, rs_recv_e, dev_m).start()

    def hook(step, strip):
        def at(role, want_step, want_strip, fn):
            pl.when(jnp.logical_and(role, jnp.logical_and(step == want_step, strip == want_strip)))(fn)

        def int_a():
            arrive(mir(3), 1, ag_send_m, dev_m)
            arrive(mir(1), 1, ag_send_e, dev_e)

        at(is_int, 0, 1, int_a)
        at(is_int, 1, 0, lambda: arrive(mir(0), 0, ag_send_e, dev_e))
        at(is_int, 1, 3, lambda: arrive(mir(0), 1, ag_send_e, dev_e))
        at(is_end, 0, 2, lambda: arrive(mir(1), 0, None, None))
        at(is_end, 1, 0, lambda: end_send(mir(2)))
        at(is_end, 1, 2, lambda: arrive(mir(0), 0, None, None))
        at(is_end, 2, 0, lambda: end_send(mir(1)))
        at(is_end, 3, 0, lambda: end_send(mir(0)))

    def swiglu(lhs, at, count):
        gate = lax.dot_general(lhs, wg[pl.ds(at, count)], (((1,), (1,)), ((), ())), preferred_element_type=jnp.float32)
        up = lax.dot_general(lhs, wu[pl.ds(at, count)], (((1,), (1,)), ((), ())), preferred_element_type=jnp.float32)
        return (gate / (1.0 + jnp.exp(-gate)) * up).astype(jnp.bfloat16)

    whole = ffn // STRIP
    rest = ffn - whole * STRIP

    def one_step(step, carry):
        chip = mir(jnp.where(is_end, lax.rem(6 - step, 4), jnp.where(step == 0, 2, jnp.where(step == 1, 3, 3 - step))))

        @pl.when(jnp.logical_and(step == 0, is_int))
        def _():
            arrive(mir(3), 0, ag_send_m, dev_m)
            arrive(mir(1), 0, ag_send_e, dev_e)

        @pl.when(jnp.logical_and(step == 0, is_end))
        def _():
            arrive(mir(2), 0, None, None)
            arrive(mir(2), 1, None, None)

        @pl.when(jnp.logical_and(step == 1, is_end))
        def _():
            arrive(mir(1), 1, None, None)

        @pl.when(jnp.logical_and(step == 2, is_end))
        def _():
            arrive(mir(0), 1, None, None)

        both(chip)

        @pl.when(step == 0)
        def _():
            w_copies[0].wait()
            w_copies[1].wait()
            w_copies[2].start()

        def one_strip(strip, carry):
            at = pl.multiple_of(strip * STRIP, STRIP)
            act[:, pl.ds(at, STRIP)] = swiglu(g_all[chip].reshape(2 * rows, width), at, STRIP)
            hook(step, strip)
            return carry

        lax.fori_loop(0, whole, one_strip, 0)
        act[:, whole * STRIP:] = swiglu(g_all[chip].reshape(2 * rows, width), whole * STRIP, rest)

        @pl.when(step == 0)
        def _():
            w_copies[2].wait()

        def one_part(part, carry):
            wide = width // HALVES
            span = pl.ds(pl.multiple_of(part * wide, wide), wide)
            down = jnp.dot(act[...], wd[:, span], preferred_element_type=jnp.float32)
            psend[chip, :, span] = down[rows:].astype(jnp.bfloat16)
            pown[chip, :, span] = down[:rows]
            rd_copy(chip, part).start()
            return carry

        lax.fori_loop(0, HALVES, one_part, 0)
        return carry

    lax.fori_loop(0, 4, one_step, 0)

    @pl.when(is_end)
    def _():
        rd_wait(z)
        base = pown[z] + precv[z].astype(jnp.float32) + resid_ref[...].astype(jnp.float32)
        pown[z] = base
        for k in range(NRS):
            span = pl.ds(k * rsub, rsub)
            rs_copy(z, k, rrecv_m, rs_recv_m, dev_m).wait_recv()
            out_ref[span] = (pown[z, span] + rrecv_m[z, span].astype(jnp.float32)).astype(jnp.bfloat16)

    @pl.when(is_int)
    def _():
        def pass_on(chip, dst_in, sem_in, dst_out, sem_out, dev):
            rd_wait(chip)
            for k in range(NRS):
                span = pl.ds(k * rsub, rsub)
                rs_copy(chip, k, dst_in, sem_in, dev_m).wait_recv()
                rsend[chip, span] = (rs_base(chip, k) + dst_in[chip, span].astype(jnp.float32)).astype(jnp.bfloat16)
                rs_copy(chip, k, dst_out, sem_out, dev).start()

        def own_send(chip):
            pass_on(chip, rrecv_e, rs_recv_e, rrecv_m, rs_recv_m, dev_m)

        own_send(mir(1))
        rd_wait(z)
        for k in range(NRS):
            rs_copy(z, k, rrecv_e, rs_recv_e, dev_m).wait_recv()
        pown[z] = pown[z] + precv[z].astype(jnp.float32) + resid_ref[...].astype(jnp.float32) + rrecv_e[z].astype(jnp.float32)
        own_send(mir(0))
        for k in range(NRS):
            span = pl.ds(k * rsub, rsub)
            rs_copy(z, k, rrecv_m, rs_recv_m, dev_m).wait_recv()
            out_ref[span] = (pown[z, span] + rrecv_m[z, span].astype(jnp.float32)).astype(jnp.bfloat16)
        pass_on(mir(3), rrecv_m, rs_recv_m, rrecv_m, rs_recv_m, dev_e)

    for k in range(NSUB):
        for chip in range(4):
            ag_d2d(landed(chip, k), chip, k).wait_send()
        ag_copy(landed(z, k), z, k, ag_send_m, dev_m).wait_send()

        @pl.when(is_int)
        def _():
            ag_copy(landed(z, k), z, k, ag_send_e, dev_e).wait_send()
            ag_copy(landed(mir(3), k), mir(3), k, ag_send_m, dev_m).wait_send()
            ag_copy(landed(mir(1), k), mir(1), k, ag_send_e, dev_e).wait_send()
            ag_copy(landed(mir(0), k), mir(0), k, ag_send_e, dev_e).wait_send()

    for chip in range(4):
        for part in range(HALVES):
            rd_copy(chip, part).wait_send()

        @pl.when(chip != z)
        def _():
            for k in range(NRS):
                rs_copy(chip, k, rrecv_m, rs_recv_m, dev_m).wait_send()


def mlp_block(mlp_in, resid, w_gate_t, w_up_t, w_down):
    rows, width = mlp_in.shape
    ffn = w_gate_t.shape[0]
    bf16, f32 = jnp.bfloat16, jnp.float32
    vmem = pl.BlockSpec(memory_space=pltpu.VMEM)
    hbm = pl.BlockSpec(memory_space=pl.ANY)
    dma = pltpu.SemaphoreType.DMA
    flops = 3 * 2 * 8 * rows * width * ffn
    return pl.pallas_call(
        mlp_kernel,
        out_shape=jax.ShapeDtypeStruct((rows, width), bf16),
        in_specs=[vmem, vmem, hbm, hbm, hbm],
        out_specs=vmem,
        scratch_shapes=[
            pltpu.VMEM((4, 2, rows, width), bf16),
            pltpu.VMEM((ffn, width), bf16),
            pltpu.VMEM((ffn, width), bf16),
            pltpu.VMEM((ffn, width), bf16),
            pltpu.VMEM((2 * rows, ffn), bf16),
            pltpu.VMEM((4, rows, width), f32),
            pltpu.VMEM((4, rows, width), bf16),
            pltpu.VMEM((4, rows, width), bf16),
            pltpu.VMEM((4, rows, width), bf16),
            pltpu.VMEM((4, rows, width), bf16),
            pltpu.VMEM((4, rows, width), bf16),
            dma((3,)),
            dma((4, NSUB)), dma((4, NSUB)), dma((4, NSUB)), dma((4, NSUB)), dma((4, NSUB)),
            dma((4, HALVES)), dma((4, HALVES)),
            dma((4, NRS)), dma((4, NRS)), dma((4, NRS)),
        ],
        compiler_params=pltpu.CompilerParams(collective_id=0, has_side_effects=True, vmem_limit_bytes=60 * 1024 * 1024),
        cost_estimate=pl.CostEstimate(flops=flops, bytes_accessed=3 * 2 * ffn * width, transcendentals=8 * rows * ffn),
        name='mlp_exchange',
    )(mlp_in, resid, w_gate_t, w_up_t, w_down)


def solution(mesh):
    rows_spec = P(('dp', 'tp'), None)
    cache_spec = P(('dp', 'tp'), None, None)
    whole = P()
    in_specs = (rows_spec, cache_spec, cache_spec, P(('dp', 'tp')), whole, whole, whole, whole, whole, whole, whole, whole, P(None, 'tp'), P(None, 'tp'), P('tp', None))
    out_specs = (rows_spec, rows_spec, rows_spec)

    def device_step(hidden, cache_lat, cache_rope, seq_lens, attn_norm, w_query, w_kv_down, kv_norm, w_key_up, w_val_up, w_out, mlp_norm, w_gate, w_up, w_down):
        resid, mlp_in, lat_new, rope_new = attention_block(hidden, cache_lat, cache_rope, seq_lens, attn_norm, w_query, w_kv_down, kv_norm, w_key_up, w_val_up, w_out, mlp_norm)
        out_hidden = mlp_block(mlp_in, resid, w_gate.T, w_up.T, w_down)
        return out_hidden, lat_new, rope_new

    return jax.shard_map(device_step, mesh=mesh, in_specs=in_specs, out_specs=out_specs, check_vma=False)
```

```python
import math

import jax
import jax.numpy as jnp
from jax import lax
from jax.experimental import pallas as pl
from jax.experimental.pallas import tpu as pltpu
from jax.sharding import PartitionSpec as P

EPS = 1e-6
ROPE_BASE = 10000.0
ROPE_DIM = 64
NOPE_DIM = 128
VAL_DIM = 128
SCALE = (NOPE_DIM + ROPE_DIM) ** -0.5


GROUP = 4
SLOTS = 7
BLOCK = 128
Q_CHUNKS = 4
VMEM_LIMIT = 63 * 1024 * 1024


def attn_kernel(lens_ref, hidden_ref, lens_vec, attn_gain, kv_gain, mlp_gain, lat_hbm, rope_hbm, wq_hbm, wkv_hbm, wk_hbm, wv_hbm, wo_hbm,
                resid_ref, mlp_in_ref, lat_new_ref, rope_new_ref,
                keys, rope, wq, wkv, wk, wv, wo, normed, qs, ol, qr, lat_row, rope_row, heads_out, order, key_sem, w_sem):
    f32, bf16 = jnp.float32, jnp.bfloat16
    rows, width = hidden_ref.shape
    rank = wk.shape[0]
    heads = wk.shape[1] // NOPE_DIM
    groups = rows // GROUP
    classes = keys.shape[2] // BLOCK

    chunk = wq.shape[2]
    w_copies = [pltpu.make_async_copy(wkv_hbm, wkv, w_sem.at[0]), pltpu.make_async_copy(wk_hbm, wk, w_sem.at[1])]
    w_copies += [pltpu.make_async_copy(wq_hbm.at[:, pl.ds(j * chunk, chunk)], wq.at[j], w_sem.at[2 + j]) for j in range(Q_CHUNKS)]
    rope_copy = pltpu.make_async_copy(rope_hbm, rope, w_sem.at[2 + Q_CHUNKS])
    late_copies = [pltpu.make_async_copy(wv_hbm, wv, w_sem.at[3 + Q_CHUNKS])]
    late_copies += [pltpu.make_async_copy(wo_hbm.at[:, pl.ds(n * 512, 512)], wo.at[n], w_sem.at[4 + Q_CHUNKS + n]) for n in range(width // 512)]
    for copy in w_copies:
        copy.start()
    rope_copy.start()

    def kind(b):
        return lax.div(lens_ref[b], BLOCK)

    def count(b, counts):
        k = kind(b)
        return tuple(n + jnp.where(k == i, 1, 0) for i, n in enumerate(counts))

    zero = jnp.int32(0)
    counts = lax.fori_loop(0, rows, count, (zero,) * classes)
    firsts = []
    total = zero
    for i in reversed(range(classes)):
        firsts.append(total)
        total = total + counts[i]
    firsts = tuple(reversed(firsts))

    def place(b, firsts):
        k = kind(b)
        at = firsts[0]
        for i in range(1, classes):
            at = jnp.where(k == i, firsts[i], at)
        order[at] = b
        return tuple(n + jnp.where(k == i, 1, 0) for i, n in enumerate(firsts))

    lax.fori_loop(0, rows, place, firsts)

    def group_copies(g, blocks):
        slot = lax.rem(g, SLOTS)
        return [pltpu.make_async_copy(lat_hbm.at[order[g * GROUP + i], pl.ds(0, blocks * BLOCK)], keys.at[slot, i, pl.ds(0, blocks * BLOCK)], key_sem.at[slot, i]) for i in range(GROUP)]

    def per_class(g, fn):
        k = kind(order[g * GROUP])
        for i in range(classes):
            @pl.when(k == i)
            def _():
                fn(i + 1)

    def start_group(g):
        def start(blocks):
            for copy in group_copies(g, blocks):
                copy.start()

        per_class(g, start)

    def start_first(g, carry):
        start_group(g)
        return carry

    lax.fori_loop(0, SLOTS, start_first, 0)

    vals = hidden_ref[...].astype(f32)
    inv_rms = lax.rsqrt(jnp.mean(vals * vals, axis=-1, keepdims=True) + EPS)
    normed[...] = (vals * inv_rms * attn_gain[...].astype(f32)[None]).astype(bf16)

    lane = lax.broadcasted_iota(jnp.int32, (rows, 2 * ROPE_DIM), 1)
    half = ROPE_DIM // 2
    freq = jnp.exp(lax.rem(lane, half).astype(f32) * (-math.log(ROPE_BASE) / half))
    square_ids = (rows, rows)
    diagonal = lax.broadcasted_iota(jnp.int32, square_ids, 0) == lax.broadcasted_iota(jnp.int32, square_ids, 1)
    lens = jnp.sum(jnp.where(diagonal, lens_vec[...].astype(f32)[None], 0.0), axis=1, keepdims=True)
    angles = lens * freq
    cos_tab = jnp.cos(angles)
    is_first = lax.rem(lane, ROPE_DIM) < half
    sin_tab = jnp.where(is_first, -jnp.sin(angles), jnp.sin(angles))

    def rotate_pair(pair):
        swapped = jnp.where(is_first, pltpu.roll(pair, 2 * ROPE_DIM - half, 1), pltpu.roll(pair, half, 1))
        return (pair * cos_tab + swapped * sin_tab).astype(bf16).astype(f32)

    w_copies[0].wait()
    kv = lax.dot_general(normed[...], wkv[...], (((1,), (1,)), ((), ())), preferred_element_type=f32).astype(bf16).astype(f32)
    lat = kv[:, :rank]
    inv_lat = lax.rsqrt(jnp.mean(lat * lat, axis=-1, keepdims=True) + EPS)
    lat_new = (lat * inv_lat * kv_gain[...].astype(f32)[None]).astype(bf16)
    lat_new_ref[...] = lat_new
    lat_row[...] = lat_new.astype(f32)
    pe = kv[:, rank:]
    rope_new = rotate_pair(jnp.concatenate([pe, pe], axis=1))
    rope_new_ref[...] = rope_new[:, :ROPE_DIM].astype(bf16)
    rope_row[...] = rope_new

    w_copies[1].wait()
    low = lane < ROPE_DIM

    def put_head(head, nope, pe_rot):
        key_up = wk[:, head * NOPE_DIM:(head + 1) * NOPE_DIM]
        q_lat = lax.dot_general(nope.astype(bf16), key_up, (((1,), (1,)), ((), ())), preferred_element_type=f32).astype(bf16).astype(f32)
        for part in range(rank // 128):
            qs[part, pl.ds(head, rows, stride=heads), :] = q_lat[:, part * 128:(part + 1) * 128]
        qr[pl.ds(head, rows, stride=heads), :] = pe_rot

    for j in range(Q_CHUNKS):
        w_copies[2 + j].wait()
        query = jnp.dot(normed[...], wq[j], preferred_element_type=f32).astype(bf16).astype(f32)
        for pair in range(chunk // 384):
            base = pair * 384
            part_a, part_b, part_c = (query[:, base + 128 * i:base + 128 * (i + 1)] for i in range(3))
            pe_rot = rotate_pair(jnp.where(low, part_b, part_c))
            head = (j * chunk + base) // 192
            put_head(head, part_a, pe_rot)
            put_head(head + 1, jnp.where(low, pltpu.roll(part_b, ROPE_DIM, 1), pltpu.roll(part_c, ROPE_DIM, 1)), pltpu.roll(pe_rot, ROPE_DIM, 1))

    rope_copy.wait()

    def attend(g, blocks):
        slot = lax.rem(g, SLOTS)
        span = blocks * BLOCK
        for copy in group_copies(g, blocks):
            copy.wait()
        scores = []
        picks = [order[g * GROUP + i] for i in range(GROUP)]
        for i, b in enumerate(picks):
            length = lens_ref[b]
            base = pl.multiple_of(lax.div(length, 16) * 16, 16)
            tile = keys[slot, i, pl.ds(base, 16), :].astype(f32)
            sub = lax.broadcasted_iota(jnp.int32, (16, rank), 0)
            keys[slot, i, pl.ds(base, 16), :] = jnp.where(sub == length - base, lat_row[pl.ds(b, 1), :], tile).astype(bf16)
        for i, b in enumerate(picks):
            length = lens_ref[b]
            mine = pl.ds(pl.multiple_of(b * heads, heads), heads)
            q_lat = jnp.concatenate([qs[part, mine, :] for part in range(rank // 128)], axis=1).astype(bf16)
            q_rot = qr[mine, :]
            score = lax.dot_general(q_lat, keys[slot, i, :span], (((1,), (1,)), ((), ())), preferred_element_type=f32)
            near = jnp.dot(q_rot[:, :ROPE_DIM].astype(bf16), rope[b, :, :span], preferred_element_type=f32)
            first = lax.broadcasted_iota(jnp.int32, (heads, 2 * ROPE_DIM), 1) < ROPE_DIM
            new = jnp.sum(jnp.where(first, q_rot * rope_row[pl.ds(b, 1), :], 0.0), axis=1, keepdims=True)
            at = lax.broadcasted_iota(jnp.int32, (heads, span), 1)
            score = (score + jnp.where(at == length, new, near)) * SCALE
            scores.append(jnp.where(at <= length, score, -jnp.inf))
        probs = []
        for score in scores:
            expo = jnp.exp(score - jnp.max(score, axis=1, keepdims=True))
            probs.append((expo / jnp.sum(expo, axis=1, keepdims=True)).astype(bf16))
        for i, b in enumerate(picks):
            out = jnp.dot(probs[i], keys[slot, i, :span], preferred_element_type=f32)
            for part in range(rank // 128):
                ol[part, pl.ds(b, heads, stride=rows), :] = out[:, part * 128:(part + 1) * 128]

    def one_group(g, carry):
        per_class(g, lambda blocks: attend(g, blocks))

        @pl.when(g + SLOTS < groups)
        def _():
            start_group(g + SLOTS)

        @pl.when(g == groups - SLOTS - 2)
        def _():
            for copy in late_copies:
                copy.start()

        return carry

    lax.fori_loop(0, groups, one_group, 0)

    late_copies[0].wait()
    for head in range(heads):
        cols = slice(head * VAL_DIM, (head + 1) * VAL_DIM)
        lat_out = jnp.concatenate([ol[part, head * rows:(head + 1) * rows, :] for part in range(rank // 128)], axis=1).astype(bf16)
        heads_out[:, cols] = jnp.dot(lat_out, wv[:, cols], preferred_element_type=f32).astype(bf16)
    square = jnp.zeros((rows, 1), f32)
    for n in range(width // 512):
        cols = slice(n * 512, (n + 1) * 512)
        late_copies[1 + n].wait()
        attn_out = jnp.dot(heads_out[...], wo[n], preferred_element_type=f32)
        resid = (hidden_ref[:, cols].astype(f32) + attn_out).astype(bf16)
        resid_ref[:, cols] = resid
        square = square + jnp.sum(resid.astype(f32) * resid.astype(f32), axis=-1, keepdims=True)
    inv_rms = lax.rsqrt(square * (1.0 / width) + EPS)
    mlp_in_ref[...] = (resid_ref[...].astype(f32) * inv_rms * mlp_gain[...].astype(f32)[None]).astype(bf16)


def attention_block(hidden, cache_lat, cache_rope, seq_lens, attn_norm, w_query, w_kv_down, kv_norm, w_key_up, w_val_up, w_out, mlp_norm):
    rows, width = hidden.shape
    slots, rank = cache_lat.shape[1:]
    bf16, f32 = jnp.bfloat16, jnp.float32
    heads = w_key_up.shape[1] // NOPE_DIM
    q_width = w_query.shape[1]
    vmem = pl.BlockSpec(memory_space=pltpu.VMEM)
    hbm = pl.BlockSpec(memory_space=pl.ANY)
    smem = pl.BlockSpec(memory_space=pltpu.SMEM)
    dma = pltpu.SemaphoreType.DMA
    flops = 2 * rows * (width * (q_width + rank + ROPE_DIM + width) + heads * rank * (NOPE_DIM + VAL_DIM) + heads * slots * (2 * rank + ROPE_DIM))
    moved = 2 * (width * (q_width + rank + ROPE_DIM + width) + heads * rank * (NOPE_DIM + VAL_DIM) + rows * slots * (rank + ROPE_DIM))
    return pl.pallas_call(
        attn_kernel,
        out_shape=(
            jax.ShapeDtypeStruct((rows, width), bf16),
            jax.ShapeDtypeStruct((rows, width), bf16),
            jax.ShapeDtypeStruct((rows, rank), bf16),
            jax.ShapeDtypeStruct((rows, ROPE_DIM), bf16),
        ),
        in_specs=[smem] + [vmem] * 5 + [hbm] * 7,
        out_specs=(vmem,) * 4,
        scratch_shapes=[
            pltpu.VMEM((SLOTS, GROUP, slots, rank), bf16),
            pltpu.VMEM((rows, ROPE_DIM, slots), bf16),
            pltpu.VMEM((Q_CHUNKS, width, q_width // Q_CHUNKS), bf16),
            pltpu.VMEM((rank + ROPE_DIM, width), bf16),
            pltpu.VMEM((rank, heads * NOPE_DIM), bf16),
            pltpu.VMEM((rank, heads * VAL_DIM), bf16),
            pltpu.VMEM((width // 512, heads * VAL_DIM, 512), bf16),
            pltpu.VMEM((rows, width), bf16),
            pltpu.VMEM((rank // 128, rows * heads, 128), f32),
            pltpu.VMEM((rank // 128, rows * heads, 128), f32),
            pltpu.VMEM((rows * heads, 2 * ROPE_DIM), f32),
            pltpu.VMEM((rows, rank), f32),
            pltpu.VMEM((rows, 2 * ROPE_DIM), f32),
            pltpu.VMEM((rows, heads * VAL_DIM), bf16),
            pltpu.SMEM((rows,), jnp.int32),
            dma((SLOTS, GROUP)),
            dma((4 + Q_CHUNKS + width // 512,)),
        ],
        compiler_params=pltpu.CompilerParams(vmem_limit_bytes=VMEM_LIMIT),
        cost_estimate=pl.CostEstimate(flops=flops, bytes_accessed=moved, transcendentals=rows * heads * slots),
        name='latent_attention',
    )(seq_lens, hidden, seq_lens, attn_norm, kv_norm, mlp_norm, cache_lat, jnp.swapaxes(cache_rope, 1, 2), w_query, w_kv_down.T, w_key_up, w_val_up, w_out)


MESH = pl.DeviceIdType.MESH
NSUB = 2
NRS = 8
STRIP = 512
HALVES = 2
TURN = 128


def mlp_kernel(g_ref, resid_ref, wg_hbm, wu_hbm, wd_hbm, out_ref,
               g_all, wg_rows, wu_rows, wg, wu, wd, act, pown, psend, precv, rsend, rrecv_e, rrecv_m,
               w_sem, d_sem, ag_recv, ag_recv_d, ag_send_e, ag_send_m, ag_send_d,
               rd_recv, rd_send, rs_recv_e, rs_recv_m, rs_send):
    ffn = wd.shape[0]
    padded = wg.shape[1]
    rows, width = g_ref.shape
    sub = rows // NSUB
    rsub = rows // NRS
    me = lax.axis_index('tp')
    z = lax.div(me, 2)
    c = lax.rem(me, 2)
    upper = z >= 2
    is_end = jnp.logical_or(z == 0, z == 3)
    is_int = jnp.logical_not(is_end)

    def mir(k):
        return jnp.where(upper, k, 3 - k)

    partner = 2 * z + (1 - c)
    dev_e = jnp.where(is_end, me, 2 * mir(3) + c)
    dev_m = 2 * jnp.where(is_end, mir(2), mir(1)) + c

    turns = padded // TURN
    last = ffn - (turns - 1) * TURN

    def w_piece(src, dst, idx, at, count):
        return pltpu.make_async_copy(src.at[pl.ds(at * TURN, count)], dst.at[pl.ds(at * TURN, count)], w_sem.at[idx, at])

    def w_both(at, count):
        return [w_piece(wg_hbm, wg_rows, 0, at, count), w_piece(wu_hbm, wu_rows, 1, at, count)]

    down_copy = pltpu.make_async_copy(wd_hbm, wd, d_sem)

    def start_piece(at, carry):
        for copy in w_both(at, TURN):
            copy.start()
        return carry

    lax.fori_loop(0, turns - 1, start_piece, 0)
    for copy in w_both(turns - 1, last):
        copy.start()
    down_copy.start()

    barrier = pltpu.get_barrier_semaphore()
    pl.semaphore_signal(barrier, inc=1, device_id={'tp': partner}, device_id_type=MESH)
    pl.semaphore_signal(barrier, inc=1, device_id={'tp': dev_m}, device_id_type=MESH)

    @pl.when(is_int)
    def _():
        pl.semaphore_signal(barrier, inc=1, device_id={'tp': dev_e}, device_id_type=MESH)
        pl.semaphore_wait(barrier, 3)

    @pl.when(is_end)
    def _():
        pl.semaphore_wait(barrier, 2)

    def remote(src, dst, send_sem, recv_sem, dev):
        return pltpu.make_async_remote_copy(src_ref=src, dst_ref=dst, send_sem=send_sem, recv_sem=recv_sem, device_id={'tp': dev}, device_id_type=MESH)

    def ag_copy(src, chip, k, send_sem, dev):
        return remote(src, g_all.at[chip, 0, pl.ds(k * sub, sub)], send_sem.at[chip, k], ag_recv.at[chip, k], dev)

    def ag_d2d(src, chip, k):
        return remote(src, g_all.at[chip, 1, pl.ds(k * sub, sub)], ag_send_d.at[chip, k], ag_recv_d.at[chip, k], partner)

    for k in range(NSUB):
        piece = g_ref.at[pl.ds(k * sub, sub)]
        ag_copy(piece, z, k, ag_send_m, dev_m).start()

        @pl.when(is_int)
        def _():
            ag_copy(piece, z, k, ag_send_e, dev_e).start()

        ag_d2d(piece, z, k).start()
    g_all[z, 0] = g_ref[...]

    def landed(chip, k):
        return g_all.at[chip, 0, pl.ds(k * sub, sub)]

    def arrive(chip, k, send_sem, dev):
        src = landed(chip, k)
        ag_copy(src, chip, k, ag_send_d, dev_m).wait_recv()
        if dev is not None:
            ag_copy(src, chip, k, send_sem, dev).start()
        ag_d2d(src, chip, k).start()

    def both(chip):
        for k in range(NSUB):
            ag_d2d(landed(chip, k), chip, k).wait_recv()

    def rd_copy(chip, part):
        span = pl.ds(pl.multiple_of(part * (width // HALVES), width // HALVES), width // HALVES)
        return remote(psend.at[chip, :, span], precv.at[chip, :, span], rd_send.at[chip, part], rd_recv.at[chip, part], partner)

    def rd_wait(chip):
        for part in range(HALVES):
            rd_copy(chip, part).wait_recv()

    def rs_copy(chip, k, dst, recv_sem, dev):
        span = pl.ds(k * rsub, rsub)
        return remote(rsend.at[chip, span], dst.at[chip, span], rs_send.at[chip, k], recv_sem.at[chip, k], dev)

    def rs_base(chip, k):
        span = pl.ds(k * rsub, rsub)
        return pown[chip, span] + precv[chip, span].astype(jnp.float32)

    def end_send(chip):
        rd_wait(chip)
        for k in range(NRS):
            rsend[chip, pl.ds(k * rsub, rsub)] = rs_base(chip, k).astype(jnp.bfloat16)
            rs_copy(chip, k, rrecv_e, rs_recv_e, dev_m).start()

    def hook(step, strip):
        def at(role, want_step, want_strip, fn):
            if strip == want_strip:
                pl.when(jnp.logical_and(role, step == want_step))(fn)

        at(is_int, 0, 1, lambda: arrive(mir(0), 0, ag_send_e, dev_e))
        at(is_int, 1, 0, lambda: arrive(mir(0), 1, ag_send_e, dev_e))
        at(is_end, 0, 0, lambda: arrive(mir(1), 0, None, None))
        at(is_end, 1, 0, lambda: end_send(mir(2)))
        at(is_end, 1, 1, lambda: arrive(mir(0), 0, None, None))
        at(is_end, 2, 0, lambda: end_send(mir(1)))
        at(is_end, 3, 0, lambda: end_send(mir(0)))

    def swiglu(lhs, span):
        gate = jnp.dot(lhs, wg[:, span], preferred_element_type=jnp.float32)
        up = jnp.dot(lhs, wu[:, span], preferred_element_type=jnp.float32)
        return (gate / (1.0 + jnp.exp(-gate)) * up).astype(jnp.bfloat16)

    def first_arrivals(k):
        @pl.when(is_int)
        def _():
            arrive(mir(3), k, ag_send_m, dev_m)
            arrive(mir(1), k, ag_send_e, dev_e)

        @pl.when(is_end)
        def _():
            arrive(mir(2), k, None, None)

    def turn(at, carry):
        span = pl.ds(pl.multiple_of(at * TURN, TURN), TURN)
        for copy in w_both(at, TURN):
            copy.wait()
        wg[:, span] = wg_rows[span].T
        wu[:, span] = wu_rows[span].T
        pl.when(at == turns // 2)(lambda: first_arrivals(0))
        return carry

    lax.fori_loop(0, turns - 1, turn, 0)
    for copy in w_both(turns - 1, last):
        copy.wait()
    tail = slice((turns - 1) * TURN, padded)
    for src in (wg_rows, wu_rows):
        src[ffn:] = jnp.zeros((padded - ffn, width), jnp.bfloat16)
    wg[:, tail] = wg_rows[tail].T
    wu[:, tail] = wu_rows[tail].T
    first_arrivals(1)


    def one_step(step, carry):
        chip = mir(jnp.where(is_end, lax.rem(6 - step, 4), jnp.where(step == 0, 2, jnp.where(step == 1, 3, 3 - step))))

        @pl.when(jnp.logical_and(step == 1, is_end))
        def _():
            arrive(mir(1), 1, None, None)

        @pl.when(jnp.logical_and(step == 2, is_end))
        def _():
            arrive(mir(0), 1, None, None)

        both(chip)

        for strip, at in enumerate(range(0, padded, STRIP)):
            span = slice(at, min(at + STRIP, padded))
            act[:, span] = swiglu(g_all[chip].reshape(2 * rows, width), span)
            hook(step, strip)

        @pl.when(step == 0)
        def _():
            down_copy.wait()

        def one_part(part, carry):
            wide = width // HALVES
            span = pl.ds(pl.multiple_of(part * wide, wide), wide)
            down = jnp.dot(act[:, :ffn], wd[:, span], preferred_element_type=jnp.float32)
            psend[chip, :, span] = down[rows:].astype(jnp.bfloat16)
            pown[chip, :, span] = down[:rows]
            rd_copy(chip, part).start()
            return carry

        lax.fori_loop(0, HALVES, one_part, 0)
        return carry

    lax.fori_loop(0, 4, one_step, 0)

    @pl.when(is_end)
    def _():
        rd_wait(z)
        base = pown[z] + precv[z].astype(jnp.float32) + resid_ref[...].astype(jnp.float32)
        pown[z] = base
        for k in range(NRS):
            span = pl.ds(k * rsub, rsub)
            rs_copy(z, k, rrecv_m, rs_recv_m, dev_m).wait_recv()
            out_ref[span] = (pown[z, span] + rrecv_m[z, span].astype(jnp.float32)).astype(jnp.bfloat16)

    @pl.when(is_int)
    def _():
        def pass_on(chip, dst_in, sem_in, dst_out, sem_out, dev):
            rd_wait(chip)
            for k in range(NRS):
                span = pl.ds(k * rsub, rsub)
                rs_copy(chip, k, dst_in, sem_in, dev_m).wait_recv()
                rsend[chip, span] = (rs_base(chip, k) + dst_in[chip, span].astype(jnp.float32)).astype(jnp.bfloat16)
                rs_copy(chip, k, dst_out, sem_out, dev).start()

        def own_send(chip):
            pass_on(chip, rrecv_e, rs_recv_e, rrecv_m, rs_recv_m, dev_m)

        own_send(mir(1))
        rd_wait(z)
        for k in range(NRS):
            rs_copy(z, k, rrecv_e, rs_recv_e, dev_m).wait_recv()
        pown[z] = pown[z] + precv[z].astype(jnp.float32) + resid_ref[...].astype(jnp.float32) + rrecv_e[z].astype(jnp.float32)
        own_send(mir(0))
        for k in range(NRS):
            span = pl.ds(k * rsub, rsub)
            rs_copy(z, k, rrecv_m, rs_recv_m, dev_m).wait_recv()
            out_ref[span] = (pown[z, span] + rrecv_m[z, span].astype(jnp.float32)).astype(jnp.bfloat16)
        pass_on(mir(3), rrecv_m, rs_recv_m, rrecv_m, rs_recv_m, dev_e)

    for k in range(NSUB):
        for chip in range(4):
            ag_d2d(landed(chip, k), chip, k).wait_send()
        ag_copy(landed(z, k), z, k, ag_send_m, dev_m).wait_send()

        @pl.when(is_int)
        def _():
            ag_copy(landed(z, k), z, k, ag_send_e, dev_e).wait_send()
            ag_copy(landed(mir(3), k), mir(3), k, ag_send_m, dev_m).wait_send()
            ag_copy(landed(mir(1), k), mir(1), k, ag_send_e, dev_e).wait_send()
            ag_copy(landed(mir(0), k), mir(0), k, ag_send_e, dev_e).wait_send()

    for chip in range(4):
        for part in range(HALVES):
            rd_copy(chip, part).wait_send()

        @pl.when(chip != z)
        def _():
            for k in range(NRS):
                rs_copy(chip, k, rrecv_m, rs_recv_m, dev_m).wait_send()


def mlp_block(mlp_in, resid, w_gate_t, w_up_t, w_down):
    rows, width = mlp_in.shape
    ffn = w_gate_t.shape[0]
    padded = -(-ffn // TURN) * TURN
    bf16, f32 = jnp.bfloat16, jnp.float32
    vmem = pl.BlockSpec(memory_space=pltpu.VMEM)
    hbm = pl.BlockSpec(memory_space=pl.ANY)
    dma = pltpu.SemaphoreType.DMA
    flops = 3 * 2 * 8 * rows * width * ffn
    return pl.pallas_call(
        mlp_kernel,
        out_shape=jax.ShapeDtypeStruct((rows, width), bf16),
        in_specs=[vmem, vmem, hbm, hbm, hbm],
        out_specs=vmem,
        scratch_shapes=[
            pltpu.VMEM((4, 2, rows, width), bf16),
            pltpu.VMEM((padded, width), bf16),
            pltpu.VMEM((padded, width), bf16),
            pltpu.VMEM((width, padded), bf16),
            pltpu.VMEM((width, padded), bf16),
            pltpu.VMEM((ffn, width), bf16),
            pltpu.VMEM((2 * rows, padded), bf16),
            pltpu.VMEM((4, rows, width), f32),
            pltpu.VMEM((4, rows, width), bf16),
            pltpu.VMEM((4, rows, width), bf16),
            pltpu.VMEM((4, rows, width), bf16),
            pltpu.VMEM((4, rows, width), bf16),
            pltpu.VMEM((4, rows, width), bf16),
            dma((2, padded // TURN)),
            dma,
            dma((4, NSUB)), dma((4, NSUB)), dma((4, NSUB)), dma((4, NSUB)), dma((4, NSUB)),
            dma((4, HALVES)), dma((4, HALVES)),
            dma((4, NRS)), dma((4, NRS)), dma((4, NRS)),
        ],
        compiler_params=pltpu.CompilerParams(collective_id=0, has_side_effects=True, vmem_limit_bytes=60 * 1024 * 1024),
        cost_estimate=pl.CostEstimate(flops=flops, bytes_accessed=3 * 2 * ffn * width, transcendentals=8 * rows * ffn),
        name='mlp_exchange',
    )(mlp_in, resid, w_gate_t, w_up_t, w_down)


def solution(mesh):
    rows_spec = P(('dp', 'tp'), None)
    cache_spec = P(('dp', 'tp'), None, None)
    whole = P()
    in_specs = (rows_spec, cache_spec, cache_spec, P(('dp', 'tp')), whole, whole, whole, whole, whole, whole, whole, whole, P(None, 'tp'), P(None, 'tp'), P('tp', None))
    out_specs = (rows_spec, rows_spec, rows_spec)

    def device_step(hidden, cache_lat, cache_rope, seq_lens, attn_norm, w_query, w_kv_down, kv_norm, w_key_up, w_val_up, w_out, mlp_norm, w_gate, w_up, w_down):
        resid, mlp_in, lat_new, rope_new = attention_block(hidden, cache_lat, cache_rope, seq_lens, attn_norm, w_query, w_kv_down, kv_norm, w_key_up, w_val_up, w_out, mlp_norm)
        out_hidden = mlp_block(mlp_in, resid, w_gate.T, w_up.T, w_down)
        return out_hidden, lat_new, rope_new

    return jax.shard_map(device_step, mesh=mesh, in_specs=in_specs, out_specs=out_specs, check_vma=False)
```

```python
import math

import jax
import jax.numpy as jnp
from jax import lax
from jax.experimental import pallas as pl
from jax.experimental.pallas import tpu as pltpu
from jax.sharding import PartitionSpec as P

EPS = 1e-6
ROPE_BASE = 10000.0
ROPE_DIM = 64
NOPE_DIM = 128
VAL_DIM = 128
SCALE = (NOPE_DIM + ROPE_DIM) ** -0.5


GROUP = 8
SLOTS = 4
LAG = 2
PITCH = 72
BLOCK = 128
Q_CHUNKS = 4
VMEM_LIMIT = 63 * 1024 * 1024


def attn_kernel(lens_ref, hidden_ref, lens_vec, attn_gain, kv_gain, mlp_gain, lat_hbm, rope_hbm, wq_hbm, wkv_hbm, wk_hbm, wv_hbm, wo_hbm,
                resid_ref, mlp_in_ref, lat_new_ref, rope_new_ref,
                keys, rope, wq, wkv, wk, wv, wo, normed, qs, ol, qr, lat_row, rope_row, heads_out, order, key_sem, w_sem):
    f32, bf16 = jnp.float32, jnp.bfloat16
    rows, width = hidden_ref.shape
    rank = wk.shape[0]
    heads = wk.shape[1] // NOPE_DIM
    groups = rows // GROUP
    classes = keys.shape[2] // BLOCK

    chunk = wq.shape[2]
    w_copies = [pltpu.make_async_copy(wkv_hbm, wkv, w_sem.at[0]), pltpu.make_async_copy(wk_hbm, wk, w_sem.at[1])]
    w_copies += [pltpu.make_async_copy(wq_hbm.at[:, pl.ds(j * chunk, chunk)], wq.at[j], w_sem.at[2 + j]) for j in range(Q_CHUNKS)]
    rope_copy = pltpu.make_async_copy(rope_hbm, rope, w_sem.at[2 + Q_CHUNKS])
    late_copies = [pltpu.make_async_copy(wv_hbm, wv, w_sem.at[3 + Q_CHUNKS])]
    late_copies += [pltpu.make_async_copy(wo_hbm.at[:, pl.ds(n * 512, 512)], wo.at[n], w_sem.at[4 + Q_CHUNKS + n]) for n in range(width // 512)]
    for copy in w_copies:
        copy.start()
    rope_copy.start()

    def kind(b):
        return lax.div(lens_ref[b], BLOCK)

    def count(b, counts):
        k = kind(b)
        return tuple(n + jnp.where(k == i, 1, 0) for i, n in enumerate(counts))

    zero = jnp.int32(0)
    counts = lax.fori_loop(0, rows, count, (zero,) * classes)
    firsts = []
    total = zero
    for i in reversed(range(classes)):
        firsts.append(total)
        total = total + counts[i]
    firsts = tuple(reversed(firsts))

    def place(b, firsts):
        k = kind(b)
        at = firsts[0]
        for i in range(1, classes):
            at = jnp.where(k == i, firsts[i], at)
        order[at] = b
        return tuple(n + jnp.where(k == i, 1, 0) for i, n in enumerate(firsts))

    lax.fori_loop(0, rows, place, firsts)

    def group_copies(g, blocks):
        slot = lax.rem(g, SLOTS)
        return [pltpu.make_async_copy(lat_hbm.at[order[g * GROUP + i], pl.ds(0, blocks * BLOCK)], keys.at[slot, i, pl.ds(0, blocks * BLOCK)], key_sem.at[slot, i]) for i in range(GROUP)]

    def per_class(g, fn):
        k = kind(order[g * GROUP])
        for i in range(classes):
            @pl.when(k == i)
            def _():
                fn(i + 1)

    def start_group(g):
        def start(blocks):
            for copy in group_copies(g, blocks):
                copy.start()

        per_class(g, start)

    def start_first(g, carry):
        start_group(g)
        return carry

    lax.fori_loop(0, SLOTS, start_first, 0)

    vals = hidden_ref[...].astype(f32)
    inv_rms = lax.rsqrt(jnp.mean(vals * vals, axis=-1, keepdims=True) + EPS)
    normed[...] = (vals * inv_rms * attn_gain[...].astype(f32)[None]).astype(bf16)

    lane = lax.broadcasted_iota(jnp.int32, (rows, 2 * ROPE_DIM), 1)
    half = ROPE_DIM // 2
    freq = jnp.exp(lax.rem(lane, half).astype(f32) * (-math.log(ROPE_BASE) / half))
    square_ids = (rows, rows)
    diagonal = lax.broadcasted_iota(jnp.int32, square_ids, 0) == lax.broadcasted_iota(jnp.int32, square_ids, 1)
    lens = jnp.sum(jnp.where(diagonal, lens_vec[...].astype(f32)[None], 0.0), axis=1, keepdims=True)
    angles = lens * freq
    cos_tab = jnp.cos(angles)
    is_first = lax.rem(lane, ROPE_DIM) < half
    sin_tab = jnp.where(is_first, -jnp.sin(angles), jnp.sin(angles))

    def rotate_pair(pair):
        swapped = jnp.where(is_first, pltpu.roll(pair, 2 * ROPE_DIM - half, 1), pltpu.roll(pair, half, 1))
        return (pair * cos_tab + swapped * sin_tab).astype(bf16).astype(f32)

    w_copies[0].wait()
    kv = lax.dot_general(normed[...], wkv[...], (((1,), (1,)), ((), ())), preferred_element_type=f32).astype(bf16).astype(f32)
    lat = kv[:, :rank]
    inv_lat = lax.rsqrt(jnp.mean(lat * lat, axis=-1, keepdims=True) + EPS)
    lat_new = (lat * inv_lat * kv_gain[...].astype(f32)[None]).astype(bf16)
    lat_new_ref[...] = lat_new
    lat_row[...] = lat_new.astype(f32)
    pe = kv[:, rank:]
    rope_new = rotate_pair(jnp.concatenate([pe, pe], axis=1))
    rope_new_ref[...] = rope_new[:, :ROPE_DIM].astype(bf16)
    rope_row[...] = rope_new

    w_copies[1].wait()
    low = lane < ROPE_DIM

    def put_head(head, nope, pe_rot):
        key_up = wk[:, head * NOPE_DIM:(head + 1) * NOPE_DIM]
        q_lat = lax.dot_general(nope.astype(bf16), key_up, (((1,), (1,)), ((), ())), preferred_element_type=f32).astype(bf16).astype(f32)
        for part in range(rank // 128):
            qs[part, pl.ds(head, rows, stride=heads), :] = q_lat[:, part * 128:(part + 1) * 128]
        qr[pl.ds(head, rows, stride=heads), :] = pe_rot

    for j in range(Q_CHUNKS):
        w_copies[2 + j].wait()
        query = jnp.dot(normed[...], wq[j], preferred_element_type=f32).astype(bf16).astype(f32)
        for pair in range(chunk // 384):
            base = pair * 384
            part_a, part_b, part_c = (query[:, base + 128 * i:base + 128 * (i + 1)] for i in range(3))
            pe_rot = rotate_pair(jnp.where(low, part_b, part_c))
            head = (j * chunk + base) // 192
            put_head(head, part_a, pe_rot)
            put_head(head + 1, jnp.where(low, pltpu.roll(part_b, ROPE_DIM, 1), pltpu.roll(part_c, ROPE_DIM, 1)), pltpu.roll(pe_rot, ROPE_DIM, 1))

    rope_copy.wait()

    def attend(g, blocks):
        slot = lax.rem(g, SLOTS)
        span = blocks * BLOCK
        for copy in group_copies(g, blocks):
            copy.wait()
        picks = [order[g * GROUP + i] for i in range(GROUP)]
        for i, b in enumerate(picks):
            length = lens_ref[b]
            base = pl.multiple_of(lax.div(length, 16) * 16, 16)
            tile = keys[slot, i, pl.ds(base, 16), :].astype(f32)
            sub = lax.broadcasted_iota(jnp.int32, (16, rank), 0)
            keys[slot, i, pl.ds(base, 16), :] = jnp.where(sub == length - base, lat_row[pl.ds(b, 1), :], tile).astype(bf16)

        def score_of(i):
            b = picks[i]
            length = lens_ref[b]
            mine = pl.ds(pl.multiple_of(b * heads, heads), heads)
            q_lat = jnp.concatenate([qs[part, mine, :] for part in range(rank // 128)], axis=1).astype(bf16)
            q_rot = qr[mine, :]
            score = lax.dot_general(q_lat, keys[slot, i, :span], (((1,), (1,)), ((), ())), preferred_element_type=f32)
            near = jnp.dot(q_rot[:, :ROPE_DIM].astype(bf16), rope[b, :, :span], preferred_element_type=f32)
            first = lax.broadcasted_iota(jnp.int32, (heads, 2 * ROPE_DIM), 1) < ROPE_DIM
            new = jnp.sum(jnp.where(first, q_rot * rope_row[pl.ds(b, 1), :], 0.0), axis=1, keepdims=True)
            at = lax.broadcasted_iota(jnp.int32, (heads, span), 1)
            score = (score + jnp.where(at == length, new, near)) * SCALE
            return jnp.where(at <= length, score, -jnp.inf)

        def finish(i, score):
            expo = jnp.exp(score - jnp.max(score, axis=1, keepdims=True))
            prob = (expo / jnp.sum(expo, axis=1, keepdims=True)).astype(bf16)
            out = jnp.dot(prob, keys[slot, i, :span], preferred_element_type=f32)
            for part in range(rank // 128):
                ol[part, pl.ds(picks[i], heads, stride=PITCH), :] = out[:, part * 128:(part + 1) * 128]

        scores = {}
        for i in range(GROUP + LAG):
            if i < GROUP:
                scores[i] = score_of(i)
            if i >= LAG:
                finish(i - LAG, scores.pop(i - LAG))

    def one_group(g, carry):
        per_class(g, lambda blocks: attend(g, blocks))

        @pl.when(g + SLOTS < groups)
        def _():
            start_group(g + SLOTS)

        @pl.when(g == groups - SLOTS - 1)
        def _():
            for copy in late_copies:
                copy.start()

        return carry

    lax.fori_loop(0, groups, one_group, 0)

    late_copies[0].wait()
    for head in range(heads):
        cols = slice(head * VAL_DIM, (head + 1) * VAL_DIM)
        lat_out = jnp.concatenate([ol[part, head * PITCH:head * PITCH + rows, :] for part in range(rank // 128)], axis=1).astype(bf16)
        heads_out[:, cols] = jnp.dot(lat_out, wv[:, cols], preferred_element_type=f32).astype(bf16)
    square = jnp.zeros((rows, 1), f32)
    for n in range(width // 512):
        cols = slice(n * 512, (n + 1) * 512)
        late_copies[1 + n].wait()
        attn_out = jnp.dot(heads_out[...], wo[n], preferred_element_type=f32)
        resid = (hidden_ref[:, cols].astype(f32) + attn_out).astype(bf16)
        resid_ref[:, cols] = resid
        square = square + jnp.sum(resid.astype(f32) * resid.astype(f32), axis=-1, keepdims=True)
    inv_rms = lax.rsqrt(square * (1.0 / width) + EPS)
    mlp_in_ref[...] = (resid_ref[...].astype(f32) * inv_rms * mlp_gain[...].astype(f32)[None]).astype(bf16)


def attention_block(hidden, cache_lat, cache_rope, seq_lens, attn_norm, w_query, w_kv_down, kv_norm, w_key_up, w_val_up, w_out, mlp_norm):
    rows, width = hidden.shape
    slots, rank = cache_lat.shape[1:]
    bf16, f32 = jnp.bfloat16, jnp.float32
    heads = w_key_up.shape[1] // NOPE_DIM
    q_width = w_query.shape[1]
    vmem = pl.BlockSpec(memory_space=pltpu.VMEM)
    hbm = pl.BlockSpec(memory_space=pl.ANY)
    smem = pl.BlockSpec(memory_space=pltpu.SMEM)
    dma = pltpu.SemaphoreType.DMA
    flops = 2 * rows * (width * (q_width + rank + ROPE_DIM + width) + heads * rank * (NOPE_DIM + VAL_DIM) + heads * slots * (2 * rank + ROPE_DIM))
    moved = 2 * (width * (q_width + rank + ROPE_DIM + width) + heads * rank * (NOPE_DIM + VAL_DIM) + rows * slots * (rank + ROPE_DIM))
    return pl.pallas_call(
        attn_kernel,
        out_shape=(
            jax.ShapeDtypeStruct((rows, width), bf16),
            jax.ShapeDtypeStruct((rows, width), bf16),
            jax.ShapeDtypeStruct((rows, rank), bf16),
            jax.ShapeDtypeStruct((rows, ROPE_DIM), bf16),
        ),
        in_specs=[smem] + [vmem] * 5 + [hbm] * 7,
        out_specs=(vmem,) * 4,
        scratch_shapes=[
            pltpu.VMEM((SLOTS, GROUP, slots, rank), bf16),
            pltpu.VMEM((rows, ROPE_DIM, slots), bf16),
            pltpu.VMEM((Q_CHUNKS, width, q_width // Q_CHUNKS), bf16),
            pltpu.VMEM((rank + ROPE_DIM, width), bf16),
            pltpu.VMEM((rank, heads * NOPE_DIM), bf16),
            pltpu.VMEM((rank, heads * VAL_DIM), bf16),
            pltpu.VMEM((width // 512, heads * VAL_DIM, 512), bf16),
            pltpu.VMEM((rows, width), bf16),
            pltpu.VMEM((rank // 128, rows * heads, 128), f32),
            pltpu.VMEM((rank // 128, PITCH * heads, 128), f32),
            pltpu.VMEM((rows * heads, 2 * ROPE_DIM), f32),
            pltpu.VMEM((rows, rank), f32),
            pltpu.VMEM((rows, 2 * ROPE_DIM), f32),
            pltpu.VMEM((rows, heads * VAL_DIM), bf16),
            pltpu.SMEM((rows,), jnp.int32),
            dma((SLOTS, GROUP)),
            dma((4 + Q_CHUNKS + width // 512,)),
        ],
        compiler_params=pltpu.CompilerParams(vmem_limit_bytes=VMEM_LIMIT),
        cost_estimate=pl.CostEstimate(flops=flops, bytes_accessed=moved, transcendentals=rows * heads * slots),
        name='latent_attention',
    )(seq_lens, hidden, seq_lens, attn_norm, kv_norm, mlp_norm, cache_lat, jnp.swapaxes(cache_rope, 1, 2), w_query, w_kv_down.T, w_key_up, w_val_up, w_out)


MESH = pl.DeviceIdType.MESH
NSUB = 2
NRS = 8
STRIP = 512
HALVES = 2
TURN = 128


def mlp_kernel(g_ref, resid_ref, wg_hbm, wu_hbm, wd_hbm, out_ref,
               g_all, wg_rows, wu_rows, wg, wu, wd, act, pown, psend, precv, rsend, rrecv_e, rrecv_m,
               w_sem, d_sem, ag_recv, ag_recv_d, ag_send_e, ag_send_m, ag_send_d,
               rd_recv, rd_send, rs_recv_e, rs_recv_m, rs_send):
    ffn = wd.shape[0]
    padded = wg.shape[1]
    rows, width = g_ref.shape
    sub = rows // NSUB
    rsub = rows // NRS
    me = lax.axis_index('tp')
    z = lax.div(me, 2)
    c = lax.rem(me, 2)
    upper = z >= 2
    is_end = jnp.logical_or(z == 0, z == 3)
    is_int = jnp.logical_not(is_end)

    def mir(k):
        return jnp.where(upper, k, 3 - k)

    partner = 2 * z + (1 - c)
    dev_e = jnp.where(is_end, me, 2 * mir(3) + c)
    dev_m = 2 * jnp.where(is_end, mir(2), mir(1)) + c

    turns = padded // TURN
    last = ffn - (turns - 1) * TURN

    def w_piece(src, dst, idx, at, count):
        return pltpu.make_async_copy(src.at[pl.ds(at * TURN, count)], dst.at[pl.ds(at * TURN, count)], w_sem.at[idx, at])

    def w_both(at, count):
        return [w_piece(wg_hbm, wg_rows, 0, at, count), w_piece(wu_hbm, wu_rows, 1, at, count)]

    down_copy = pltpu.make_async_copy(wd_hbm, wd, d_sem)

    def start_piece(at, carry):
        for copy in w_both(at, TURN):
            copy.start()
        return carry

    lax.fori_loop(0, turns - 1, start_piece, 0)
    for copy in w_both(turns - 1, last):
        copy.start()
    down_copy.start()

    barrier = pltpu.get_barrier_semaphore()
    pl.semaphore_signal(barrier, inc=1, device_id={'tp': partner}, device_id_type=MESH)
    pl.semaphore_signal(barrier, inc=1, device_id={'tp': dev_m}, device_id_type=MESH)

    @pl.when(is_int)
    def _():
        pl.semaphore_signal(barrier, inc=1, device_id={'tp': dev_e}, device_id_type=MESH)
        pl.semaphore_wait(barrier, 3)

    @pl.when(is_end)
    def _():
        pl.semaphore_wait(barrier, 2)

    def remote(src, dst, send_sem, recv_sem, dev):
        return pltpu.make_async_remote_copy(src_ref=src, dst_ref=dst, send_sem=send_sem, recv_sem=recv_sem, device_id={'tp': dev}, device_id_type=MESH)

    def ag_copy(src, chip, k, send_sem, dev):
        return remote(src, g_all.at[chip, 0, pl.ds(k * sub, sub)], send_sem.at[chip, k], ag_recv.at[chip, k], dev)

    def ag_d2d(src, chip, k):
        return remote(src, g_all.at[chip, 1, pl.ds(k * sub, sub)], ag_send_d.at[chip, k], ag_recv_d.at[chip, k], partner)

    for k in range(NSUB):
        piece = g_ref.at[pl.ds(k * sub, sub)]
        ag_copy(piece, z, k, ag_send_m, dev_m).start()

        @pl.when(is_int)
        def _():
            ag_copy(piece, z, k, ag_send_e, dev_e).start()

        ag_d2d(piece, z, k).start()
    g_all[z, 0] = g_ref[...]

    def landed(chip, k):
        return g_all.at[chip, 0, pl.ds(k * sub, sub)]

    def arrive(chip, k, send_sem, dev):
        src = landed(chip, k)
        ag_copy(src, chip, k, ag_send_d, dev_m).wait_recv()
        if dev is not None:
            ag_copy(src, chip, k, send_sem, dev).start()
        ag_d2d(src, chip, k).start()

    def both(chip):
        for k in range(NSUB):
            ag_d2d(landed(chip, k), chip, k).wait_recv()

    def rd_copy(chip, part):
        span = pl.ds(pl.multiple_of(part * (width // HALVES), width // HALVES), width // HALVES)
        return remote(psend.at[chip, :, span], precv.at[chip, :, span], rd_send.at[chip, part], rd_recv.at[chip, part], partner)

    def rd_wait(chip):
        for part in range(HALVES):
            rd_copy(chip, part).wait_recv()

    def rs_copy(chip, k, dst, recv_sem, dev):
        span = pl.ds(k * rsub, rsub)
        return remote(rsend.at[chip, span], dst.at[chip, span], rs_send.at[chip, k], recv_sem.at[chip, k], dev)

    def rs_base(chip, k):
        span = pl.ds(k * rsub, rsub)
        return pown[chip, span] + precv[chip, span].astype(jnp.float32)

    def end_send(chip):
        rd_wait(chip)
        for k in range(NRS):
            rsend[chip, pl.ds(k * rsub, rsub)] = rs_base(chip, k).astype(jnp.bfloat16)
            rs_copy(chip, k, rrecv_e, rs_recv_e, dev_m).start()

    def hook(step, strip):
        def at(role, want_step, want_strip, fn):
            if strip == want_strip:
                pl.when(jnp.logical_and(role, step == want_step))(fn)

        at(is_int, 0, 1, lambda: arrive(mir(0), 0, ag_send_e, dev_e))
        at(is_int, 1, 0, lambda: arrive(mir(0), 1, ag_send_e, dev_e))
        at(is_end, 0, 0, lambda: arrive(mir(1), 0, None, None))
        at(is_end, 1, 0, lambda: end_send(mir(2)))
        at(is_end, 1, 1, lambda: arrive(mir(0), 0, None, None))
        at(is_end, 2, 0, lambda: end_send(mir(1)))
        at(is_end, 3, 0, lambda: end_send(mir(0)))

    def swiglu(lhs, span):
        gate = jnp.dot(lhs, wg[:, span], preferred_element_type=jnp.float32)
        up = jnp.dot(lhs, wu[:, span], preferred_element_type=jnp.float32)
        return (gate / (1.0 + jnp.exp(-gate)) * up).astype(jnp.bfloat16)

    def first_arrivals(k):
        @pl.when(is_int)
        def _():
            arrive(mir(3), k, ag_send_m, dev_m)
            arrive(mir(1), k, ag_send_e, dev_e)

        @pl.when(is_end)
        def _():
            arrive(mir(2), k, None, None)

    def turn(at, carry):
        span = pl.ds(pl.multiple_of(at * TURN, TURN), TURN)
        for copy in w_both(at, TURN):
            copy.wait()
        wg[:, span] = wg_rows[span].T
        wu[:, span] = wu_rows[span].T
        pl.when(at == turns // 2)(lambda: first_arrivals(0))
        return carry

    lax.fori_loop(0, turns - 1, turn, 0)
    for copy in w_both(turns - 1, last):
        copy.wait()
    tail = slice((turns - 1) * TURN, padded)
    for src in (wg_rows, wu_rows):
        src[ffn:] = jnp.zeros((padded - ffn, width), jnp.bfloat16)
    wg[:, tail] = wg_rows[tail].T
    wu[:, tail] = wu_rows[tail].T
    first_arrivals(1)


    def one_step(step, carry):
        chip = mir(jnp.where(is_end, lax.rem(6 - step, 4), jnp.where(step == 0, 2, jnp.where(step == 1, 3, 3 - step))))

        @pl.when(jnp.logical_and(step == 1, is_end))
        def _():
            arrive(mir(1), 1, None, None)

        @pl.when(jnp.logical_and(step == 2, is_end))
        def _():
            arrive(mir(0), 1, None, None)

        both(chip)

        for strip, at in enumerate(range(0, padded, STRIP)):
            span = slice(at, min(at + STRIP, padded))
            act[:, span] = swiglu(g_all[chip].reshape(2 * rows, width), span)
            hook(step, strip)

        @pl.when(step == 0)
        def _():
            down_copy.wait()

        def one_part(part, carry):
            wide = width // HALVES
            span = pl.ds(pl.multiple_of(part * wide, wide), wide)
            down = jnp.dot(act[:, :ffn], wd[:, span], preferred_element_type=jnp.float32)
            psend[chip, :, span] = down[rows:].astype(jnp.bfloat16)
            pown[chip, :, span] = down[:rows]
            rd_copy(chip, part).start()
            return carry

        lax.fori_loop(0, HALVES, one_part, 0)
        return carry

    lax.fori_loop(0, 4, one_step, 0)

    @pl.when(is_end)
    def _():
        rd_wait(z)
        base = pown[z] + precv[z].astype(jnp.float32) + resid_ref[...].astype(jnp.float32)
        pown[z] = base
        for k in range(NRS):
            span = pl.ds(k * rsub, rsub)
            rs_copy(z, k, rrecv_m, rs_recv_m, dev_m).wait_recv()
            out_ref[span] = (pown[z, span] + rrecv_m[z, span].astype(jnp.float32)).astype(jnp.bfloat16)

    @pl.when(is_int)
    def _():
        def pass_on(chip, dst_in, sem_in, dst_out, sem_out, dev):
            rd_wait(chip)
            for k in range(NRS):
                span = pl.ds(k * rsub, rsub)
                rs_copy(chip, k, dst_in, sem_in, dev_m).wait_recv()
                rsend[chip, span] = (rs_base(chip, k) + dst_in[chip, span].astype(jnp.float32)).astype(jnp.bfloat16)
                rs_copy(chip, k, dst_out, sem_out, dev).start()

        def own_send(chip):
            pass_on(chip, rrecv_e, rs_recv_e, rrecv_m, rs_recv_m, dev_m)

        own_send(mir(1))
        rd_wait(z)
        for k in range(NRS):
            rs_copy(z, k, rrecv_e, rs_recv_e, dev_m).wait_recv()
        pown[z] = pown[z] + precv[z].astype(jnp.float32) + resid_ref[...].astype(jnp.float32) + rrecv_e[z].astype(jnp.float32)
        own_send(mir(0))
        for k in range(NRS):
            span = pl.ds(k * rsub, rsub)
            rs_copy(z, k, rrecv_m, rs_recv_m, dev_m).wait_recv()
            out_ref[span] = (pown[z, span] + rrecv_m[z, span].astype(jnp.float32)).astype(jnp.bfloat16)
        pass_on(mir(3), rrecv_m, rs_recv_m, rrecv_m, rs_recv_m, dev_e)

    for k in range(NSUB):
        for chip in range(4):
            ag_d2d(landed(chip, k), chip, k).wait_send()
        ag_copy(landed(z, k), z, k, ag_send_m, dev_m).wait_send()

        @pl.when(is_int)
        def _():
            ag_copy(landed(z, k), z, k, ag_send_e, dev_e).wait_send()
            ag_copy(landed(mir(3), k), mir(3), k, ag_send_m, dev_m).wait_send()
            ag_copy(landed(mir(1), k), mir(1), k, ag_send_e, dev_e).wait_send()
            ag_copy(landed(mir(0), k), mir(0), k, ag_send_e, dev_e).wait_send()

    for chip in range(4):
        for part in range(HALVES):
            rd_copy(chip, part).wait_send()

        @pl.when(chip != z)
        def _():
            for k in range(NRS):
                rs_copy(chip, k, rrecv_m, rs_recv_m, dev_m).wait_send()


def mlp_block(mlp_in, resid, w_gate_t, w_up_t, w_down):
    rows, width = mlp_in.shape
    ffn = w_gate_t.shape[0]
    padded = -(-ffn // TURN) * TURN
    bf16, f32 = jnp.bfloat16, jnp.float32
    vmem = pl.BlockSpec(memory_space=pltpu.VMEM)
    hbm = pl.BlockSpec(memory_space=pl.ANY)
    dma = pltpu.SemaphoreType.DMA
    flops = 3 * 2 * 8 * rows * width * ffn
    return pl.pallas_call(
        mlp_kernel,
        out_shape=jax.ShapeDtypeStruct((rows, width), bf16),
        in_specs=[vmem, vmem, hbm, hbm, hbm],
        out_specs=vmem,
        scratch_shapes=[
            pltpu.VMEM((4, 2, rows, width), bf16),
            pltpu.VMEM((padded, width), bf16),
            pltpu.VMEM((padded, width), bf16),
            pltpu.VMEM((width, padded), bf16),
            pltpu.VMEM((width, padded), bf16),
            pltpu.VMEM((ffn, width), bf16),
            pltpu.VMEM((2 * rows, padded), bf16),
            pltpu.VMEM((4, rows, width), f32),
            pltpu.VMEM((4, rows, width), bf16),
            pltpu.VMEM((4, rows, width), bf16),
            pltpu.VMEM((4, rows, width), bf16),
            pltpu.VMEM((4, rows, width), bf16),
            pltpu.VMEM((4, rows, width), bf16),
            dma((2, padded // TURN)),
            dma,
            dma((4, NSUB)), dma((4, NSUB)), dma((4, NSUB)), dma((4, NSUB)), dma((4, NSUB)),
            dma((4, HALVES)), dma((4, HALVES)),
            dma((4, NRS)), dma((4, NRS)), dma((4, NRS)),
        ],
        compiler_params=pltpu.CompilerParams(collective_id=0, has_side_effects=True, vmem_limit_bytes=60 * 1024 * 1024),
        cost_estimate=pl.CostEstimate(flops=flops, bytes_accessed=3 * 2 * ffn * width, transcendentals=8 * rows * ffn),
        name='mlp_exchange',
    )(mlp_in, resid, w_gate_t, w_up_t, w_down)


def solution(mesh):
    rows_spec = P(('dp', 'tp'), None)
    cache_spec = P(('dp', 'tp'), None, None)
    whole = P()
    in_specs = (rows_spec, cache_spec, cache_spec, P(('dp', 'tp')), whole, whole, whole, whole, whole, whole, whole, whole, P(None, 'tp'), P(None, 'tp'), P('tp', None))
    out_specs = (rows_spec, rows_spec, rows_spec)

    def device_step(hidden, cache_lat, cache_rope, seq_lens, attn_norm, w_query, w_kv_down, kv_norm, w_key_up, w_val_up, w_out, mlp_norm, w_gate, w_up, w_down):
        resid, mlp_in, lat_new, rope_new = attention_block(hidden, cache_lat, cache_rope, seq_lens, attn_norm, w_query, w_kv_down, kv_norm, w_key_up, w_val_up, w_out, mlp_norm)
        out_hidden = mlp_block(mlp_in, resid, w_gate.T, w_up.T, w_down)
        return out_hidden, lat_new, rope_new

    return jax.shard_map(device_step, mesh=mesh, in_specs=in_specs, out_specs=out_specs, check_vma=False)
```

```python
import math

import jax
import jax.numpy as jnp
from jax import lax
from jax.experimental import pallas as pl
from jax.experimental.pallas import tpu as pltpu
from jax.sharding import PartitionSpec as P

EPS = 1e-6
ROPE_BASE = 10000.0
ROPE_DIM = 64
NOPE_DIM = 128
VAL_DIM = 128
SCALE = (NOPE_DIM + ROPE_DIM) ** -0.5


GROUP = 8
SLOTS = 4
LAG = 2
PITCH = 72
BLOCK = 128
Q_CHUNKS = 4
VMEM_LIMIT = 63 * 1024 * 1024


def attn_kernel(lens_ref, hidden_ref, lens_vec, attn_gain, kv_gain, mlp_gain, lat_hbm, rope_hbm, wq_hbm, wkv_hbm, wk_hbm, wv_hbm, wo_hbm,
                resid_ref, mlp_in_ref, lat_new_ref, rope_new_ref,
                keys, rope, wq, wkv, wk, wv, wo, normed, qs, ol, qr, lat_row, rope_row, heads_out, order, key_sem, w_sem):
    f32, bf16 = jnp.float32, jnp.bfloat16
    rows, width = hidden_ref.shape
    rank = wk.shape[0]
    heads = wk.shape[1] // NOPE_DIM
    groups = rows // GROUP
    classes = keys.shape[2] // BLOCK

    chunk = wq.shape[2]
    w_copies = [pltpu.make_async_copy(wkv_hbm, wkv, w_sem.at[0]), pltpu.make_async_copy(wk_hbm, wk, w_sem.at[1])]
    w_copies += [pltpu.make_async_copy(wq_hbm.at[:, pl.ds(j * chunk, chunk)], wq.at[j], w_sem.at[2 + j]) for j in range(Q_CHUNKS)]
    rope_copy = pltpu.make_async_copy(rope_hbm, rope, w_sem.at[2 + Q_CHUNKS])
    late_copies = [pltpu.make_async_copy(wv_hbm, wv, w_sem.at[3 + Q_CHUNKS])]
    late_copies += [pltpu.make_async_copy(wo_hbm.at[:, pl.ds(n * 512, 512)], wo.at[n], w_sem.at[4 + Q_CHUNKS + n]) for n in range(width // 512)]
    for copy in w_copies:
        copy.start()
    rope_copy.start()

    def kind(b):
        return lax.div(lens_ref[b], BLOCK)

    def count(b, counts):
        k = kind(b)
        return tuple(n + jnp.where(k == i, 1, 0) for i, n in enumerate(counts))

    zero = jnp.int32(0)
    counts = lax.fori_loop(0, rows, count, (zero,) * classes)
    firsts = []
    total = zero
    for i in reversed(range(classes)):
        firsts.append(total)
        total = total + counts[i]
    firsts = tuple(reversed(firsts))

    def place(b, firsts):
        k = kind(b)
        at = firsts[0]
        for i in range(1, classes):
            at = jnp.where(k == i, firsts[i], at)
        order[at] = b
        return tuple(n + jnp.where(k == i, 1, 0) for i, n in enumerate(firsts))

    lax.fori_loop(0, rows, place, firsts)

    def group_copies(g, blocks):
        slot = lax.rem(g, SLOTS)
        return [pltpu.make_async_copy(lat_hbm.at[order[g * GROUP + i], pl.ds(0, blocks * BLOCK)], keys.at[slot, i, pl.ds(0, blocks * BLOCK)], key_sem.at[slot, i]) for i in range(GROUP)]

    def per_class(g, fn):
        k = kind(order[g * GROUP])
        for i in range(classes):
            @pl.when(k == i)
            def _():
                fn(i + 1)

    def start_group(g):
        def start(blocks):
            for copy in group_copies(g, blocks):
                copy.start()

        per_class(g, start)

    def start_first(g, carry):
        start_group(g)
        return carry

    lax.fori_loop(0, SLOTS, start_first, 0)

    vals = hidden_ref[...].astype(f32)
    inv_rms = lax.rsqrt(jnp.mean(vals * vals, axis=-1, keepdims=True) + EPS)
    normed[...] = (vals * inv_rms * attn_gain[...].astype(f32)[None]).astype(bf16)

    lane = lax.broadcasted_iota(jnp.int32, (rows, 2 * ROPE_DIM), 1)
    half = ROPE_DIM // 2
    freq = jnp.exp(lax.rem(lane, half).astype(f32) * (-math.log(ROPE_BASE) / half))
    square_ids = (rows, rows)
    diagonal = lax.broadcasted_iota(jnp.int32, square_ids, 0) == lax.broadcasted_iota(jnp.int32, square_ids, 1)
    lens = jnp.sum(jnp.where(diagonal, lens_vec[...].astype(f32)[None], 0.0), axis=1, keepdims=True)
    angles = lens * freq
    cos_tab = jnp.cos(angles)
    is_first = lax.rem(lane, ROPE_DIM) < half
    sin_tab = jnp.where(is_first, -jnp.sin(angles), jnp.sin(angles))

    def rotate_pair(pair):
        swapped = jnp.where(is_first, pltpu.roll(pair, 2 * ROPE_DIM - half, 1), pltpu.roll(pair, half, 1))
        return (pair * cos_tab + swapped * sin_tab).astype(bf16).astype(f32)

    w_copies[0].wait()
    kv = lax.dot_general(normed[...], wkv[...], (((1,), (1,)), ((), ())), preferred_element_type=f32).astype(bf16).astype(f32)
    lat = kv[:, :rank]
    inv_lat = lax.rsqrt(jnp.mean(lat * lat, axis=-1, keepdims=True) + EPS)
    lat_new = (lat * inv_lat * kv_gain[...].astype(f32)[None]).astype(bf16)
    lat_new_ref[...] = lat_new
    lat_row[...] = lat_new.astype(f32)
    pe = kv[:, rank:]
    rope_new = rotate_pair(jnp.concatenate([pe, pe], axis=1))
    rope_new_ref[...] = rope_new[:, :ROPE_DIM].astype(bf16)
    rope_row[...] = rope_new

    w_copies[1].wait()
    low = lane < ROPE_DIM

    def put_head(head, nope, pe_rot):
        key_up = wk[:, head * NOPE_DIM:(head + 1) * NOPE_DIM]
        q_lat = lax.dot_general(nope.astype(bf16), key_up, (((1,), (1,)), ((), ())), preferred_element_type=f32).astype(bf16).astype(f32)
        for part in range(rank // 128):
            qs[part, pl.ds(head, rows, stride=heads), :] = q_lat[:, part * 128:(part + 1) * 128]
        qr[pl.ds(head, rows, stride=heads), :] = pe_rot

    for j in range(Q_CHUNKS):
        w_copies[2 + j].wait()
        query = jnp.dot(normed[...], wq[j], preferred_element_type=f32).astype(bf16).astype(f32)
        for pair in range(chunk // 384):
            base = pair * 384
            part_a, part_b, part_c = (query[:, base + 128 * i:base + 128 * (i + 1)] for i in range(3))
            pe_rot = rotate_pair(jnp.where(low, part_b, part_c))
            head = (j * chunk + base) // 192
            put_head(head, part_a, pe_rot)
            put_head(head + 1, jnp.where(low, pltpu.roll(part_b, ROPE_DIM, 1), pltpu.roll(part_c, ROPE_DIM, 1)), pltpu.roll(pe_rot, ROPE_DIM, 1))

    rope_copy.wait()

    def attend(g, blocks):
        slot = lax.rem(g, SLOTS)
        span = blocks * BLOCK
        for copy in group_copies(g, blocks):
            copy.wait()
        picks = [order[g * GROUP + i] for i in range(GROUP)]
        for i, b in enumerate(picks):
            length = lens_ref[b]
            base = pl.multiple_of(lax.div(length, 16) * 16, 16)
            tile = keys[slot, i, pl.ds(base, 16), :].astype(f32)
            sub = lax.broadcasted_iota(jnp.int32, (16, rank), 0)
            keys[slot, i, pl.ds(base, 16), :] = jnp.where(sub == length - base, lat_row[pl.ds(b, 1), :], tile).astype(bf16)

        def score_of(i):
            b = picks[i]
            length = lens_ref[b]
            mine = pl.ds(pl.multiple_of(b * heads, heads), heads)
            q_lat = jnp.concatenate([qs[part, mine, :] for part in range(rank // 128)], axis=1).astype(bf16)
            q_rot = qr[mine, :]
            if i % 2:
                score = lax.dot_general(keys[slot, i, :span], q_lat, (((1,), (1,)), ((), ())), preferred_element_type=f32).T
            else:
                score = lax.dot_general(q_lat, keys[slot, i, :span], (((1,), (1,)), ((), ())), preferred_element_type=f32)
            near = jnp.dot(q_rot[:, :ROPE_DIM].astype(bf16), rope[b, :, :span], preferred_element_type=f32)
            first = lax.broadcasted_iota(jnp.int32, (heads, 2 * ROPE_DIM), 1) < ROPE_DIM
            new = jnp.sum(jnp.where(first, q_rot * rope_row[pl.ds(b, 1), :], 0.0), axis=1, keepdims=True)
            at = lax.broadcasted_iota(jnp.int32, (heads, span), 1)
            score = (score + jnp.where(at == length, new, near)) * SCALE
            return jnp.where(at <= length, score, -jnp.inf)

        def finish(i, score):
            expo = jnp.exp(score - jnp.max(score, axis=1, keepdims=True))
            prob = (expo * (1.0 / jnp.sum(expo, axis=1, keepdims=True))).astype(bf16)
            out = jnp.dot(prob, keys[slot, i, :span], preferred_element_type=f32)
            for part in range(rank // 128):
                ol[part, pl.ds(picks[i], heads, stride=PITCH), :] = out[:, part * 128:(part + 1) * 128]

        scores = {}
        for i in range(GROUP + LAG):
            if i < GROUP:
                scores[i] = score_of(i)
            if i >= LAG:
                finish(i - LAG, scores.pop(i - LAG))

    def one_group(g, carry):
        per_class(g, lambda blocks: attend(g, blocks))

        @pl.when(g + SLOTS < groups)
        def _():
            start_group(g + SLOTS)

        @pl.when(g == groups - SLOTS - 1)
        def _():
            for copy in late_copies:
                copy.start()

        return carry

    lax.fori_loop(0, groups, one_group, 0)

    late_copies[0].wait()
    for head in range(heads):
        cols = slice(head * VAL_DIM, (head + 1) * VAL_DIM)
        lat_out = jnp.concatenate([ol[part, head * PITCH:head * PITCH + rows, :] for part in range(rank // 128)], axis=1).astype(bf16)
        heads_out[:, cols] = jnp.dot(lat_out, wv[:, cols], preferred_element_type=f32).astype(bf16)
    square = jnp.zeros((rows, 1), f32)
    for n in range(width // 512):
        cols = slice(n * 512, (n + 1) * 512)
        late_copies[1 + n].wait()
        attn_out = jnp.dot(heads_out[...], wo[n], preferred_element_type=f32)
        resid = (hidden_ref[:, cols].astype(f32) + attn_out).astype(bf16)
        resid_ref[:, cols] = resid
        square = square + jnp.sum(resid.astype(f32) * resid.astype(f32), axis=-1, keepdims=True)
    inv_rms = lax.rsqrt(square * (1.0 / width) + EPS)
    mlp_in_ref[...] = (resid_ref[...].astype(f32) * inv_rms * mlp_gain[...].astype(f32)[None]).astype(bf16)


def attention_block(hidden, cache_lat, cache_rope, seq_lens, attn_norm, w_query, w_kv_down, kv_norm, w_key_up, w_val_up, w_out, mlp_norm):
    rows, width = hidden.shape
    slots, rank = cache_lat.shape[1:]
    bf16, f32 = jnp.bfloat16, jnp.float32
    heads = w_key_up.shape[1] // NOPE_DIM
    q_width = w_query.shape[1]
    vmem = pl.BlockSpec(memory_space=pltpu.VMEM)
    hbm = pl.BlockSpec(memory_space=pl.ANY)
    smem = pl.BlockSpec(memory_space=pltpu.SMEM)
    dma = pltpu.SemaphoreType.DMA
    flops = 2 * rows * (width * (q_width + rank + ROPE_DIM + width) + heads * rank * (NOPE_DIM + VAL_DIM) + heads * slots * (2 * rank + ROPE_DIM))
    moved = 2 * (width * (q_width + rank + ROPE_DIM + width) + heads * rank * (NOPE_DIM + VAL_DIM) + rows * slots * (rank + ROPE_DIM))
    return pl.pallas_call(
        attn_kernel,
        out_shape=(
            jax.ShapeDtypeStruct((rows, width), bf16),
            jax.ShapeDtypeStruct((rows, width), bf16),
            jax.ShapeDtypeStruct((rows, rank), bf16),
            jax.ShapeDtypeStruct((rows, ROPE_DIM), bf16),
        ),
        in_specs=[smem] + [vmem] * 5 + [hbm] * 7,
        out_specs=(vmem,) * 4,
        scratch_shapes=[
            pltpu.VMEM((SLOTS, GROUP, slots, rank), bf16),
            pltpu.VMEM((rows, ROPE_DIM, slots), bf16),
            pltpu.VMEM((Q_CHUNKS, width, q_width // Q_CHUNKS), bf16),
            pltpu.VMEM((rank + ROPE_DIM, width), bf16),
            pltpu.VMEM((rank, heads * NOPE_DIM), bf16),
            pltpu.VMEM((rank, heads * VAL_DIM), bf16),
            pltpu.VMEM((width // 512, heads * VAL_DIM, 512), bf16),
            pltpu.VMEM((rows, width), bf16),
            pltpu.VMEM((rank // 128, rows * heads, 128), f32),
            pltpu.VMEM((rank // 128, PITCH * heads, 128), f32),
            pltpu.VMEM((rows * heads, 2 * ROPE_DIM), f32),
            pltpu.VMEM((rows, rank), f32),
            pltpu.VMEM((rows, 2 * ROPE_DIM), f32),
            pltpu.VMEM((rows, heads * VAL_DIM), bf16),
            pltpu.SMEM((rows,), jnp.int32),
            dma((SLOTS, GROUP)),
            dma((4 + Q_CHUNKS + width // 512,)),
        ],
        compiler_params=pltpu.CompilerParams(vmem_limit_bytes=VMEM_LIMIT),
        cost_estimate=pl.CostEstimate(flops=flops, bytes_accessed=moved, transcendentals=rows * heads * slots),
        name='latent_attention',
    )(seq_lens, hidden, seq_lens, attn_norm, kv_norm, mlp_norm, cache_lat, jnp.swapaxes(cache_rope, 1, 2), w_query, w_kv_down.T, w_key_up, w_val_up, w_out)


MESH = pl.DeviceIdType.MESH
NSUB = 2
NRS = 8
STRIP = 512
HALVES = 2
TURN = 128


def mlp_kernel(g_ref, resid_ref, wg_hbm, wu_hbm, wd_hbm, out_ref,
               g_all, wg_rows, wu_rows, wg, wu, wd, act, pown, psend, precv, rsend, rrecv_e, rrecv_m,
               w_sem, d_sem, ag_recv, ag_recv_d, ag_send_e, ag_send_m, ag_send_d,
               rd_recv, rd_send, rs_recv_e, rs_recv_m, rs_send):
    ffn = wd.shape[0]
    padded = wg.shape[1]
    rows, width = g_ref.shape
    sub = rows // NSUB
    rsub = rows // NRS
    me = lax.axis_index('tp')
    z = lax.div(me, 2)
    c = lax.rem(me, 2)
    upper = z >= 2
    is_end = jnp.logical_or(z == 0, z == 3)
    is_int = jnp.logical_not(is_end)

    def mir(k):
        return jnp.where(upper, k, 3 - k)

    partner = 2 * z + (1 - c)
    dev_e = jnp.where(is_end, me, 2 * mir(3) + c)
    dev_m = 2 * jnp.where(is_end, mir(2), mir(1)) + c

    turns = padded // TURN
    last = ffn - (turns - 1) * TURN

    def w_piece(src, dst, idx, at, count):
        return pltpu.make_async_copy(src.at[pl.ds(at * TURN, count)], dst.at[pl.ds(at * TURN, count)], w_sem.at[idx, at])

    def w_both(at, count):
        return [w_piece(wg_hbm, wg_rows, 0, at, count), w_piece(wu_hbm, wu_rows, 1, at, count)]

    down_copy = pltpu.make_async_copy(wd_hbm, wd, d_sem)

    def start_piece(at, carry):
        for copy in w_both(at, TURN):
            copy.start()
        return carry

    lax.fori_loop(0, turns - 1, start_piece, 0)
    for copy in w_both(turns - 1, last):
        copy.start()
    down_copy.start()

    barrier = pltpu.get_barrier_semaphore()
    pl.semaphore_signal(barrier, inc=1, device_id={'tp': partner}, device_id_type=MESH)
    pl.semaphore_signal(barrier, inc=1, device_id={'tp': dev_m}, device_id_type=MESH)

    @pl.when(is_int)
    def _():
        pl.semaphore_signal(barrier, inc=1, device_id={'tp': dev_e}, device_id_type=MESH)
        pl.semaphore_wait(barrier, 3)

    @pl.when(is_end)
    def _():
        pl.semaphore_wait(barrier, 2)

    def remote(src, dst, send_sem, recv_sem, dev):
        return pltpu.make_async_remote_copy(src_ref=src, dst_ref=dst, send_sem=send_sem, recv_sem=recv_sem, device_id={'tp': dev}, device_id_type=MESH)

    def ag_copy(src, chip, k, send_sem, dev):
        return remote(src, g_all.at[chip, 0, pl.ds(k * sub, sub)], send_sem.at[chip, k], ag_recv.at[chip, k], dev)

    def ag_d2d(src, chip, k):
        return remote(src, g_all.at[chip, 1, pl.ds(k * sub, sub)], ag_send_d.at[chip, k], ag_recv_d.at[chip, k], partner)

    for k in range(NSUB):
        piece = g_ref.at[pl.ds(k * sub, sub)]
        ag_copy(piece, z, k, ag_send_m, dev_m).start()

        @pl.when(is_int)
        def _():
            ag_copy(piece, z, k, ag_send_e, dev_e).start()

        ag_d2d(piece, z, k).start()
    g_all[z, 0] = g_ref[...]

    def landed(chip, k):
        return g_all.at[chip, 0, pl.ds(k * sub, sub)]

    def arrive(chip, k, send_sem, dev):
        src = landed(chip, k)
        ag_copy(src, chip, k, ag_send_d, dev_m).wait_recv()
        if dev is not None:
            ag_copy(src, chip, k, send_sem, dev).start()
        ag_d2d(src, chip, k).start()

    def both(chip):
        for k in range(NSUB):
            ag_d2d(landed(chip, k), chip, k).wait_recv()

    def rd_copy(chip, part):
        span = pl.ds(pl.multiple_of(part * (width // HALVES), width // HALVES), width // HALVES)
        return remote(psend.at[chip, :, span], precv.at[chip, :, span], rd_send.at[chip, part], rd_recv.at[chip, part], partner)

    def rd_wait(chip):
        for part in range(HALVES):
            rd_copy(chip, part).wait_recv()

    def rs_copy(chip, k, dst, recv_sem, dev):
        span = pl.ds(k * rsub, rsub)
        return remote(rsend.at[chip, span], dst.at[chip, span], rs_send.at[chip, k], recv_sem.at[chip, k], dev)

    def rs_base(chip, k):
        span = pl.ds(k * rsub, rsub)
        return pown[chip, span] + precv[chip, span].astype(jnp.float32)

    def end_send(chip):
        rd_wait(chip)
        for k in range(NRS):
            rsend[chip, pl.ds(k * rsub, rsub)] = rs_base(chip, k).astype(jnp.bfloat16)
            rs_copy(chip, k, rrecv_e, rs_recv_e, dev_m).start()

    def hook(step, strip):
        def at(role, want_step, want_strip, fn):
            if strip == want_strip:
                pl.when(jnp.logical_and(role, step == want_step))(fn)

        at(is_int, 0, 1, lambda: arrive(mir(0), 0, ag_send_e, dev_e))
        at(is_int, 1, 0, lambda: arrive(mir(0), 1, ag_send_e, dev_e))
        at(is_end, 0, 0, lambda: arrive(mir(1), 0, None, None))
        at(is_end, 1, 0, lambda: end_send(mir(2)))
        at(is_end, 1, 1, lambda: arrive(mir(0), 0, None, None))
        at(is_end, 2, 0, lambda: end_send(mir(1)))
        at(is_end, 3, 0, lambda: end_send(mir(0)))

    def swiglu(lhs, span):
        gate = jnp.dot(lhs, wg[:, span], preferred_element_type=jnp.float32)
        up = jnp.dot(lhs, wu[:, span], preferred_element_type=jnp.float32)
        return (gate / (1.0 + jnp.exp(-gate)) * up).astype(jnp.bfloat16)

    def first_arrivals(k):
        @pl.when(is_int)
        def _():
            arrive(mir(3), k, ag_send_m, dev_m)
            arrive(mir(1), k, ag_send_e, dev_e)

        @pl.when(is_end)
        def _():
            arrive(mir(2), k, None, None)

    def turn(at, carry):
        span = pl.ds(pl.multiple_of(at * TURN, TURN), TURN)
        for copy in w_both(at, TURN):
            copy.wait()
        wg[:, span] = wg_rows[span].T
        wu[:, span] = wu_rows[span].T
        pl.when(at == turns // 2)(lambda: first_arrivals(0))
        return carry

    lax.fori_loop(0, turns - 1, turn, 0)
    for copy in w_both(turns - 1, last):
        copy.wait()
    tail = slice((turns - 1) * TURN, padded)
    for src in (wg_rows, wu_rows):
        src[ffn:] = jnp.zeros((padded - ffn, width), jnp.bfloat16)
    wg[:, tail] = wg_rows[tail].T
    wu[:, tail] = wu_rows[tail].T
    first_arrivals(1)


    def one_step(step, carry):
        chip = mir(jnp.where(is_end, lax.rem(6 - step, 4), jnp.where(step == 0, 2, jnp.where(step == 1, 3, 3 - step))))

        @pl.when(jnp.logical_and(step == 1, is_end))
        def _():
            arrive(mir(1), 1, None, None)

        @pl.when(jnp.logical_and(step == 2, is_end))
        def _():
            arrive(mir(0), 1, None, None)

        both(chip)

        for strip, at in enumerate(range(0, padded, STRIP)):
            span = slice(at, min(at + STRIP, padded))
            act[:, span] = swiglu(g_all[chip].reshape(2 * rows, width), span)
            hook(step, strip)

        @pl.when(step == 0)
        def _():
            down_copy.wait()

        def one_part(part, carry):
            wide = width // HALVES
            span = pl.ds(pl.multiple_of(part * wide, wide), wide)
            down = jnp.dot(act[:, :ffn], wd[:, span], preferred_element_type=jnp.float32)
            psend[chip, :, span] = down[rows:].astype(jnp.bfloat16)
            pown[chip, :, span] = down[:rows]
            rd_copy(chip, part).start()
            return carry

        lax.fori_loop(0, HALVES, one_part, 0)
        return carry

    lax.fori_loop(0, 4, one_step, 0)

    @pl.when(is_end)
    def _():
        rd_wait(z)
        base = pown[z] + precv[z].astype(jnp.float32) + resid_ref[...].astype(jnp.float32)
        pown[z] = base
        for k in range(NRS):
            span = pl.ds(k * rsub, rsub)
            rs_copy(z, k, rrecv_m, rs_recv_m, dev_m).wait_recv()
            out_ref[span] = (pown[z, span] + rrecv_m[z, span].astype(jnp.float32)).astype(jnp.bfloat16)

    @pl.when(is_int)
    def _():
        def pass_on(chip, dst_in, sem_in, dst_out, sem_out, dev):
            rd_wait(chip)
            for k in range(NRS):
                span = pl.ds(k * rsub, rsub)
                rs_copy(chip, k, dst_in, sem_in, dev_m).wait_recv()
                rsend[chip, span] = (rs_base(chip, k) + dst_in[chip, span].astype(jnp.float32)).astype(jnp.bfloat16)
                rs_copy(chip, k, dst_out, sem_out, dev).start()

        def own_send(chip):
            pass_on(chip, rrecv_e, rs_recv_e, rrecv_m, rs_recv_m, dev_m)

        own_send(mir(1))
        rd_wait(z)
        for k in range(NRS):
            rs_copy(z, k, rrecv_e, rs_recv_e, dev_m).wait_recv()
        pown[z] = pown[z] + precv[z].astype(jnp.float32) + resid_ref[...].astype(jnp.float32) + rrecv_e[z].astype(jnp.float32)
        own_send(mir(0))
        for k in range(NRS):
            span = pl.ds(k * rsub, rsub)
            rs_copy(z, k, rrecv_m, rs_recv_m, dev_m).wait_recv()
            out_ref[span] = (pown[z, span] + rrecv_m[z, span].astype(jnp.float32)).astype(jnp.bfloat16)
        pass_on(mir(3), rrecv_m, rs_recv_m, rrecv_m, rs_recv_m, dev_e)

    for k in range(NSUB):
        for chip in range(4):
            ag_d2d(landed(chip, k), chip, k).wait_send()
        ag_copy(landed(z, k), z, k, ag_send_m, dev_m).wait_send()

        @pl.when(is_int)
        def _():
            ag_copy(landed(z, k), z, k, ag_send_e, dev_e).wait_send()
            ag_copy(landed(mir(3), k), mir(3), k, ag_send_m, dev_m).wait_send()
            ag_copy(landed(mir(1), k), mir(1), k, ag_send_e, dev_e).wait_send()
            ag_copy(landed(mir(0), k), mir(0), k, ag_send_e, dev_e).wait_send()

    for chip in range(4):
        for part in range(HALVES):
            rd_copy(chip, part).wait_send()

        @pl.when(chip != z)
        def _():
            for k in range(NRS):
                rs_copy(chip, k, rrecv_m, rs_recv_m, dev_m).wait_send()


def mlp_block(mlp_in, resid, w_gate_t, w_up_t, w_down):
    rows, width = mlp_in.shape
    ffn = w_gate_t.shape[0]
    padded = -(-ffn // TURN) * TURN
    bf16, f32 = jnp.bfloat16, jnp.float32
    vmem = pl.BlockSpec(memory_space=pltpu.VMEM)
    hbm = pl.BlockSpec(memory_space=pl.ANY)
    dma = pltpu.SemaphoreType.DMA
    flops = 3 * 2 * 8 * rows * width * ffn
    return pl.pallas_call(
        mlp_kernel,
        out_shape=jax.ShapeDtypeStruct((rows, width), bf16),
        in_specs=[vmem, vmem, hbm, hbm, hbm],
        out_specs=vmem,
        scratch_shapes=[
            pltpu.VMEM((4, 2, rows, width), bf16),
            pltpu.VMEM((padded, width), bf16),
            pltpu.VMEM((padded, width), bf16),
            pltpu.VMEM((width, padded), bf16),
            pltpu.VMEM((width, padded), bf16),
            pltpu.VMEM((ffn, width), bf16),
            pltpu.VMEM((2 * rows, padded), bf16),
            pltpu.VMEM((4, rows, width), f32),
            pltpu.VMEM((4, rows, width), bf16),
            pltpu.VMEM((4, rows, width), bf16),
            pltpu.VMEM((4, rows, width), bf16),
            pltpu.VMEM((4, rows, width), bf16),
            pltpu.VMEM((4, rows, width), bf16),
            dma((2, padded // TURN)),
            dma,
            dma((4, NSUB)), dma((4, NSUB)), dma((4, NSUB)), dma((4, NSUB)), dma((4, NSUB)),
            dma((4, HALVES)), dma((4, HALVES)),
            dma((4, NRS)), dma((4, NRS)), dma((4, NRS)),
        ],
        compiler_params=pltpu.CompilerParams(collective_id=0, has_side_effects=True, vmem_limit_bytes=60 * 1024 * 1024),
        cost_estimate=pl.CostEstimate(flops=flops, bytes_accessed=3 * 2 * ffn * width, transcendentals=8 * rows * ffn),
        name='mlp_exchange',
    )(mlp_in, resid, w_gate_t, w_up_t, w_down)


def solution(mesh):
    rows_spec = P(('dp', 'tp'), None)
    cache_spec = P(('dp', 'tp'), None, None)
    whole = P()
    in_specs = (rows_spec, cache_spec, cache_spec, P(('dp', 'tp')), whole, whole, whole, whole, whole, whole, whole, whole, P(None, 'tp'), P(None, 'tp'), P('tp', None))
    out_specs = (rows_spec, rows_spec, rows_spec)

    def device_step(hidden, cache_lat, cache_rope, seq_lens, attn_norm, w_query, w_kv_down, kv_norm, w_key_up, w_val_up, w_out, mlp_norm, w_gate, w_up, w_down):
        resid, mlp_in, lat_new, rope_new = attention_block(hidden, cache_lat, cache_rope, seq_lens, attn_norm, w_query, w_kv_down, kv_norm, w_key_up, w_val_up, w_out, mlp_norm)
        out_hidden = mlp_block(mlp_in, resid, w_gate.T, w_up.T, w_down)
        return out_hidden, lat_new, rope_new

    return jax.shard_map(device_step, mesh=mesh, in_specs=in_specs, out_specs=out_specs, check_vma=False)
```

```python
import math

import jax
import jax.numpy as jnp
from jax import lax
from jax.experimental import pallas as pl
from jax.experimental.pallas import tpu as pltpu
from jax.sharding import PartitionSpec as P

EPS = 1e-6
ROPE_BASE = 10000.0
ROPE_DIM = 64
NOPE_DIM = 128
VAL_DIM = 128
SCALE = (NOPE_DIM + ROPE_DIM) ** -0.5


GROUP = 4
SLOTS = 7
BLOCK = 64
PITCH = 24
Q_CHUNKS = 4
VMEM_LIMIT = 63 * 1024 * 1024


def attn_kernel(lens_ref, hidden_hbm, lens_vec, attn_gain, kv_gain, mlp_gain, lat_hbm, rope_hbm, wq_hbm, wkv_hbm, wk_hbm, wv_hbm, wo_hbm,
                resid_ref, mlp_in_ref, lat_new_ref, rope_new_ref,
                hidden_ref, keys, rope, wq, wkv, wk, wv, wo, normed, qs, ol, qr, lat_row, rope_row, heads_out, order, place, key_sem, w_sem, hidden_sem):
    f32, bf16 = jnp.float32, jnp.bfloat16
    rows, width = hidden_ref.shape
    hidden_copy = pltpu.make_async_copy(hidden_hbm, hidden_ref, hidden_sem)
    hidden_copy.start()
    rank = wk.shape[0]
    heads = wk.shape[1] // NOPE_DIM
    groups = rows // GROUP
    classes = keys.shape[2] // BLOCK

    chunk = wq.shape[2]
    w_copies = [pltpu.make_async_copy(wkv_hbm, wkv, w_sem.at[0]), pltpu.make_async_copy(wk_hbm, wk, w_sem.at[1])]
    w_copies += [pltpu.make_async_copy(wq_hbm.at[:, pl.ds(j * chunk, chunk)], wq.at[j], w_sem.at[2 + j]) for j in range(Q_CHUNKS)]
    rope_copy = pltpu.make_async_copy(rope_hbm, rope, w_sem.at[2 + Q_CHUNKS])
    late_copies = [pltpu.make_async_copy(wv_hbm, wv, w_sem.at[3 + Q_CHUNKS])]
    late_copies += [pltpu.make_async_copy(wo_hbm.at[:, pl.ds(n * 512, 512)], wo.at[n], w_sem.at[4 + Q_CHUNKS + n]) for n in range(width // 512)]
    for copy in w_copies:
        copy.start()
    rope_copy.start()

    def kind(b):
        return lax.div(lens_ref[b], BLOCK)

    for i in range(classes):
        place[i] = 0

    def count(b, carry):
        place[kind(b)] += 1
        return carry

    lax.fori_loop(0, rows, count, 0)
    total = jnp.int32(0)
    for i in reversed(range(classes)):
        here = place[i]
        place[i] = total
        total = total + here

    def put(b, carry):
        k = kind(b)
        at = place[k]
        order[at] = b
        place[k] = at + 1
        return carry

    lax.fori_loop(0, rows, put, 0)

    def group_copies(g, blocks):
        slot = lax.rem(g, SLOTS)
        return [pltpu.make_async_copy(lat_hbm.at[order[g * GROUP + i], pl.ds(0, blocks * BLOCK)], keys.at[slot, i, pl.ds(0, blocks * BLOCK)], key_sem.at[slot, i]) for i in range(GROUP)]

    def per_class(g, fn):
        k = kind(order[g * GROUP])
        for i in range(classes):
            @pl.when(k == i)
            def _():
                fn(i + 1)

    def start_group(g):
        def start(blocks):
            for copy in group_copies(g, blocks):
                copy.start()

        per_class(g, start)

    def start_first(g, carry):
        start_group(g)
        return carry

    lax.fori_loop(0, SLOTS, start_first, 0)

    hidden_copy.wait()
    vals = hidden_ref[...].astype(f32)
    inv_rms = lax.rsqrt(jnp.mean(vals * vals, axis=-1, keepdims=True) + EPS)
    normed[...] = (vals * inv_rms * attn_gain[...].astype(f32)[None]).astype(bf16)

    lane = lax.broadcasted_iota(jnp.int32, (rows, 2 * ROPE_DIM), 1)
    half = ROPE_DIM // 2
    freq = jnp.exp(lax.rem(lane, half).astype(f32) * (-math.log(ROPE_BASE) / half))
    square_ids = (rows, rows)
    diagonal = lax.broadcasted_iota(jnp.int32, square_ids, 0) == lax.broadcasted_iota(jnp.int32, square_ids, 1)
    lens = jnp.sum(jnp.where(diagonal, lens_vec[...].astype(f32)[None], 0.0), axis=1, keepdims=True)
    angles = lens * freq
    cos_tab = jnp.cos(angles)
    is_first = lax.rem(lane, ROPE_DIM) < half
    sin_tab = jnp.where(is_first, -jnp.sin(angles), jnp.sin(angles))

    def rotate_pair(pair):
        swapped = jnp.where(is_first, pltpu.roll(pair, 2 * ROPE_DIM - half, 1), pltpu.roll(pair, half, 1))
        return (pair * cos_tab + swapped * sin_tab).astype(bf16).astype(f32)

    w_copies[0].wait()
    kv = lax.dot_general(normed[...], wkv[...], (((1,), (1,)), ((), ())), preferred_element_type=f32).astype(bf16).astype(f32)
    lat = kv[:, :rank]
    inv_lat = lax.rsqrt(jnp.mean(lat * lat, axis=-1, keepdims=True) + EPS)
    lat_new = (lat * inv_lat * kv_gain[...].astype(f32)[None]).astype(bf16)
    lat_new_ref[...] = lat_new
    lat_row[...] = lat_new.astype(f32)
    pe = kv[:, rank:]
    rope_new = rotate_pair(jnp.concatenate([pe, pe], axis=1))
    rope_new_ref[...] = rope_new[:, :ROPE_DIM].astype(bf16)
    rope_row[...] = rope_new

    w_copies[1].wait()
    low = lane < ROPE_DIM

    def put_head(head, nope, pe_rot):
        key_up = wk[:, head * NOPE_DIM:(head + 1) * NOPE_DIM]
        q_lat = lax.dot_general(nope.astype(bf16), key_up, (((1,), (1,)), ((), ())), preferred_element_type=f32).astype(bf16).astype(f32)
        for part in range(rank // 128):
            qs[part, pl.ds(head, rows, stride=PITCH), :] = q_lat[:, part * 128:(part + 1) * 128]
        qr[pl.ds(head, rows, stride=PITCH), :] = pe_rot

    for j in range(Q_CHUNKS):
        w_copies[2 + j].wait()
        query = jnp.dot(normed[...], wq[j], preferred_element_type=f32).astype(bf16).astype(f32)
        for pair in range(chunk // 384):
            base = pair * 384
            part_a, part_b, part_c = (query[:, base + 128 * i:base + 128 * (i + 1)] for i in range(3))
            pe_rot = rotate_pair(jnp.where(low, part_b, part_c))
            head = (j * chunk + base) // 192
            put_head(head, part_a, pe_rot)
            put_head(head + 1, jnp.where(low, pltpu.roll(part_b, ROPE_DIM, 1), pltpu.roll(part_c, ROPE_DIM, 1)), pltpu.roll(pe_rot, ROPE_DIM, 1))

    rope_copy.wait()

    def attend(g, blocks):
        slot = lax.rem(g, SLOTS)
        span = blocks * BLOCK
        for copy in group_copies(g, blocks):
            copy.wait()
        scores = []
        picks = [order[g * GROUP + i] for i in range(GROUP)]
        for i, b in enumerate(picks):
            length = lens_ref[b]
            base = pl.multiple_of(lax.div(length, 16) * 16, 16)
            tile = keys[slot, i, pl.ds(base, 16), :].astype(f32)
            sub = lax.broadcasted_iota(jnp.int32, (16, rank), 0)
            keys[slot, i, pl.ds(base, 16), :] = jnp.where(sub == length - base, lat_row[pl.ds(b, 1), :], tile).astype(bf16)
        for i, b in enumerate(picks):
            length = lens_ref[b]
            mine = pl.ds(pl.multiple_of(b * PITCH, 8), heads)
            q_lat = jnp.concatenate([qs[part, mine, :] for part in range(rank // 128)], axis=1).astype(bf16)
            q_rot = qr[mine, :]
            score = lax.dot_general(q_lat, keys[slot, i, :span], (((1,), (1,)), ((), ())), preferred_element_type=f32)
            near = jnp.dot(q_rot[:, :ROPE_DIM].astype(bf16), rope[b, :, :span], preferred_element_type=f32)
            first = lax.broadcasted_iota(jnp.int32, (heads, 2 * ROPE_DIM), 1) < ROPE_DIM
            new = jnp.sum(jnp.where(first, q_rot * rope_row[pl.ds(b, 1), :], 0.0), axis=1, keepdims=True)
            at = lax.broadcasted_iota(jnp.int32, (heads, span), 1)
            score = (score + jnp.where(at == length, new, near)) * SCALE
            scores.append(jnp.where(at <= length, score, -jnp.inf))
        probs = []
        for score in scores:
            expo = jnp.exp(score - jnp.max(score, axis=1, keepdims=True))
            probs.append((expo * (1.0 / jnp.sum(expo, axis=1, keepdims=True))).astype(bf16))
        for i, b in enumerate(picks):
            out = jnp.dot(probs[i], keys[slot, i, :span], preferred_element_type=f32)
            for part in range(rank // 128):
                ol[part, pl.ds(pl.multiple_of(b * PITCH, 8), heads), :] = out[:, part * 128:(part + 1) * 128]

    def one_group(g, carry):
        per_class(g, lambda blocks: attend(g, blocks))

        @pl.when(g + SLOTS < groups)
        def _():
            start_group(g + SLOTS)

        @pl.when(g == groups - SLOTS - 2)
        def _():
            for copy in late_copies:
                copy.start()

        return carry

    lax.fori_loop(0, groups, one_group, 0)

    late_copies[0].wait()
    for head in range(heads):
        cols = slice(head * VAL_DIM, (head + 1) * VAL_DIM)
        lat_out = jnp.concatenate([ol[part, pl.ds(head, rows, stride=PITCH), :] for part in range(rank // 128)], axis=1).astype(bf16)
        heads_out[:, cols] = jnp.dot(lat_out, wv[:, cols], preferred_element_type=f32).astype(bf16)
    square = jnp.zeros((rows, 1), f32)
    for n in range(width // 512):
        cols = slice(n * 512, (n + 1) * 512)
        late_copies[1 + n].wait()
        attn_out = jnp.dot(heads_out[...], wo[n], preferred_element_type=f32)
        resid = (hidden_ref[:, cols].astype(f32) + attn_out).astype(bf16)
        resid_ref[:, cols] = resid
        square = square + jnp.sum(resid.astype(f32) * resid.astype(f32), axis=-1, keepdims=True)
    inv_rms = lax.rsqrt(square * (1.0 / width) + EPS)
    mlp_in_ref[...] = (resid_ref[...].astype(f32) * inv_rms * mlp_gain[...].astype(f32)[None]).astype(bf16)


def attention_block(hidden, cache_lat, cache_rope, seq_lens, attn_norm, w_query, w_kv_down, kv_norm, w_key_up, w_val_up, w_out, mlp_norm):
    rows, width = hidden.shape
    slots, rank = cache_lat.shape[1:]
    bf16, f32 = jnp.bfloat16, jnp.float32
    heads = w_key_up.shape[1] // NOPE_DIM
    q_width = w_query.shape[1]
    vmem = pl.BlockSpec(memory_space=pltpu.VMEM)
    hbm = pl.BlockSpec(memory_space=pl.ANY)
    smem = pl.BlockSpec(memory_space=pltpu.SMEM)
    dma = pltpu.SemaphoreType.DMA
    flops = 2 * rows * (width * (q_width + rank + ROPE_DIM + width) + heads * rank * (NOPE_DIM + VAL_DIM) + heads * slots * (2 * rank + ROPE_DIM))
    moved = 2 * (width * (q_width + rank + ROPE_DIM + width) + heads * rank * (NOPE_DIM + VAL_DIM) + rows * slots * (rank + ROPE_DIM))
    return pl.pallas_call(
        attn_kernel,
        out_shape=(
            jax.ShapeDtypeStruct((rows, width), bf16),
            jax.ShapeDtypeStruct((rows, width), bf16),
            jax.ShapeDtypeStruct((rows, rank), bf16),
            jax.ShapeDtypeStruct((rows, ROPE_DIM), bf16),
        ),
        in_specs=[smem, hbm] + [vmem] * 4 + [hbm] * 7,
        out_specs=(vmem,) * 4,
        scratch_shapes=[
            pltpu.VMEM((rows, width), bf16),
            pltpu.VMEM((SLOTS, GROUP, slots, rank), bf16),
            pltpu.VMEM((rows, ROPE_DIM, slots), bf16),
            pltpu.VMEM((Q_CHUNKS, width, q_width // Q_CHUNKS), bf16),
            pltpu.VMEM((rank + ROPE_DIM, width), bf16),
            pltpu.VMEM((rank, heads * NOPE_DIM), bf16),
            pltpu.VMEM((rank, heads * VAL_DIM), bf16),
            pltpu.VMEM((width // 512, heads * VAL_DIM, 512), bf16),
            pltpu.VMEM((rows, width), bf16),
            pltpu.VMEM((rank // 128, rows * PITCH, 128), f32),
            pltpu.VMEM((rank // 128, rows * PITCH, 128), f32),
            pltpu.VMEM((rows * PITCH, 2 * ROPE_DIM), f32),
            pltpu.VMEM((rows, rank), f32),
            pltpu.VMEM((rows, 2 * ROPE_DIM), f32),
            pltpu.VMEM((rows, heads * VAL_DIM), bf16),
            pltpu.SMEM((rows,), jnp.int32),
            pltpu.SMEM((slots // BLOCK,), jnp.int32),
            dma((SLOTS, GROUP)),
            dma((4 + Q_CHUNKS + width // 512,)),
            dma,
        ],
        compiler_params=pltpu.CompilerParams(vmem_limit_bytes=VMEM_LIMIT),
        cost_estimate=pl.CostEstimate(flops=flops, bytes_accessed=moved, transcendentals=rows * heads * slots),
        name='latent_attention',
    )(seq_lens, hidden, seq_lens, attn_norm, kv_norm, mlp_norm, cache_lat, jnp.swapaxes(cache_rope, 1, 2), w_query, w_kv_down.T, w_key_up, w_val_up, w_out)


MESH = pl.DeviceIdType.MESH
NSUB = 2
NRS = 8
STRIP = 512
HALVES = 2
TURN = 128


def mlp_kernel(g_hbm, resid_ref, wg_hbm, wu_hbm, wd_hbm, out_ref,
               g_ref, g_all, wg_rows, wu_rows, wg, wu, wd, act, pown, psend, precv, rsend, rrecv_e, rrecv_m,
               g_sem, w_sem, d_sem, ag_recv, ag_recv_d, ag_send_e, ag_send_m, ag_send_d,
               rd_recv, rd_send, rs_recv_e, rs_recv_m, rs_send):
    ffn = wd.shape[0]
    padded = wg.shape[1]
    rows, width = g_ref.shape
    g_copy = pltpu.make_async_copy(g_hbm, g_ref, g_sem)
    g_copy.start()
    sub = rows // NSUB
    rsub = rows // NRS
    me = lax.axis_index('tp')
    z = lax.div(me, 2)
    c = lax.rem(me, 2)
    upper = z >= 2
    is_end = jnp.logical_or(z == 0, z == 3)
    is_int = jnp.logical_not(is_end)

    def mir(k):
        return jnp.where(upper, k, 3 - k)

    partner = 2 * z + (1 - c)
    dev_e = jnp.where(is_end, me, 2 * mir(3) + c)
    dev_m = 2 * jnp.where(is_end, mir(2), mir(1)) + c

    turns = padded // TURN
    last = ffn - (turns - 1) * TURN

    def w_piece(src, dst, idx, at, count):
        return pltpu.make_async_copy(src.at[pl.ds(at * TURN, count)], dst.at[pl.ds(at * TURN, count)], w_sem.at[idx, at])

    def w_both(at, count):
        return [w_piece(wg_hbm, wg_rows, 0, at, count), w_piece(wu_hbm, wu_rows, 1, at, count)]

    down_copy = pltpu.make_async_copy(wd_hbm, wd, d_sem)

    def start_piece(at, carry):
        for copy in w_both(at, TURN):
            copy.start()
        return carry

    lax.fori_loop(0, turns - 1, start_piece, 0)
    for copy in w_both(turns - 1, last):
        copy.start()
    down_copy.start()

    barrier = pltpu.get_barrier_semaphore()
    pl.semaphore_signal(barrier, inc=1, device_id={'tp': partner}, device_id_type=MESH)
    pl.semaphore_signal(barrier, inc=1, device_id={'tp': dev_m}, device_id_type=MESH)

    @pl.when(is_int)
    def _():
        pl.semaphore_signal(barrier, inc=1, device_id={'tp': dev_e}, device_id_type=MESH)
        pl.semaphore_wait(barrier, 3)

    @pl.when(is_end)
    def _():
        pl.semaphore_wait(barrier, 2)

    def remote(src, dst, send_sem, recv_sem, dev):
        return pltpu.make_async_remote_copy(src_ref=src, dst_ref=dst, send_sem=send_sem, recv_sem=recv_sem, device_id={'tp': dev}, device_id_type=MESH)

    def ag_copy(src, chip, k, send_sem, dev):
        return remote(src, g_all.at[chip, 0, pl.ds(k * sub, sub)], send_sem.at[chip, k], ag_recv.at[chip, k], dev)

    def ag_d2d(src, chip, k):
        return remote(src, g_all.at[chip, 1, pl.ds(k * sub, sub)], ag_send_d.at[chip, k], ag_recv_d.at[chip, k], partner)

    g_copy.wait()
    for k in range(NSUB):
        piece = g_ref.at[pl.ds(k * sub, sub)]
        ag_copy(piece, z, k, ag_send_m, dev_m).start()

        @pl.when(is_int)
        def _():
            ag_copy(piece, z, k, ag_send_e, dev_e).start()

        ag_d2d(piece, z, k).start()
    g_all[z, 0] = g_ref[...]

    def landed(chip, k):
        return g_all.at[chip, 0, pl.ds(k * sub, sub)]

    def arrive(chip, k, send_sem, dev):
        src = landed(chip, k)
        ag_copy(src, chip, k, ag_send_d, dev_m).wait_recv()
        if dev is not None:
            ag_copy(src, chip, k, send_sem, dev).start()
        ag_d2d(src, chip, k).start()

    def both(chip):
        for k in range(NSUB):
            ag_d2d(landed(chip, k), chip, k).wait_recv()

    def rd_copy(chip, part):
        span = pl.ds(pl.multiple_of(part * (width // HALVES), width // HALVES), width // HALVES)
        return remote(psend.at[chip, :, span], precv.at[chip, :, span], rd_send.at[chip, part], rd_recv.at[chip, part], partner)

    def rd_wait(chip):
        for part in range(HALVES):
            rd_copy(chip, part).wait_recv()

    def rs_copy(chip, k, dst, recv_sem, dev):
        span = pl.ds(k * rsub, rsub)
        return remote(rsend.at[chip, span], dst.at[chip, span], rs_send.at[chip, k], recv_sem.at[chip, k], dev)

    def rs_base(chip, k):
        span = pl.ds(k * rsub, rsub)
        return pown[chip, span] + precv[chip, span].astype(jnp.float32)

    def end_send(chip):
        rd_wait(chip)
        for k in range(NRS):
            rsend[chip, pl.ds(k * rsub, rsub)] = rs_base(chip, k).astype(jnp.bfloat16)
            rs_copy(chip, k, rrecv_e, rs_recv_e, dev_m).start()

    def hook(step, strip):
        def at(role, want_step, want_strip, fn):
            if strip == want_strip:
                pl.when(jnp.logical_and(role, step == want_step))(fn)

        at(is_int, 0, 1, lambda: arrive(mir(0), 0, ag_send_e, dev_e))
        at(is_int, 1, 0, lambda: arrive(mir(0), 1, ag_send_e, dev_e))
        at(is_end, 0, 0, lambda: arrive(mir(1), 0, None, None))
        at(is_end, 1, 0, lambda: end_send(mir(2)))
        at(is_end, 1, 1, lambda: arrive(mir(0), 0, None, None))
        at(is_end, 2, 0, lambda: end_send(mir(1)))
        at(is_end, 3, 0, lambda: end_send(mir(0)))

    def swiglu(lhs, span):
        gate = jnp.dot(lhs, wg[:, span], preferred_element_type=jnp.float32)
        up = jnp.dot(lhs, wu[:, span], preferred_element_type=jnp.float32)
        return (gate / (1.0 + jnp.exp(-gate)) * up).astype(jnp.bfloat16)

    def first_arrivals(k):
        @pl.when(is_int)
        def _():
            arrive(mir(3), k, ag_send_m, dev_m)
            arrive(mir(1), k, ag_send_e, dev_e)

        @pl.when(is_end)
        def _():
            arrive(mir(2), k, None, None)

    def turn(at, carry):
        span = pl.ds(pl.multiple_of(at * TURN, TURN), TURN)
        for copy in w_both(at, TURN):
            copy.wait()
        wg[:, span] = wg_rows[span].T
        wu[:, span] = wu_rows[span].T
        pl.when(at == turns // 2)(lambda: first_arrivals(0))
        return carry

    lax.fori_loop(0, turns - 1, turn, 0)
    for copy in w_both(turns - 1, last):
        copy.wait()
    tail = slice((turns - 1) * TURN, padded)
    for src in (wg_rows, wu_rows):
        src[ffn:] = jnp.zeros((padded - ffn, width), jnp.bfloat16)
    wg[:, tail] = wg_rows[tail].T
    wu[:, tail] = wu_rows[tail].T
    first_arrivals(1)


    def one_step(step, carry):
        chip = mir(jnp.where(is_end, lax.rem(6 - step, 4), jnp.where(step == 0, 2, jnp.where(step == 1, 3, 3 - step))))

        @pl.when(jnp.logical_and(step == 1, is_end))
        def _():
            arrive(mir(1), 1, None, None)

        @pl.when(jnp.logical_and(step == 2, is_end))
        def _():
            arrive(mir(0), 1, None, None)

        both(chip)

        for strip, at in enumerate(range(0, padded, STRIP)):
            span = slice(at, min(at + STRIP, padded))
            act[:, span] = swiglu(g_all[chip].reshape(2 * rows, width), span)
            hook(step, strip)

        @pl.when(step == 0)
        def _():
            down_copy.wait()

        def one_part(part, carry):
            wide = width // HALVES
            span = pl.ds(pl.multiple_of(part * wide, wide), wide)
            down = jnp.dot(act[:, :ffn], wd[:, span], preferred_element_type=jnp.float32)
            psend[chip, :, span] = down[rows:].astype(jnp.bfloat16)
            pown[chip, :, span] = down[:rows]
            rd_copy(chip, part).start()
            return carry

        lax.fori_loop(0, HALVES, one_part, 0)
        return carry

    lax.fori_loop(0, 4, one_step, 0)

    @pl.when(is_end)
    def _():
        rd_wait(z)
        base = pown[z] + precv[z].astype(jnp.float32) + resid_ref[...].astype(jnp.float32)
        pown[z] = base
        for k in range(NRS):
            span = pl.ds(k * rsub, rsub)
            rs_copy(z, k, rrecv_m, rs_recv_m, dev_m).wait_recv()
            out_ref[span] = (pown[z, span] + rrecv_m[z, span].astype(jnp.float32)).astype(jnp.bfloat16)

    @pl.when(is_int)
    def _():
        def pass_on(chip, dst_in, sem_in, dst_out, sem_out, dev):
            rd_wait(chip)
            for k in range(NRS):
                span = pl.ds(k * rsub, rsub)
                rs_copy(chip, k, dst_in, sem_in, dev_m).wait_recv()
                rsend[chip, span] = (rs_base(chip, k) + dst_in[chip, span].astype(jnp.float32)).astype(jnp.bfloat16)
                rs_copy(chip, k, dst_out, sem_out, dev).start()

        def own_send(chip):
            pass_on(chip, rrecv_e, rs_recv_e, rrecv_m, rs_recv_m, dev_m)

        own_send(mir(1))
        rd_wait(z)
        for k in range(NRS):
            rs_copy(z, k, rrecv_e, rs_recv_e, dev_m).wait_recv()
        pown[z] = pown[z] + precv[z].astype(jnp.float32) + resid_ref[...].astype(jnp.float32) + rrecv_e[z].astype(jnp.float32)
        own_send(mir(0))
        for k in range(NRS):
            span = pl.ds(k * rsub, rsub)
            rs_copy(z, k, rrecv_m, rs_recv_m, dev_m).wait_recv()
            out_ref[span] = (pown[z, span] + rrecv_m[z, span].astype(jnp.float32)).astype(jnp.bfloat16)
        pass_on(mir(3), rrecv_m, rs_recv_m, rrecv_m, rs_recv_m, dev_e)

    for k in range(NSUB):
        for chip in range(4):
            ag_d2d(landed(chip, k), chip, k).wait_send()
        ag_copy(landed(z, k), z, k, ag_send_m, dev_m).wait_send()

        @pl.when(is_int)
        def _():
            ag_copy(landed(z, k), z, k, ag_send_e, dev_e).wait_send()
            ag_copy(landed(mir(3), k), mir(3), k, ag_send_m, dev_m).wait_send()
            ag_copy(landed(mir(1), k), mir(1), k, ag_send_e, dev_e).wait_send()
            ag_copy(landed(mir(0), k), mir(0), k, ag_send_e, dev_e).wait_send()

    for chip in range(4):
        for part in range(HALVES):
            rd_copy(chip, part).wait_send()

        @pl.when(chip != z)
        def _():
            for k in range(NRS):
                rs_copy(chip, k, rrecv_m, rs_recv_m, dev_m).wait_send()


def mlp_block(mlp_in, resid, w_gate_t, w_up_t, w_down):
    rows, width = mlp_in.shape
    ffn = w_gate_t.shape[0]
    padded = -(-ffn // TURN) * TURN
    bf16, f32 = jnp.bfloat16, jnp.float32
    vmem = pl.BlockSpec(memory_space=pltpu.VMEM)
    hbm = pl.BlockSpec(memory_space=pl.ANY)
    dma = pltpu.SemaphoreType.DMA
    flops = 3 * 2 * 8 * rows * width * ffn
    return pl.pallas_call(
        mlp_kernel,
        out_shape=jax.ShapeDtypeStruct((rows, width), bf16),
        in_specs=[hbm, vmem, hbm, hbm, hbm],
        out_specs=vmem,
        scratch_shapes=[
            pltpu.VMEM((rows, width), bf16),
            pltpu.VMEM((4, 2, rows, width), bf16),
            pltpu.VMEM((padded, width), bf16),
            pltpu.VMEM((padded, width), bf16),
            pltpu.VMEM((width, padded), bf16),
            pltpu.VMEM((width, padded), bf16),
            pltpu.VMEM((ffn, width), bf16),
            pltpu.VMEM((2 * rows, padded), bf16),
            pltpu.VMEM((4, rows, width), f32),
            pltpu.VMEM((4, rows, width), bf16),
            pltpu.VMEM((4, rows, width), bf16),
            pltpu.VMEM((4, rows, width), bf16),
            pltpu.VMEM((4, rows, width), bf16),
            pltpu.VMEM((4, rows, width), bf16),
            dma,
            dma((2, padded // TURN)),
            dma,
            dma((4, NSUB)), dma((4, NSUB)), dma((4, NSUB)), dma((4, NSUB)), dma((4, NSUB)),
            dma((4, HALVES)), dma((4, HALVES)),
            dma((4, NRS)), dma((4, NRS)), dma((4, NRS)),
        ],
        compiler_params=pltpu.CompilerParams(collective_id=0, has_side_effects=True, vmem_limit_bytes=60 * 1024 * 1024),
        cost_estimate=pl.CostEstimate(flops=flops, bytes_accessed=3 * 2 * ffn * width, transcendentals=8 * rows * ffn),
        name='mlp_exchange',
    )(mlp_in, resid, w_gate_t, w_up_t, w_down)


def solution(mesh):
    rows_spec = P(('dp', 'tp'), None)
    cache_spec = P(('dp', 'tp'), None, None)
    whole = P()
    in_specs = (rows_spec, cache_spec, cache_spec, P(('dp', 'tp')), whole, whole, whole, whole, whole, whole, whole, whole, P(None, 'tp'), P(None, 'tp'), P('tp', None))
    out_specs = (rows_spec, rows_spec, rows_spec)

    def device_step(hidden, cache_lat, cache_rope, seq_lens, attn_norm, w_query, w_kv_down, kv_norm, w_key_up, w_val_up, w_out, mlp_norm, w_gate, w_up, w_down):
        resid, mlp_in, lat_new, rope_new = attention_block(hidden, cache_lat, cache_rope, seq_lens, attn_norm, w_query, w_kv_down, kv_norm, w_key_up, w_val_up, w_out, mlp_norm)
        out_hidden = mlp_block(mlp_in, resid, w_gate.T, w_up.T, w_down)
        return out_hidden, lat_new, rope_new

    return jax.shard_map(device_step, mesh=mesh, in_specs=in_specs, out_specs=out_specs, check_vma=False)
```

```python
import math

import jax
import jax.numpy as jnp
from jax import lax
from jax.experimental import pallas as pl
from jax.experimental.pallas import tpu as pltpu
from jax.sharding import PartitionSpec as P

EPS = 1e-6
ROPE_BASE = 10000.0
ROPE_DIM = 64
NOPE_DIM = 128
VAL_DIM = 128
SCALE = (NOPE_DIM + ROPE_DIM) ** -0.5


GROUP = 4
SLOTS = 7
BLOCK = 128
Q_CHUNKS = 4
VMEM_LIMIT = 63 * 1024 * 1024


def attn_kernel(lens_ref, hidden_ref, lens_vec, attn_gain, kv_gain, mlp_gain, lat_hbm, rope_hbm, wq_hbm, wkv_hbm, wk_hbm, wv_hbm, wo_hbm,
                resid_ref, mlp_in_ref, lat_new_ref, rope_new_ref,
                keys, rope, wq, wkv, wk, wv, wo, normed, qs, qr, lat_row, rope_row, heads_out, order, key_sem, w_sem):
    f32, bf16 = jnp.float32, jnp.bfloat16
    rows, width = hidden_ref.shape
    rank = wk.shape[0]
    heads = wk.shape[1] // NOPE_DIM
    groups = rows // GROUP
    classes = keys.shape[2] // BLOCK

    chunk = wq.shape[2]
    w_copies = [pltpu.make_async_copy(wkv_hbm, wkv, w_sem.at[0]), pltpu.make_async_copy(wk_hbm, wk, w_sem.at[1])]
    w_copies += [pltpu.make_async_copy(wq_hbm.at[:, pl.ds(j * chunk, chunk)], wq.at[j], w_sem.at[2 + j]) for j in range(Q_CHUNKS)]
    rope_copy = pltpu.make_async_copy(rope_hbm, rope, w_sem.at[2 + Q_CHUNKS])
    late_copies = [pltpu.make_async_copy(wv_hbm, wv, w_sem.at[3 + Q_CHUNKS])]
    late_copies += [pltpu.make_async_copy(wo_hbm.at[:, pl.ds(n * 512, 512)], wo.at[n], w_sem.at[4 + Q_CHUNKS + n]) for n in range(width // 512)]
    for copy in w_copies:
        copy.start()
    rope_copy.start()

    def kind(b):
        return lax.div(lens_ref[b], BLOCK)

    def count(b, counts):
        k = kind(b)
        return tuple(n + jnp.where(k == i, 1, 0) for i, n in enumerate(counts))

    zero = jnp.int32(0)
    counts = lax.fori_loop(0, rows, count, (zero,) * classes)
    firsts = []
    total = zero
    for i in reversed(range(classes)):
        firsts.append(total)
        total = total + counts[i]
    firsts = tuple(reversed(firsts))

    def place(b, firsts):
        k = kind(b)
        at = firsts[0]
        for i in range(1, classes):
            at = jnp.where(k == i, firsts[i], at)
        order[at] = b
        return tuple(n + jnp.where(k == i, 1, 0) for i, n in enumerate(firsts))

    lax.fori_loop(0, rows, place, firsts)

    def group_copies(g, blocks):
        slot = lax.rem(g, SLOTS)
        return [pltpu.make_async_copy(lat_hbm.at[order[g * GROUP + i], pl.ds(0, blocks * BLOCK)], keys.at[slot, i, pl.ds(0, blocks * BLOCK)], key_sem.at[slot, i]) for i in range(GROUP)]

    def per_class(g, fn):
        k = kind(order[g * GROUP])
        for i in range(classes):
            @pl.when(k == i)
            def _():
                fn(i + 1)

    def start_group(g):
        def start(blocks):
            for copy in group_copies(g, blocks):
                copy.start()

        per_class(g, start)

    def start_first(g, carry):
        start_group(g)
        return carry

    lax.fori_loop(0, SLOTS, start_first, 0)

    vals = hidden_ref[...].astype(f32)
    inv_rms = lax.rsqrt(jnp.mean(vals * vals, axis=-1, keepdims=True) + EPS)
    normed[...] = (vals * inv_rms * attn_gain[...].astype(f32)[None]).astype(bf16)

    lane = lax.broadcasted_iota(jnp.int32, (rows, 2 * ROPE_DIM), 1)
    half = ROPE_DIM // 2
    freq = jnp.exp(lax.rem(lane, half).astype(f32) * (-math.log(ROPE_BASE) / half))
    square_ids = (rows, rows)
    diagonal = lax.broadcasted_iota(jnp.int32, square_ids, 0) == lax.broadcasted_iota(jnp.int32, square_ids, 1)
    lens = jnp.sum(jnp.where(diagonal, lens_vec[...].astype(f32)[None], 0.0), axis=1, keepdims=True)
    angles = lens * freq
    cos_tab = jnp.cos(angles)
    is_first = lax.rem(lane, ROPE_DIM) < half
    sin_tab = jnp.where(is_first, -jnp.sin(angles), jnp.sin(angles))

    def rotate_pair(pair):
        swapped = jnp.where(is_first, pltpu.roll(pair, 2 * ROPE_DIM - half, 1), pltpu.roll(pair, half, 1))
        return (pair * cos_tab + swapped * sin_tab).astype(bf16).astype(f32)

    w_copies[0].wait()
    kv = lax.dot_general(normed[...], wkv[...], (((1,), (1,)), ((), ())), preferred_element_type=f32).astype(bf16).astype(f32)
    lat = kv[:, :rank]
    inv_lat = lax.rsqrt(jnp.mean(lat * lat, axis=-1, keepdims=True) + EPS)
    lat_new = (lat * inv_lat * kv_gain[...].astype(f32)[None]).astype(bf16)
    lat_new_ref[...] = lat_new
    lat_row[...] = lat_new.astype(f32)
    pe = kv[:, rank:]
    rope_new = rotate_pair(jnp.concatenate([pe, pe], axis=1))
    rope_new_ref[...] = rope_new[:, :ROPE_DIM].astype(bf16)
    rope_row[...] = rope_new

    w_copies[1].wait()
    low = lane < ROPE_DIM

    def put_head(head, nope, pe_rot):
        key_up = wk[:, head * NOPE_DIM:(head + 1) * NOPE_DIM]
        q_lat = lax.dot_general(nope.astype(bf16), key_up, (((1,), (1,)), ((), ())), preferred_element_type=f32).astype(bf16).astype(f32)
        for part in range(rank // 128):
            qs[part, pl.ds(head, rows, stride=heads), :] = q_lat[:, part * 128:(part + 1) * 128]
        qr[pl.ds(head, rows, stride=heads), :] = pe_rot

    for j in range(Q_CHUNKS):
        w_copies[2 + j].wait()
        query = jnp.dot(normed[...], wq[j], preferred_element_type=f32).astype(bf16).astype(f32)
        for pair in range(chunk // 384):
            base = pair * 384
            part_a, part_b, part_c = (query[:, base + 128 * i:base + 128 * (i + 1)] for i in range(3))
            pe_rot = rotate_pair(jnp.where(low, part_b, part_c))
            head = (j * chunk + base) // 192
            put_head(head, part_a, pe_rot)
            put_head(head + 1, jnp.where(low, pltpu.roll(part_b, ROPE_DIM, 1), pltpu.roll(part_c, ROPE_DIM, 1)), pltpu.roll(pe_rot, ROPE_DIM, 1))

    rope_copy.wait()

    def attend(g, blocks):
        slot = lax.rem(g, SLOTS)
        span = blocks * BLOCK
        for copy in group_copies(g, blocks):
            copy.wait()
        scores = []
        picks = [order[g * GROUP + i] for i in range(GROUP)]
        for i, b in enumerate(picks):
            length = lens_ref[b]
            base = pl.multiple_of(lax.div(length, 16) * 16, 16)
            tile = keys[slot, i, pl.ds(base, 16), :].astype(f32)
            sub = lax.broadcasted_iota(jnp.int32, (16, rank), 0)
            keys[slot, i, pl.ds(base, 16), :] = jnp.where(sub == length - base, lat_row[pl.ds(b, 1), :], tile).astype(bf16)
        for i, b in enumerate(picks):
            length = lens_ref[b]
            mine = pl.ds(pl.multiple_of(b * heads, heads), heads)
            q_lat = jnp.concatenate([qs[part, mine, :] for part in range(rank // 128)], axis=1).astype(bf16)
            q_rot = qr[mine, :]
            score = lax.dot_general(q_lat, keys[slot, i, :span], (((1,), (1,)), ((), ())), preferred_element_type=f32)
            near = jnp.dot(q_rot[:, :ROPE_DIM].astype(bf16), rope[b, :, :span], preferred_element_type=f32)
            first = lax.broadcasted_iota(jnp.int32, (heads, 2 * ROPE_DIM), 1) < ROPE_DIM
            new = jnp.sum(jnp.where(first, q_rot * rope_row[pl.ds(b, 1), :], 0.0), axis=1, keepdims=True)
            at = lax.broadcasted_iota(jnp.int32, (heads, span), 1)
            score = (score + jnp.where(at == length, new, near)) * SCALE
            scores.append(jnp.where(at <= length, score, -jnp.inf))
        probs = []
        for score in scores:
            expo = jnp.exp(score - jnp.max(score, axis=1, keepdims=True))
            probs.append((expo / jnp.sum(expo, axis=1, keepdims=True)).astype(bf16))
        for i, b in enumerate(picks):
            mine = pl.ds(pl.multiple_of(b * heads, heads), heads)
            out = jnp.dot(probs[i], keys[slot, i, :span], preferred_element_type=f32)
            for part in range(rank // 128):
                qs[part, mine, :] = out[:, part * 128:(part + 1) * 128]

    def one_group(g, carry):
        per_class(g, lambda blocks: attend(g, blocks))

        @pl.when(g + SLOTS < groups)
        def _():
            start_group(g + SLOTS)

        @pl.when(g == groups - SLOTS - 2)
        def _():
            for copy in late_copies:
                copy.start()

        return carry

    lax.fori_loop(0, groups, one_group, 0)

    late_copies[0].wait()
    for head in range(heads):
        cols = slice(head * VAL_DIM, (head + 1) * VAL_DIM)
        lat_out = jnp.concatenate([qs[part, pl.ds(head, rows, stride=heads), :] for part in range(rank // 128)], axis=1).astype(bf16)
        heads_out[:, cols] = jnp.dot(lat_out, wv[:, cols], preferred_element_type=f32).astype(bf16)
    square = jnp.zeros((rows, 1), f32)
    for n in range(width // 512):
        cols = slice(n * 512, (n + 1) * 512)
        late_copies[1 + n].wait()
        attn_out = jnp.dot(heads_out[...], wo[n], preferred_element_type=f32)
        resid = (hidden_ref[:, cols].astype(f32) + attn_out).astype(bf16)
        resid_ref[:, cols] = resid
        square = square + jnp.sum(resid.astype(f32) * resid.astype(f32), axis=-1, keepdims=True)
    inv_rms = lax.rsqrt(square * (1.0 / width) + EPS)
    mlp_in_ref[...] = (resid_ref[...].astype(f32) * inv_rms * mlp_gain[...].astype(f32)[None]).astype(bf16)


def attention_block(hidden, cache_lat, cache_rope, seq_lens, attn_norm, w_query, w_kv_down, kv_norm, w_key_up, w_val_up, w_out, mlp_norm):
    rows, width = hidden.shape
    slots, rank = cache_lat.shape[1:]
    bf16, f32 = jnp.bfloat16, jnp.float32
    heads = w_key_up.shape[1] // NOPE_DIM
    q_width = w_query.shape[1]
    vmem = pl.BlockSpec(memory_space=pltpu.VMEM)
    hbm = pl.BlockSpec(memory_space=pl.ANY)
    smem = pl.BlockSpec(memory_space=pltpu.SMEM)
    dma = pltpu.SemaphoreType.DMA
    flops = 2 * rows * (width * (q_width + rank + ROPE_DIM + width) + heads * rank * (NOPE_DIM + VAL_DIM) + heads * slots * (2 * rank + ROPE_DIM))
    moved = 2 * (width * (q_width + rank + ROPE_DIM + width) + heads * rank * (NOPE_DIM + VAL_DIM) + rows * slots * (rank + ROPE_DIM))
    return pl.pallas_call(
        attn_kernel,
        out_shape=(
            jax.ShapeDtypeStruct((rows, width), bf16),
            jax.ShapeDtypeStruct((rows, width), bf16),
            jax.ShapeDtypeStruct((rows, rank), bf16),
            jax.ShapeDtypeStruct((rows, ROPE_DIM), bf16),
        ),
        in_specs=[smem] + [vmem] * 5 + [hbm] * 7,
        out_specs=(vmem,) * 4,
        scratch_shapes=[
            pltpu.VMEM((SLOTS, GROUP, slots, rank), bf16),
            pltpu.VMEM((rows, ROPE_DIM, slots), bf16),
            pltpu.VMEM((Q_CHUNKS, width, q_width // Q_CHUNKS), bf16),
            pltpu.VMEM((rank + ROPE_DIM, width), bf16),
            pltpu.VMEM((rank, heads * NOPE_DIM), bf16),
            pltpu.VMEM((rank, heads * VAL_DIM), bf16),
            pltpu.VMEM((width // 512, heads * VAL_DIM, 512), bf16),
            pltpu.VMEM((rows, width), bf16),
            pltpu.VMEM((rank // 128, rows * heads, 128), f32),
            pltpu.VMEM((rows * heads, 2 * ROPE_DIM), f32),
            pltpu.VMEM((rows, rank), f32),
            pltpu.VMEM((rows, 2 * ROPE_DIM), f32),
            pltpu.VMEM((rows, heads * VAL_DIM), bf16),
            pltpu.SMEM((rows,), jnp.int32),
            dma((SLOTS, GROUP)),
            dma((4 + Q_CHUNKS + width // 512,)),
        ],
        compiler_params=pltpu.CompilerParams(vmem_limit_bytes=VMEM_LIMIT),
        cost_estimate=pl.CostEstimate(flops=flops, bytes_accessed=moved, transcendentals=rows * heads * slots),
        name='latent_attention',
    )(seq_lens, hidden, seq_lens, attn_norm, kv_norm, mlp_norm, cache_lat, jnp.swapaxes(cache_rope, 1, 2), w_query, w_kv_down.T, w_key_up, w_val_up, w_out)


MESH = pl.DeviceIdType.MESH
NSUB = 2
NRS = 8
STRIP = 512
HALVES = 2
TURN = 128


def mlp_kernel(g_ref, resid_ref, wg_hbm, wu_hbm, wd_hbm, out_ref,
               g_all, wg_rows, wu_rows, wg, wu, wd, act, pown, psend, precv, rsend, rrecv_e, rrecv_m,
               w_sem, d_sem, ag_recv, ag_recv_d, ag_send_e, ag_send_m, ag_send_d,
               rd_recv, rd_send, rs_recv_e, rs_recv_m, rs_send):
    ffn = wd.shape[0]
    padded = wg.shape[1]
    rows, width = g_ref.shape
    sub = rows // NSUB
    rsub = rows // NRS
    me = lax.axis_index('tp')
    z = lax.div(me, 2)
    c = lax.rem(me, 2)
    upper = z >= 2
    is_end = jnp.logical_or(z == 0, z == 3)
    is_int = jnp.logical_not(is_end)

    def mir(k):
        return jnp.where(upper, k, 3 - k)

    partner = 2 * z + (1 - c)
    dev_e = jnp.where(is_end, me, 2 * mir(3) + c)
    dev_m = 2 * jnp.where(is_end, mir(2), mir(1)) + c

    turns = padded // TURN
    last = ffn - (turns - 1) * TURN

    def w_piece(src, dst, idx, at, count):
        return pltpu.make_async_copy(src.at[pl.ds(at * TURN, count)], dst.at[pl.ds(at * TURN, count)], w_sem.at[idx, at])

    def w_both(at, count):
        return [w_piece(wg_hbm, wg_rows, 0, at, count), w_piece(wu_hbm, wu_rows, 1, at, count)]

    down_copy = pltpu.make_async_copy(wd_hbm, wd, d_sem)

    def start_piece(at, carry):
        for copy in w_both(at, TURN):
            copy.start()
        return carry

    lax.fori_loop(0, turns - 1, start_piece, 0)
    for copy in w_both(turns - 1, last):
        copy.start()
    down_copy.start()

    barrier = pltpu.get_barrier_semaphore()
    pl.semaphore_signal(barrier, inc=1, device_id={'tp': partner}, device_id_type=MESH)
    pl.semaphore_signal(barrier, inc=1, device_id={'tp': dev_m}, device_id_type=MESH)

    @pl.when(is_int)
    def _():
        pl.semaphore_signal(barrier, inc=1, device_id={'tp': dev_e}, device_id_type=MESH)
        pl.semaphore_wait(barrier, 3)

    @pl.when(is_end)
    def _():
        pl.semaphore_wait(barrier, 2)

    def remote(src, dst, send_sem, recv_sem, dev):
        return pltpu.make_async_remote_copy(src_ref=src, dst_ref=dst, send_sem=send_sem, recv_sem=recv_sem, device_id={'tp': dev}, device_id_type=MESH)

    def ag_copy(src, chip, k, send_sem, dev):
        return remote(src, g_all.at[chip, 0, pl.ds(k * sub, sub)], send_sem.at[chip, k], ag_recv.at[chip, k], dev)

    def ag_d2d(src, chip, k):
        return remote(src, g_all.at[chip, 1, pl.ds(k * sub, sub)], ag_send_d.at[chip, k], ag_recv_d.at[chip, k], partner)

    for k in range(NSUB):
        piece = g_ref.at[pl.ds(k * sub, sub)]
        ag_copy(piece, z, k, ag_send_m, dev_m).start()

        @pl.when(is_int)
        def _():
            ag_copy(piece, z, k, ag_send_e, dev_e).start()

        ag_d2d(piece, z, k).start()
    g_all[z, 0] = g_ref[...]

    def landed(chip, k):
        return g_all.at[chip, 0, pl.ds(k * sub, sub)]

    def arrive(chip, k, send_sem, dev):
        src = landed(chip, k)
        ag_copy(src, chip, k, ag_send_d, dev_m).wait_recv()
        if dev is not None:
            ag_copy(src, chip, k, send_sem, dev).start()
        ag_d2d(src, chip, k).start()

    def both(chip):
        for k in range(NSUB):
            ag_d2d(landed(chip, k), chip, k).wait_recv()

    def rd_copy(chip, part):
        span = pl.ds(pl.multiple_of(part * (width // HALVES), width // HALVES), width // HALVES)
        return remote(psend.at[chip, :, span], precv.at[chip, :, span], rd_send.at[chip, part], rd_recv.at[chip, part], partner)

    def rd_wait(chip):
        for part in range(HALVES):
            rd_copy(chip, part).wait_recv()

    def rs_copy(chip, k, dst, recv_sem, dev):
        span = pl.ds(k * rsub, rsub)
        return remote(rsend.at[chip, span], dst.at[chip, span], rs_send.at[chip, k], recv_sem.at[chip, k], dev)

    def rs_base(chip, k):
        span = pl.ds(k * rsub, rsub)
        return pown[chip, span] + precv[chip, span].astype(jnp.float32)

    def end_send(chip):
        rd_wait(chip)
        for k in range(NRS):
            rsend[chip, pl.ds(k * rsub, rsub)] = rs_base(chip, k).astype(jnp.bfloat16)
            rs_copy(chip, k, rrecv_e, rs_recv_e, dev_m).start()

    def hook(step, strip):
        def at(role, want_step, want_strip, fn):
            if strip == want_strip:
                pl.when(jnp.logical_and(role, step == want_step))(fn)

        at(is_int, 0, 1, lambda: arrive(mir(0), 0, ag_send_e, dev_e))
        at(is_int, 1, 0, lambda: arrive(mir(0), 1, ag_send_e, dev_e))
        at(is_end, 0, 0, lambda: arrive(mir(1), 0, None, None))
        at(is_end, 1, 0, lambda: end_send(mir(2)))
        at(is_end, 1, 1, lambda: arrive(mir(0), 0, None, None))
        at(is_end, 2, 0, lambda: end_send(mir(1)))
        at(is_end, 3, 0, lambda: end_send(mir(0)))

    def swiglu(lhs, span):
        gate = jnp.dot(lhs, wg[:, span], preferred_element_type=jnp.float32)
        up = jnp.dot(lhs, wu[:, span], preferred_element_type=jnp.float32)
        return (gate / (1.0 + jnp.exp(-gate)) * up).astype(jnp.bfloat16)

    def first_arrivals(k):
        @pl.when(is_int)
        def _():
            arrive(mir(3), k, ag_send_m, dev_m)
            arrive(mir(1), k, ag_send_e, dev_e)

        @pl.when(is_end)
        def _():
            arrive(mir(2), k, None, None)

    def turn(at, carry):
        span = pl.ds(pl.multiple_of(at * TURN, TURN), TURN)
        for copy in w_both(at, TURN):
            copy.wait()
        wg[:, span] = wg_rows[span].T
        wu[:, span] = wu_rows[span].T
        pl.when(at == turns // 2)(lambda: first_arrivals(0))
        return carry

    lax.fori_loop(0, turns - 1, turn, 0)
    for copy in w_both(turns - 1, last):
        copy.wait()
    tail = slice((turns - 1) * TURN, padded)
    for src in (wg_rows, wu_rows):
        src[ffn:] = jnp.zeros((padded - ffn, width), jnp.bfloat16)
    wg[:, tail] = wg_rows[tail].T
    wu[:, tail] = wu_rows[tail].T
    first_arrivals(1)


    def one_step(step, carry):
        chip = mir(jnp.where(is_end, lax.rem(6 - step, 4), jnp.where(step == 0, 2, jnp.where(step == 1, 3, 3 - step))))

        @pl.when(jnp.logical_and(step == 1, is_end))
        def _():
            arrive(mir(1), 1, None, None)

        @pl.when(jnp.logical_and(step == 2, is_end))
        def _():
            arrive(mir(0), 1, None, None)

        both(chip)

        for strip, at in enumerate(range(0, padded, STRIP)):
            span = slice(at, min(at + STRIP, padded))
            act[:, span] = swiglu(g_all[chip].reshape(2 * rows, width), span)
            hook(step, strip)

        @pl.when(step == 0)
        def _():
            down_copy.wait()

        def one_part(part, carry):
            wide = width // HALVES
            span = pl.ds(pl.multiple_of(part * wide, wide), wide)
            down = jnp.dot(act[:, :ffn], wd[:, span], preferred_element_type=jnp.float32)
            psend[chip, :, span] = down[rows:].astype(jnp.bfloat16)
            pown[chip, :, span] = down[:rows]
            rd_copy(chip, part).start()
            return carry

        lax.fori_loop(0, HALVES, one_part, 0)
        return carry

    lax.fori_loop(0, 4, one_step, 0)

    @pl.when(is_end)
    def _():
        rd_wait(z)
        base = pown[z] + precv[z].astype(jnp.float32) + resid_ref[...].astype(jnp.float32)
        pown[z] = base
        for k in range(NRS):
            span = pl.ds(k * rsub, rsub)
            rs_copy(z, k, rrecv_m, rs_recv_m, dev_m).wait_recv()
            out_ref[span] = (pown[z, span] + rrecv_m[z, span].astype(jnp.float32)).astype(jnp.bfloat16)

    @pl.when(is_int)
    def _():
        def pass_on(chip, dst_in, sem_in, dst_out, sem_out, dev):
            rd_wait(chip)
            for k in range(NRS):
                span = pl.ds(k * rsub, rsub)
                rs_copy(chip, k, dst_in, sem_in, dev_m).wait_recv()
                rsend[chip, span] = (rs_base(chip, k) + dst_in[chip, span].astype(jnp.float32)).astype(jnp.bfloat16)
                rs_copy(chip, k, dst_out, sem_out, dev).start()

        def own_send(chip):
            pass_on(chip, rrecv_e, rs_recv_e, rrecv_m, rs_recv_m, dev_m)

        own_send(mir(1))
        rd_wait(z)
        for k in range(NRS):
            rs_copy(z, k, rrecv_e, rs_recv_e, dev_m).wait_recv()
        pown[z] = pown[z] + precv[z].astype(jnp.float32) + resid_ref[...].astype(jnp.float32) + rrecv_e[z].astype(jnp.float32)
        own_send(mir(0))
        for k in range(NRS):
            span = pl.ds(k * rsub, rsub)
            rs_copy(z, k, rrecv_m, rs_recv_m, dev_m).wait_recv()
            out_ref[span] = (pown[z, span] + rrecv_m[z, span].astype(jnp.float32)).astype(jnp.bfloat16)
        pass_on(mir(3), rrecv_m, rs_recv_m, rrecv_m, rs_recv_m, dev_e)

    for k in range(NSUB):
        for chip in range(4):
            ag_d2d(landed(chip, k), chip, k).wait_send()
        ag_copy(landed(z, k), z, k, ag_send_m, dev_m).wait_send()

        @pl.when(is_int)
        def _():
            ag_copy(landed(z, k), z, k, ag_send_e, dev_e).wait_send()
            ag_copy(landed(mir(3), k), mir(3), k, ag_send_m, dev_m).wait_send()
            ag_copy(landed(mir(1), k), mir(1), k, ag_send_e, dev_e).wait_send()
            ag_copy(landed(mir(0), k), mir(0), k, ag_send_e, dev_e).wait_send()

    for chip in range(4):
        for part in range(HALVES):
            rd_copy(chip, part).wait_send()

        @pl.when(chip != z)
        def _():
            for k in range(NRS):
                rs_copy(chip, k, rrecv_m, rs_recv_m, dev_m).wait_send()


def mlp_block(mlp_in, resid, w_gate_t, w_up_t, w_down):
    rows, width = mlp_in.shape
    ffn = w_gate_t.shape[0]
    padded = -(-ffn // TURN) * TURN
    bf16, f32 = jnp.bfloat16, jnp.float32
    vmem = pl.BlockSpec(memory_space=pltpu.VMEM)
    hbm = pl.BlockSpec(memory_space=pl.ANY)
    dma = pltpu.SemaphoreType.DMA
    flops = 3 * 2 * 8 * rows * width * ffn
    return pl.pallas_call(
        mlp_kernel,
        out_shape=jax.ShapeDtypeStruct((rows, width), bf16),
        in_specs=[vmem, vmem, hbm, hbm, hbm],
        out_specs=vmem,
        scratch_shapes=[
            pltpu.VMEM((4, 2, rows, width), bf16),
            pltpu.VMEM((padded, width), bf16),
            pltpu.VMEM((padded, width), bf16),
            pltpu.VMEM((width, padded), bf16),
            pltpu.VMEM((width, padded), bf16),
            pltpu.VMEM((ffn, width), bf16),
            pltpu.VMEM((2 * rows, padded), bf16),
            pltpu.VMEM((4, rows, width), f32),
            pltpu.VMEM((4, rows, width), bf16),
            pltpu.VMEM((4, rows, width), bf16),
            pltpu.VMEM((4, rows, width), bf16),
            pltpu.VMEM((4, rows, width), bf16),
            pltpu.VMEM((4, rows, width), bf16),
            dma((2, padded // TURN)),
            dma,
            dma((4, NSUB)), dma((4, NSUB)), dma((4, NSUB)), dma((4, NSUB)), dma((4, NSUB)),
            dma((4, HALVES)), dma((4, HALVES)),
            dma((4, NRS)), dma((4, NRS)), dma((4, NRS)),
        ],
        compiler_params=pltpu.CompilerParams(collective_id=0, has_side_effects=True, vmem_limit_bytes=60 * 1024 * 1024),
        cost_estimate=pl.CostEstimate(flops=flops, bytes_accessed=3 * 2 * ffn * width, transcendentals=8 * rows * ffn),
        name='mlp_exchange',
    )(mlp_in, resid, w_gate_t, w_up_t, w_down)


def solution(mesh):
    rows_spec = P(('dp', 'tp'), None)
    cache_spec = P(('dp', 'tp'), None, None)
    whole = P()
    in_specs = (rows_spec, cache_spec, cache_spec, P(('dp', 'tp')), whole, whole, whole, whole, whole, whole, whole, whole, P(None, 'tp'), P(None, 'tp'), P('tp', None))
    out_specs = (rows_spec, rows_spec, rows_spec)

    def device_step(hidden, cache_lat, cache_rope, seq_lens, attn_norm, w_query, w_kv_down, kv_norm, w_key_up, w_val_up, w_out, mlp_norm, w_gate, w_up, w_down):
        resid, mlp_in, lat_new, rope_new = attention_block(hidden, cache_lat, cache_rope, seq_lens, attn_norm, w_query, w_kv_down, kv_norm, w_key_up, w_val_up, w_out, mlp_norm)
        out_hidden = mlp_block(mlp_in, resid, w_gate.T, w_up.T, w_down)
        return out_hidden, lat_new, rope_new

    return jax.shard_map(device_step, mesh=mesh, in_specs=in_specs, out_specs=out_specs, check_vma=False)
```

```python
import math

import jax
import jax.numpy as jnp
from jax import lax
from jax.experimental import pallas as pl
from jax.experimental.pallas import tpu as pltpu
from jax.sharding import PartitionSpec as P

EPS = 1e-6
ROPE_BASE = 10000.0
ROPE_DIM = 64
NOPE_DIM = 128
VAL_DIM = 128
SCALE = (NOPE_DIM + ROPE_DIM) ** -0.5


GROUP = 8
SLOTS = 4
LAG = 2
BLOCK = 128
Q_CHUNKS = 4
VMEM_LIMIT = 63 * 1024 * 1024


def attn_kernel(lens_ref, hidden_ref, lens_vec, attn_gain, kv_gain, mlp_gain, lat_hbm, rope_hbm, wq_hbm, wkv_hbm, wk_hbm, wv_hbm, wo_hbm,
                resid_ref, mlp_in_ref, lat_new_ref, rope_new_ref,
                keys, rope, wq, wkv, wk, wv, wo, normed, qs, qr, lat_row, rope_row, heads_out, order, key_sem, w_sem):
    f32, bf16 = jnp.float32, jnp.bfloat16
    rows, width = hidden_ref.shape
    rank = wk.shape[0]
    heads = wk.shape[1] // NOPE_DIM
    groups = rows // GROUP
    classes = keys.shape[2] // BLOCK

    chunk = wq.shape[2]
    w_copies = [pltpu.make_async_copy(wkv_hbm, wkv, w_sem.at[0]), pltpu.make_async_copy(wk_hbm, wk, w_sem.at[1])]
    w_copies += [pltpu.make_async_copy(wq_hbm.at[:, pl.ds(j * chunk, chunk)], wq.at[j], w_sem.at[2 + j]) for j in range(Q_CHUNKS)]
    rope_copy = pltpu.make_async_copy(rope_hbm, rope, w_sem.at[2 + Q_CHUNKS])
    late_copies = [pltpu.make_async_copy(wv_hbm, wv, w_sem.at[3 + Q_CHUNKS])]
    late_copies += [pltpu.make_async_copy(wo_hbm.at[:, pl.ds(n * 512, 512)], wo.at[n], w_sem.at[4 + Q_CHUNKS + n]) for n in range(width // 512)]
    for copy in w_copies:
        copy.start()
    rope_copy.start()

    def kind(b):
        return lax.div(lens_ref[b], BLOCK)

    def count(b, counts):
        k = kind(b)
        return tuple(n + jnp.where(k == i, 1, 0) for i, n in enumerate(counts))

    zero = jnp.int32(0)
    counts = lax.fori_loop(0, rows, count, (zero,) * classes)
    firsts = []
    total = zero
    for i in reversed(range(classes)):
        firsts.append(total)
        total = total + counts[i]
    firsts = tuple(reversed(firsts))

    def place(b, firsts):
        k = kind(b)
        at = firsts[0]
        for i in range(1, classes):
            at = jnp.where(k == i, firsts[i], at)
        order[at] = b
        return tuple(n + jnp.where(k == i, 1, 0) for i, n in enumerate(firsts))

    lax.fori_loop(0, rows, place, firsts)

    def group_copies(g, blocks):
        slot = lax.rem(g, SLOTS)
        return [pltpu.make_async_copy(lat_hbm.at[order[g * GROUP + i], pl.ds(0, blocks * BLOCK)], keys.at[slot, i, pl.ds(0, blocks * BLOCK)], key_sem.at[slot, i]) for i in range(GROUP)]

    def per_class(g, fn):
        k = kind(order[g * GROUP])
        for i in range(classes):
            @pl.when(k == i)
            def _():
                fn(i + 1)

    def start_group(g):
        def start(blocks):
            for copy in group_copies(g, blocks):
                copy.start()

        per_class(g, start)

    def start_first(g, carry):
        start_group(g)
        return carry

    lax.fori_loop(0, SLOTS, start_first, 0)

    vals = hidden_ref[...].astype(f32)
    inv_rms = lax.rsqrt(jnp.mean(vals * vals, axis=-1, keepdims=True) + EPS)
    normed[...] = (vals * inv_rms * attn_gain[...].astype(f32)[None]).astype(bf16)

    lane = lax.broadcasted_iota(jnp.int32, (rows, 2 * ROPE_DIM), 1)
    half = ROPE_DIM // 2
    freq = jnp.exp(lax.rem(lane, half).astype(f32) * (-math.log(ROPE_BASE) / half))
    square_ids = (rows, rows)
    diagonal = lax.broadcasted_iota(jnp.int32, square_ids, 0) == lax.broadcasted_iota(jnp.int32, square_ids, 1)
    lens = jnp.sum(jnp.where(diagonal, lens_vec[...].astype(f32)[None], 0.0), axis=1, keepdims=True)
    angles = lens * freq
    cos_tab = jnp.cos(angles)
    is_first = lax.rem(lane, ROPE_DIM) < half
    sin_tab = jnp.where(is_first, -jnp.sin(angles), jnp.sin(angles))

    def rotate_pair(pair):
        swapped = jnp.where(is_first, pltpu.roll(pair, 2 * ROPE_DIM - half, 1), pltpu.roll(pair, half, 1))
        return (pair * cos_tab + swapped * sin_tab).astype(bf16).astype(f32)

    w_copies[0].wait()
    kv = lax.dot_general(normed[...], wkv[...], (((1,), (1,)), ((), ())), preferred_element_type=f32).astype(bf16).astype(f32)
    lat = kv[:, :rank]
    inv_lat = lax.rsqrt(jnp.mean(lat * lat, axis=-1, keepdims=True) + EPS)
    lat_new = (lat * inv_lat * kv_gain[...].astype(f32)[None]).astype(bf16)
    lat_new_ref[...] = lat_new
    lat_row[...] = lat_new.astype(f32)
    pe = kv[:, rank:]
    rope_new = rotate_pair(jnp.concatenate([pe, pe], axis=1))
    rope_new_ref[...] = rope_new[:, :ROPE_DIM].astype(bf16)
    rope_row[...] = rope_new

    w_copies[1].wait()
    low = lane < ROPE_DIM

    def put_head(head, nope, pe_rot):
        key_up = wk[:, head * NOPE_DIM:(head + 1) * NOPE_DIM]
        q_lat = lax.dot_general(nope.astype(bf16), key_up, (((1,), (1,)), ((), ())), preferred_element_type=f32).astype(bf16).astype(f32)
        for part in range(rank // 128):
            qs[part, pl.ds(head, rows, stride=heads), :] = q_lat[:, part * 128:(part + 1) * 128]
        qr[pl.ds(head, rows, stride=heads), :] = pe_rot

    for j in range(Q_CHUNKS):
        w_copies[2 + j].wait()
        query = jnp.dot(normed[...], wq[j], preferred_element_type=f32).astype(bf16).astype(f32)
        for pair in range(chunk // 384):
            base = pair * 384
            part_a, part_b, part_c = (query[:, base + 128 * i:base + 128 * (i + 1)] for i in range(3))
            pe_rot = rotate_pair(jnp.where(low, part_b, part_c))
            head = (j * chunk + base) // 192
            put_head(head, part_a, pe_rot)
            put_head(head + 1, jnp.where(low, pltpu.roll(part_b, ROPE_DIM, 1), pltpu.roll(part_c, ROPE_DIM, 1)), pltpu.roll(pe_rot, ROPE_DIM, 1))

    rope_copy.wait()

    def attend(g, blocks):
        slot = lax.rem(g, SLOTS)
        span = blocks * BLOCK
        for copy in group_copies(g, blocks):
            copy.wait()
        picks = [order[g * GROUP + i] for i in range(GROUP)]
        for i, b in enumerate(picks):
            length = lens_ref[b]
            base = pl.multiple_of(lax.div(length, 16) * 16, 16)
            tile = keys[slot, i, pl.ds(base, 16), :].astype(f32)
            sub = lax.broadcasted_iota(jnp.int32, (16, rank), 0)
            keys[slot, i, pl.ds(base, 16), :] = jnp.where(sub == length - base, lat_row[pl.ds(b, 1), :], tile).astype(bf16)

        def score_of(i):
            b = picks[i]
            length = lens_ref[b]
            mine = pl.ds(pl.multiple_of(b * heads, heads), heads)
            q_lat = jnp.concatenate([qs[part, mine, :] for part in range(rank // 128)], axis=1).astype(bf16)
            q_rot = qr[mine, :]
            score = lax.dot_general(q_lat, keys[slot, i, :span], (((1,), (1,)), ((), ())), preferred_element_type=f32)
            near = jnp.dot(q_rot[:, :ROPE_DIM].astype(bf16), rope[b, :, :span], preferred_element_type=f32)
            first = lax.broadcasted_iota(jnp.int32, (heads, 2 * ROPE_DIM), 1) < ROPE_DIM
            new = jnp.sum(jnp.where(first, q_rot * rope_row[pl.ds(b, 1), :], 0.0), axis=1, keepdims=True)
            at = lax.broadcasted_iota(jnp.int32, (heads, span), 1)
            score = (score + jnp.where(at == length, new, near)) * SCALE
            return jnp.where(at <= length, score, -jnp.inf)

        def finish(i, score):
            expo = jnp.exp(score - jnp.max(score, axis=1, keepdims=True))
            prob = (expo * (1.0 / jnp.sum(expo, axis=1, keepdims=True))).astype(bf16)
            mine = pl.ds(pl.multiple_of(picks[i] * heads, heads), heads)
            out = jnp.dot(prob, keys[slot, i, :span], preferred_element_type=f32)
            for part in range(rank // 128):
                qs[part, mine, :] = out[:, part * 128:(part + 1) * 128]

        scores = {}
        for i in range(GROUP + LAG):
            if i < GROUP:
                scores[i] = score_of(i)
            if i >= LAG:
                finish(i - LAG, scores.pop(i - LAG))

    def one_group(g, carry):
        per_class(g, lambda blocks: attend(g, blocks))

        @pl.when(g + SLOTS < groups)
        def _():
            start_group(g + SLOTS)

        @pl.when(g == groups - SLOTS - 1)
        def _():
            for copy in late_copies:
                copy.start()

        return carry

    lax.fori_loop(0, groups, one_group, 0)

    late_copies[0].wait()
    for head in range(heads):
        cols = slice(head * VAL_DIM, (head + 1) * VAL_DIM)
        lat_out = jnp.concatenate([qs[part, pl.ds(head, rows, stride=heads), :] for part in range(rank // 128)], axis=1).astype(bf16)
        heads_out[:, cols] = jnp.dot(lat_out, wv[:, cols], preferred_element_type=f32).astype(bf16)
    square = jnp.zeros((rows, 1), f32)
    for n in range(width // 512):
        cols = slice(n * 512, (n + 1) * 512)
        late_copies[1 + n].wait()
        attn_out = jnp.dot(heads_out[...], wo[n], preferred_element_type=f32)
        resid = (hidden_ref[:, cols].astype(f32) + attn_out).astype(bf16)
        resid_ref[:, cols] = resid
        square = square + jnp.sum(resid.astype(f32) * resid.astype(f32), axis=-1, keepdims=True)
    inv_rms = lax.rsqrt(square * (1.0 / width) + EPS)
    mlp_in_ref[...] = (resid_ref[...].astype(f32) * inv_rms * mlp_gain[...].astype(f32)[None]).astype(bf16)


def attention_block(hidden, cache_lat, cache_rope, seq_lens, attn_norm, w_query, w_kv_down, kv_norm, w_key_up, w_val_up, w_out, mlp_norm):
    rows, width = hidden.shape
    slots, rank = cache_lat.shape[1:]
    bf16, f32 = jnp.bfloat16, jnp.float32
    heads = w_key_up.shape[1] // NOPE_DIM
    q_width = w_query.shape[1]
    vmem = pl.BlockSpec(memory_space=pltpu.VMEM)
    hbm = pl.BlockSpec(memory_space=pl.ANY)
    smem = pl.BlockSpec(memory_space=pltpu.SMEM)
    dma = pltpu.SemaphoreType.DMA
    flops = 2 * rows * (width * (q_width + rank + ROPE_DIM + width) + heads * rank * (NOPE_DIM + VAL_DIM) + heads * slots * (2 * rank + ROPE_DIM))
    moved = 2 * (width * (q_width + rank + ROPE_DIM + width) + heads * rank * (NOPE_DIM + VAL_DIM) + rows * slots * (rank + ROPE_DIM))
    return pl.pallas_call(
        attn_kernel,
        out_shape=(
            jax.ShapeDtypeStruct((rows, width), bf16),
            jax.ShapeDtypeStruct((rows, width), bf16),
            jax.ShapeDtypeStruct((rows, rank), bf16),
            jax.ShapeDtypeStruct((rows, ROPE_DIM), bf16),
        ),
        in_specs=[smem] + [vmem] * 5 + [hbm] * 7,
        out_specs=(vmem,) * 4,
        scratch_shapes=[
            pltpu.VMEM((SLOTS, GROUP, slots, rank), bf16),
            pltpu.VMEM((rows, ROPE_DIM, slots), bf16),
            pltpu.VMEM((Q_CHUNKS, width, q_width // Q_CHUNKS), bf16),
            pltpu.VMEM((rank + ROPE_DIM, width), bf16),
            pltpu.VMEM((rank, heads * NOPE_DIM), bf16),
            pltpu.VMEM((rank, heads * VAL_DIM), bf16),
            pltpu.VMEM((width // 512, heads * VAL_DIM, 512), bf16),
            pltpu.VMEM((rows, width), bf16),
            pltpu.VMEM((rank // 128, rows * heads, 128), f32),
            pltpu.VMEM((rows * heads, 2 * ROPE_DIM), f32),
            pltpu.VMEM((rows, rank), f32),
            pltpu.VMEM((rows, 2 * ROPE_DIM), f32),
            pltpu.VMEM((rows, heads * VAL_DIM), bf16),
            pltpu.SMEM((rows,), jnp.int32),
            dma((SLOTS, GROUP)),
            dma((4 + Q_CHUNKS + width // 512,)),
        ],
        compiler_params=pltpu.CompilerParams(vmem_limit_bytes=VMEM_LIMIT),
        cost_estimate=pl.CostEstimate(flops=flops, bytes_accessed=moved, transcendentals=rows * heads * slots),
        name='latent_attention',
    )(seq_lens, hidden, seq_lens, attn_norm, kv_norm, mlp_norm, cache_lat, jnp.swapaxes(cache_rope, 1, 2), w_query, w_kv_down.T, w_key_up, w_val_up, w_out)


MESH = pl.DeviceIdType.MESH
NSUB = 2
NRS = 8
STRIP = 512
HALVES = 2
TURN = 128


def mlp_kernel(g_ref, resid_ref, wg_hbm, wu_hbm, wd_hbm, out_ref,
               g_all, wg_rows, wu_rows, wg, wu, wd, act, pown, psend, precv, rsend, rrecv_e, rrecv_m,
               w_sem, d_sem, ag_recv, ag_recv_d, ag_send_e, ag_send_m, ag_send_d,
               rd_recv, rd_send, rs_recv_e, rs_recv_m, rs_send):
    ffn = wd.shape[0]
    padded = wg.shape[1]
    rows, width = g_ref.shape
    sub = rows // NSUB
    rsub = rows // NRS
    me = lax.axis_index('tp')
    z = lax.div(me, 2)
    c = lax.rem(me, 2)
    upper = z >= 2
    is_end = jnp.logical_or(z == 0, z == 3)
    is_int = jnp.logical_not(is_end)

    def mir(k):
        return jnp.where(upper, k, 3 - k)

    partner = 2 * z + (1 - c)
    dev_e = jnp.where(is_end, me, 2 * mir(3) + c)
    dev_m = 2 * jnp.where(is_end, mir(2), mir(1)) + c

    turns = padded // TURN
    last = ffn - (turns - 1) * TURN

    def w_piece(src, dst, idx, at, count):
        return pltpu.make_async_copy(src.at[pl.ds(at * TURN, count)], dst.at[pl.ds(at * TURN, count)], w_sem.at[idx, at])

    def w_both(at, count):
        return [w_piece(wg_hbm, wg_rows, 0, at, count), w_piece(wu_hbm, wu_rows, 1, at, count)]

    down_copy = pltpu.make_async_copy(wd_hbm, wd, d_sem)

    def start_piece(at, carry):
        for copy in w_both(at, TURN):
            copy.start()
        return carry

    lax.fori_loop(0, turns - 1, start_piece, 0)
    for copy in w_both(turns - 1, last):
        copy.start()
    down_copy.start()

    barrier = pltpu.get_barrier_semaphore()
    pl.semaphore_signal(barrier, inc=1, device_id={'tp': partner}, device_id_type=MESH)
    pl.semaphore_signal(barrier, inc=1, device_id={'tp': dev_m}, device_id_type=MESH)

    @pl.when(is_int)
    def _():
        pl.semaphore_signal(barrier, inc=1, device_id={'tp': dev_e}, device_id_type=MESH)
        pl.semaphore_wait(barrier, 3)

    @pl.when(is_end)
    def _():
        pl.semaphore_wait(barrier, 2)

    def remote(src, dst, send_sem, recv_sem, dev):
        return pltpu.make_async_remote_copy(src_ref=src, dst_ref=dst, send_sem=send_sem, recv_sem=recv_sem, device_id={'tp': dev}, device_id_type=MESH)

    def ag_copy(src, chip, k, send_sem, dev):
        return remote(src, g_all.at[chip, 0, pl.ds(k * sub, sub)], send_sem.at[chip, k], ag_recv.at[chip, k], dev)

    def ag_d2d(src, chip, k):
        return remote(src, g_all.at[chip, 1, pl.ds(k * sub, sub)], ag_send_d.at[chip, k], ag_recv_d.at[chip, k], partner)

    for k in range(NSUB):
        piece = g_ref.at[pl.ds(k * sub, sub)]
        ag_copy(piece, z, k, ag_send_m, dev_m).start()

        @pl.when(is_int)
        def _():
            ag_copy(piece, z, k, ag_send_e, dev_e).start()

        ag_d2d(piece, z, k).start()
    g_all[z, 0] = g_ref[...]

    def landed(chip, k):
        return g_all.at[chip, 0, pl.ds(k * sub, sub)]

    def arrive(chip, k, send_sem, dev):
        src = landed(chip, k)
        ag_copy(src, chip, k, ag_send_d, dev_m).wait_recv()
        if dev is not None:
            ag_copy(src, chip, k, send_sem, dev).start()
        ag_d2d(src, chip, k).start()

    def both(chip):
        for k in range(NSUB):
            ag_d2d(landed(chip, k), chip, k).wait_recv()

    def rd_copy(chip, part):
        span = pl.ds(part * (width // HALVES), width // HALVES)
        return remote(psend.at[chip, :, span], precv.at[chip, :, span], rd_send.at[chip, part], rd_recv.at[chip, part], partner)

    def rd_wait(chip):
        for part in range(HALVES):
            rd_copy(chip, part).wait_recv()

    def rs_copy(chip, k, dst, recv_sem, dev):
        span = pl.ds(k * rsub, rsub)
        return remote(rsend.at[chip, span], dst.at[chip, span], rs_send.at[chip, k], recv_sem.at[chip, k], dev)

    def rs_base(chip, k):
        span = pl.ds(k * rsub, rsub)
        return pown[chip, span] + precv[chip, span].astype(jnp.float32)

    def end_send(chip):
        rd_wait(chip)
        for k in range(NRS):
            rsend[chip, pl.ds(k * rsub, rsub)] = rs_base(chip, k).astype(jnp.bfloat16)
            rs_copy(chip, k, rrecv_e, rs_recv_e, dev_m).start()

    def hook(step, strip):
        def at(role, want_step, want_strip, fn):
            if strip == want_strip:
                pl.when(jnp.logical_and(role, step == want_step))(fn)

        at(is_int, 0, 1, lambda: arrive(mir(0), 0, ag_send_e, dev_e))
        at(is_int, 1, 0, lambda: arrive(mir(0), 1, ag_send_e, dev_e))
        at(is_end, 0, 0, lambda: arrive(mir(1), 0, None, None))
        at(is_end, 1, 0, lambda: end_send(mir(2)))
        at(is_end, 1, 1, lambda: arrive(mir(0), 0, None, None))
        at(is_end, 2, 0, lambda: end_send(mir(1)))
        at(is_end, 3, 0, lambda: end_send(mir(0)))

    def swiglu(lhs, span):
        gate = jnp.dot(lhs, wg[:, span], preferred_element_type=jnp.float32)
        up = jnp.dot(lhs, wu[:, span], preferred_element_type=jnp.float32)
        return (gate / (1.0 + jnp.exp(-gate)) * up).astype(jnp.bfloat16)

    def first_arrivals(k):
        @pl.when(is_int)
        def _():
            arrive(mir(3), k, ag_send_m, dev_m)
            arrive(mir(1), k, ag_send_e, dev_e)

        @pl.when(is_end)
        def _():
            arrive(mir(2), k, None, None)

    def turn(at, carry):
        span = pl.ds(pl.multiple_of(at * TURN, TURN), TURN)
        for copy in w_both(at, TURN):
            copy.wait()
        wg[:, span] = wg_rows[span].T
        wu[:, span] = wu_rows[span].T
        pl.when(at == turns // 2)(lambda: first_arrivals(0))
        return carry

    lax.fori_loop(0, turns - 1, turn, 0)
    for copy in w_both(turns - 1, last):
        copy.wait()
    tail = slice((turns - 1) * TURN, padded)
    for src in (wg_rows, wu_rows):
        src[ffn:] = jnp.zeros((padded - ffn, width), jnp.bfloat16)
    wg[:, tail] = wg_rows[tail].T
    wu[:, tail] = wu_rows[tail].T
    first_arrivals(1)


    def one_step(step, carry):
        chip = mir(jnp.where(is_end, lax.rem(6 - step, 4), jnp.where(step == 0, 2, jnp.where(step == 1, 3, 3 - step))))

        @pl.when(jnp.logical_and(step == 1, is_end))
        def _():
            arrive(mir(1), 1, None, None)

        @pl.when(jnp.logical_and(step == 2, is_end))
        def _():
            arrive(mir(0), 1, None, None)

        both(chip)

        for strip, at in enumerate(range(0, padded, STRIP)):
            span = slice(at, min(at + STRIP, padded))
            act[:, span] = swiglu(g_all[chip].reshape(2 * rows, width), span)
            hook(step, strip)

        @pl.when(step == 0)
        def _():
            down_copy.wait()

        for part in range(HALVES):
            wide = width // HALVES
            span = slice(part * wide, (part + 1) * wide)
            down = jnp.dot(act[:, :ffn], wd[:, span], preferred_element_type=jnp.float32)
            psend[chip, :, span] = down[rows:].astype(jnp.bfloat16)
            pown[chip, :, span] = down[:rows]
            rd_copy(chip, part).start()

        return carry

    lax.fori_loop(0, 4, one_step, 0)

    @pl.when(is_end)
    def _():
        rd_wait(z)
        base = pown[z] + precv[z].astype(jnp.float32) + resid_ref[...].astype(jnp.float32)
        pown[z] = base
        for k in range(NRS):
            span = pl.ds(k * rsub, rsub)
            rs_copy(z, k, rrecv_m, rs_recv_m, dev_m).wait_recv()
            out_ref[span] = (pown[z, span] + rrecv_m[z, span].astype(jnp.float32)).astype(jnp.bfloat16)

    @pl.when(is_int)
    def _():
        def pass_on(chip, dst_in, sem_in, dst_out, sem_out, dev):
            rd_wait(chip)
            for k in range(NRS):
                span = pl.ds(k * rsub, rsub)
                rs_copy(chip, k, dst_in, sem_in, dev_m).wait_recv()
                rsend[chip, span] = (rs_base(chip, k) + dst_in[chip, span].astype(jnp.float32)).astype(jnp.bfloat16)
                rs_copy(chip, k, dst_out, sem_out, dev).start()

        def own_send(chip):
            pass_on(chip, rrecv_e, rs_recv_e, rrecv_m, rs_recv_m, dev_m)

        own_send(mir(1))
        rd_wait(z)
        for k in range(NRS):
            rs_copy(z, k, rrecv_e, rs_recv_e, dev_m).wait_recv()
        pown[z] = pown[z] + precv[z].astype(jnp.float32) + resid_ref[...].astype(jnp.float32) + rrecv_e[z].astype(jnp.float32)
        own_send(mir(0))
        for k in range(NRS):
            span = pl.ds(k * rsub, rsub)
            rs_copy(z, k, rrecv_m, rs_recv_m, dev_m).wait_recv()
            out_ref[span] = (pown[z, span] + rrecv_m[z, span].astype(jnp.float32)).astype(jnp.bfloat16)
        pass_on(mir(3), rrecv_m, rs_recv_m, rrecv_m, rs_recv_m, dev_e)

    for k in range(NSUB):
        for chip in range(4):
            ag_d2d(landed(chip, k), chip, k).wait_send()
        ag_copy(landed(z, k), z, k, ag_send_m, dev_m).wait_send()

        @pl.when(is_int)
        def _():
            ag_copy(landed(z, k), z, k, ag_send_e, dev_e).wait_send()
            ag_copy(landed(mir(3), k), mir(3), k, ag_send_m, dev_m).wait_send()
            ag_copy(landed(mir(1), k), mir(1), k, ag_send_e, dev_e).wait_send()
            ag_copy(landed(mir(0), k), mir(0), k, ag_send_e, dev_e).wait_send()

    for chip in range(4):
        for part in range(HALVES):
            rd_copy(chip, part).wait_send()

        @pl.when(chip != z)
        def _():
            for k in range(NRS):
                rs_copy(chip, k, rrecv_m, rs_recv_m, dev_m).wait_send()


def mlp_block(mlp_in, resid, w_gate_t, w_up_t, w_down):
    rows, width = mlp_in.shape
    ffn = w_gate_t.shape[0]
    padded = -(-ffn // TURN) * TURN
    bf16, f32 = jnp.bfloat16, jnp.float32
    vmem = pl.BlockSpec(memory_space=pltpu.VMEM)
    hbm = pl.BlockSpec(memory_space=pl.ANY)
    dma = pltpu.SemaphoreType.DMA
    flops = 3 * 2 * 8 * rows * width * ffn
    return pl.pallas_call(
        mlp_kernel,
        out_shape=jax.ShapeDtypeStruct((rows, width), bf16),
        in_specs=[vmem, vmem, hbm, hbm, hbm],
        out_specs=vmem,
        scratch_shapes=[
            pltpu.VMEM((4, 2, rows, width), bf16),
            pltpu.VMEM((padded, width), bf16),
            pltpu.VMEM((padded, width), bf16),
            pltpu.VMEM((width, padded), bf16),
            pltpu.VMEM((width, padded), bf16),
            pltpu.VMEM((ffn, width), bf16),
            pltpu.VMEM((2 * rows, padded), bf16),
            pltpu.VMEM((4, rows, width), f32),
            pltpu.VMEM((4, rows, width), bf16),
            pltpu.VMEM((4, rows, width), bf16),
            pltpu.VMEM((4, rows, width), bf16),
            pltpu.VMEM((4, rows, width), bf16),
            pltpu.VMEM((4, rows, width), bf16),
            dma((2, padded // TURN)),
            dma,
            dma((4, NSUB)), dma((4, NSUB)), dma((4, NSUB)), dma((4, NSUB)), dma((4, NSUB)),
            dma((4, HALVES)), dma((4, HALVES)),
            dma((4, NRS)), dma((4, NRS)), dma((4, NRS)),
        ],
        compiler_params=pltpu.CompilerParams(collective_id=0, has_side_effects=True, vmem_limit_bytes=60 * 1024 * 1024),
        cost_estimate=pl.CostEstimate(flops=flops, bytes_accessed=3 * 2 * ffn * width, transcendentals=8 * rows * ffn),
        name='mlp_exchange',
    )(mlp_in, resid, w_gate_t, w_up_t, w_down)


def solution(mesh):
    rows_spec = P(('dp', 'tp'), None)
    cache_spec = P(('dp', 'tp'), None, None)
    whole = P()
    in_specs = (rows_spec, cache_spec, cache_spec, P(('dp', 'tp')), whole, whole, whole, whole, whole, whole, whole, whole, P(None, 'tp'), P(None, 'tp'), P('tp', None))
    out_specs = (rows_spec, rows_spec, rows_spec)

    def device_step(hidden, cache_lat, cache_rope, seq_lens, attn_norm, w_query, w_kv_down, kv_norm, w_key_up, w_val_up, w_out, mlp_norm, w_gate, w_up, w_down):
        resid, mlp_in, lat_new, rope_new = attention_block(hidden, cache_lat, cache_rope, seq_lens, attn_norm, w_query, w_kv_down, kv_norm, w_key_up, w_val_up, w_out, mlp_norm)
        out_hidden = mlp_block(mlp_in, resid, w_gate.T, w_up.T, w_down)
        return out_hidden, lat_new, rope_new

    return jax.shard_map(device_step, mesh=mesh, in_specs=in_specs, out_specs=out_specs, check_vma=False)
```

```python
import math

import jax
import jax.numpy as jnp
from jax import lax
from jax.experimental import pallas as pl
from jax.experimental.pallas import tpu as pltpu
from jax.sharding import PartitionSpec as P

EPS = 1e-6
ROPE_BASE = 10000.0
ROPE_DIM = 64
NOPE_DIM = 128
VAL_DIM = 128
SCALE = (NOPE_DIM + ROPE_DIM) ** -0.5


GROUP = 8
SLOTS = 4
LAG = 2
BLOCK = 128
Q_CHUNKS = 4
VMEM_LIMIT = 63 * 1024 * 1024


def attn_kernel(lens_ref, hidden_ref, lens_vec, attn_gain, kv_gain, mlp_gain, lat_hbm, rope_hbm, wq_hbm, wkv_hbm, wk_hbm, wv_hbm, wo_hbm,
                resid_ref, mlp_in_ref, lat_new_ref, rope_new_ref,
                keys, rope, wq, wkv, wk, wv, wo, normed, qs, qr, lat_row, rope_row, heads_out, order, key_sem, w_sem):
    f32, bf16 = jnp.float32, jnp.bfloat16
    rows, width = hidden_ref.shape
    rank = wk.shape[0]
    heads = wk.shape[1] // NOPE_DIM
    groups = rows // GROUP
    classes = keys.shape[2] // BLOCK

    chunk = wq.shape[2]
    w_copies = [pltpu.make_async_copy(wkv_hbm, wkv, w_sem.at[0]), pltpu.make_async_copy(wk_hbm, wk, w_sem.at[1])]
    w_copies += [pltpu.make_async_copy(wq_hbm.at[:, pl.ds(j * chunk, chunk)], wq.at[j], w_sem.at[2 + j]) for j in range(Q_CHUNKS)]
    rope_copy = pltpu.make_async_copy(rope_hbm, rope, w_sem.at[2 + Q_CHUNKS])
    late_copies = [pltpu.make_async_copy(wv_hbm, wv, w_sem.at[3 + Q_CHUNKS])]
    late_copies += [pltpu.make_async_copy(wo_hbm.at[:, pl.ds(n * 512, 512)], wo.at[n], w_sem.at[4 + Q_CHUNKS + n]) for n in range(width // 512)]
    for copy in w_copies:
        copy.start()
    rope_copy.start()

    def kind(b):
        return lax.div(lens_ref[b], BLOCK)

    def count(b, counts):
        k = kind(b)
        return tuple(n + jnp.where(k == i, 1, 0) for i, n in enumerate(counts))

    zero = jnp.int32(0)
    counts = lax.fori_loop(0, rows, count, (zero,) * classes)
    firsts = []
    total = zero
    for i in reversed(range(classes)):
        firsts.append(total)
        total = total + counts[i]
    firsts = tuple(reversed(firsts))

    def place(b, firsts):
        k = kind(b)
        at = firsts[0]
        for i in range(1, classes):
            at = jnp.where(k == i, firsts[i], at)
        order[at] = b
        return tuple(n + jnp.where(k == i, 1, 0) for i, n in enumerate(firsts))

    lax.fori_loop(0, rows, place, firsts)

    def group_copies(g, blocks):
        slot = lax.rem(g, SLOTS)
        return [pltpu.make_async_copy(lat_hbm.at[order[g * GROUP + i], pl.ds(0, blocks * BLOCK)], keys.at[slot, i, pl.ds(0, blocks * BLOCK)], key_sem.at[slot, i]) for i in range(GROUP)]

    def per_class(g, fn):
        k = kind(order[g * GROUP])
        for i in range(classes):
            @pl.when(k == i)
            def _():
                fn(i + 1)

    def start_group(g):
        def start(blocks):
            for copy in group_copies(g, blocks):
                copy.start()

        per_class(g, start)

    def start_first(g, carry):
        start_group(g)
        return carry

    lax.fori_loop(0, SLOTS, start_first, 0)

    vals = hidden_ref[...].astype(f32)
    inv_rms = lax.rsqrt(jnp.mean(vals * vals, axis=-1, keepdims=True) + EPS)
    normed[...] = (vals * inv_rms * attn_gain[...].astype(f32)[None]).astype(bf16)

    lane = lax.broadcasted_iota(jnp.int32, (rows, 2 * ROPE_DIM), 1)
    half = ROPE_DIM // 2
    freq = jnp.exp(lax.rem(lane, half).astype(f32) * (-math.log(ROPE_BASE) / half))
    square_ids = (rows, rows)
    diagonal = lax.broadcasted_iota(jnp.int32, square_ids, 0) == lax.broadcasted_iota(jnp.int32, square_ids, 1)
    lens = jnp.sum(jnp.where(diagonal, lens_vec[...].astype(f32)[None], 0.0), axis=1, keepdims=True)
    angles = lens * freq
    cos_tab = jnp.cos(angles)
    is_first = lax.rem(lane, ROPE_DIM) < half
    sin_tab = jnp.where(is_first, -jnp.sin(angles), jnp.sin(angles))

    def rotate_pair(pair):
        swapped = jnp.where(is_first, pltpu.roll(pair, 2 * ROPE_DIM - half, 1), pltpu.roll(pair, half, 1))
        return (pair * cos_tab + swapped * sin_tab).astype(bf16).astype(f32)

    w_copies[0].wait()
    kv = lax.dot_general(normed[...], wkv[...], (((1,), (1,)), ((), ())), preferred_element_type=f32).astype(bf16).astype(f32)
    lat = kv[:, :rank]
    inv_lat = lax.rsqrt(jnp.mean(lat * lat, axis=-1, keepdims=True) + EPS)
    lat_new = (lat * inv_lat * kv_gain[...].astype(f32)[None]).astype(bf16)
    lat_new_ref[...] = lat_new
    lat_row[...] = lat_new.astype(f32)
    pe = kv[:, rank:]
    rope_new = rotate_pair(jnp.concatenate([pe, pe], axis=1))
    rope_new_ref[...] = rope_new[:, :ROPE_DIM].astype(bf16)
    rope_row[...] = rope_new

    w_copies[1].wait()
    low = lane < ROPE_DIM

    def put_head(head, nope, pe_rot):
        key_up = wk[:, head * NOPE_DIM:(head + 1) * NOPE_DIM]
        q_lat = lax.dot_general(nope.astype(bf16), key_up, (((1,), (1,)), ((), ())), preferred_element_type=f32).astype(bf16).astype(f32)
        for part in range(rank // 128):
            qs[part, pl.ds(head, rows, stride=heads), :] = q_lat[:, part * 128:(part + 1) * 128]
        qr[pl.ds(head, rows, stride=heads), :] = pe_rot

    for j in range(Q_CHUNKS):
        w_copies[2 + j].wait()
        query = jnp.dot(normed[...], wq[j], preferred_element_type=f32).astype(bf16).astype(f32)
        for pair in range(chunk // 384):
            base = pair * 384
            part_a, part_b, part_c = (query[:, base + 128 * i:base + 128 * (i + 1)] for i in range(3))
            pe_rot = rotate_pair(jnp.where(low, part_b, part_c))
            head = (j * chunk + base) // 192
            put_head(head, part_a, pe_rot)
            put_head(head + 1, jnp.where(low, pltpu.roll(part_b, ROPE_DIM, 1), pltpu.roll(part_c, ROPE_DIM, 1)), pltpu.roll(pe_rot, ROPE_DIM, 1))

    rope_copy.wait()

    def attend(g, blocks):
        slot = lax.rem(g, SLOTS)
        span = blocks * BLOCK
        for copy in group_copies(g, blocks):
            copy.wait()
        picks = [order[g * GROUP + i] for i in range(GROUP)]
        for i, b in enumerate(picks):
            length = lens_ref[b]
            base = pl.multiple_of(lax.div(length, 16) * 16, 16)
            tile = keys[slot, i, pl.ds(base, 16), :].astype(f32)
            sub = lax.broadcasted_iota(jnp.int32, (16, rank), 0)
            keys[slot, i, pl.ds(base, 16), :] = jnp.where(sub == length - base, lat_row[pl.ds(b, 1), :], tile).astype(bf16)

        def score_of(i):
            b = picks[i]
            length = lens_ref[b]
            mine = pl.ds(pl.multiple_of(b * heads, heads), heads)
            q_lat = jnp.concatenate([qs[part, mine, :] for part in range(rank // 128)], axis=1).astype(bf16)
            q_rot = qr[mine, :]
            score = lax.dot_general(q_lat, keys[slot, i, :span], (((1,), (1,)), ((), ())), preferred_element_type=f32)
            near = jnp.dot(q_rot[:, :ROPE_DIM].astype(bf16), rope[b, :, :span], preferred_element_type=f32)
            first = lax.broadcasted_iota(jnp.int32, (heads, 2 * ROPE_DIM), 1) < ROPE_DIM
            new = jnp.sum(jnp.where(first, q_rot * rope_row[pl.ds(b, 1), :], 0.0), axis=1, keepdims=True)
            at = lax.broadcasted_iota(jnp.int32, (heads, span), 1)
            score = (score + jnp.where(at == length, new, near)) * SCALE
            return jnp.where(at <= length, score, -jnp.inf)

        def finish(i, score):
            expo = jnp.exp(score - jnp.max(score, axis=1, keepdims=True))
            prob = (expo / jnp.sum(expo, axis=1, keepdims=True)).astype(bf16)
            mine = pl.ds(pl.multiple_of(picks[i] * heads, heads), heads)
            out = jnp.dot(prob, keys[slot, i, :span], preferred_element_type=f32)
            for part in range(rank // 128):
                qs[part, mine, :] = out[:, part * 128:(part + 1) * 128]

        scores = {}
        for i in range(GROUP + LAG):
            if i < GROUP:
                scores[i] = score_of(i)
            if i >= LAG:
                finish(i - LAG, scores.pop(i - LAG))

    def one_group(g, carry):
        per_class(g, lambda blocks: attend(g, blocks))

        @pl.when(g + SLOTS < groups)
        def _():
            start_group(g + SLOTS)

        @pl.when(g == groups - SLOTS - 1)
        def _():
            for copy in late_copies:
                copy.start()

        return carry

    lax.fori_loop(0, groups, one_group, 0)

    late_copies[0].wait()
    for head in range(heads):
        cols = slice(head * VAL_DIM, (head + 1) * VAL_DIM)
        lat_out = jnp.concatenate([qs[part, pl.ds(head, rows, stride=heads), :] for part in range(rank // 128)], axis=1).astype(bf16)
        heads_out[:, cols] = jnp.dot(lat_out, wv[:, cols], preferred_element_type=f32).astype(bf16)
    square = jnp.zeros((rows, 1), f32)
    for n in range(width // 512):
        cols = slice(n * 512, (n + 1) * 512)
        late_copies[1 + n].wait()
        attn_out = jnp.dot(heads_out[...], wo[n], preferred_element_type=f32)
        resid = (hidden_ref[:, cols].astype(f32) + attn_out).astype(bf16)
        resid_ref[:, cols] = resid
        square = square + jnp.sum(resid.astype(f32) * resid.astype(f32), axis=-1, keepdims=True)
    inv_rms = lax.rsqrt(square * (1.0 / width) + EPS)
    mlp_in_ref[...] = (resid_ref[...].astype(f32) * inv_rms * mlp_gain[...].astype(f32)[None]).astype(bf16)


def attention_block(hidden, cache_lat, cache_rope, seq_lens, attn_norm, w_query, w_kv_down, kv_norm, w_key_up, w_val_up, w_out, mlp_norm):
    rows, width = hidden.shape
    slots, rank = cache_lat.shape[1:]
    bf16, f32 = jnp.bfloat16, jnp.float32
    heads = w_key_up.shape[1] // NOPE_DIM
    q_width = w_query.shape[1]
    vmem = pl.BlockSpec(memory_space=pltpu.VMEM)
    hbm = pl.BlockSpec(memory_space=pl.ANY)
    smem = pl.BlockSpec(memory_space=pltpu.SMEM)
    dma = pltpu.SemaphoreType.DMA
    flops = 2 * rows * (width * (q_width + rank + ROPE_DIM + width) + heads * rank * (NOPE_DIM + VAL_DIM) + heads * slots * (2 * rank + ROPE_DIM))
    moved = 2 * (width * (q_width + rank + ROPE_DIM + width) + heads * rank * (NOPE_DIM + VAL_DIM) + rows * slots * (rank + ROPE_DIM))
    return pl.pallas_call(
        attn_kernel,
        out_shape=(
            jax.ShapeDtypeStruct((rows, width), bf16),
            jax.ShapeDtypeStruct((rows, width), bf16),
            jax.ShapeDtypeStruct((rows, rank), bf16),
            jax.ShapeDtypeStruct((rows, ROPE_DIM), bf16),
        ),
        in_specs=[smem] + [vmem] * 5 + [hbm] * 7,
        out_specs=(vmem,) * 4,
        scratch_shapes=[
            pltpu.VMEM((SLOTS, GROUP, slots, rank), bf16),
            pltpu.VMEM((rows, ROPE_DIM, slots), bf16),
            pltpu.VMEM((Q_CHUNKS, width, q_width // Q_CHUNKS), bf16),
            pltpu.VMEM((rank + ROPE_DIM, width), bf16),
            pltpu.VMEM((rank, heads * NOPE_DIM), bf16),
            pltpu.VMEM((rank, heads * VAL_DIM), bf16),
            pltpu.VMEM((width // 512, heads * VAL_DIM, 512), bf16),
            pltpu.VMEM((rows, width), bf16),
            pltpu.VMEM((rank // 128, rows * heads, 128), f32),
            pltpu.VMEM((rows * heads, 2 * ROPE_DIM), f32),
            pltpu.VMEM((rows, rank), f32),
            pltpu.VMEM((rows, 2 * ROPE_DIM), f32),
            pltpu.VMEM((rows, heads * VAL_DIM), bf16),
            pltpu.SMEM((rows,), jnp.int32),
            dma((SLOTS, GROUP)),
            dma((4 + Q_CHUNKS + width // 512,)),
        ],
        compiler_params=pltpu.CompilerParams(vmem_limit_bytes=VMEM_LIMIT),
        cost_estimate=pl.CostEstimate(flops=flops, bytes_accessed=moved, transcendentals=rows * heads * slots),
        name='latent_attention',
    )(seq_lens, hidden, seq_lens, attn_norm, kv_norm, mlp_norm, cache_lat, jnp.swapaxes(cache_rope, 1, 2), w_query, w_kv_down.T, w_key_up, w_val_up, w_out)


MESH = pl.DeviceIdType.MESH
NSUB = 2
NRS = 8
STRIP = 512
HALVES = 2
TURN = 128


def mlp_kernel(g_ref, resid_ref, wg_hbm, wu_hbm, wd_hbm, out_ref,
               g_all, wg_rows, wu_rows, wg, wu, wd, act, pown, psend, precv, rsend, rrecv_e, rrecv_m,
               w_sem, d_sem, ag_recv, ag_recv_d, ag_send_e, ag_send_m, ag_send_d,
               rd_recv, rd_send, rs_recv_e, rs_recv_m, rs_send):
    ffn = wd.shape[0]
    padded = wg.shape[1]
    rows, width = g_ref.shape
    sub = rows // NSUB
    rsub = rows // NRS
    me = lax.axis_index('tp')
    z = lax.div(me, 2)
    c = lax.rem(me, 2)
    upper = z >= 2
    is_end = jnp.logical_or(z == 0, z == 3)
    is_int = jnp.logical_not(is_end)

    def mir(k):
        return jnp.where(upper, k, 3 - k)

    partner = 2 * z + (1 - c)
    dev_e = jnp.where(is_end, me, 2 * mir(3) + c)
    dev_m = 2 * jnp.where(is_end, mir(2), mir(1)) + c

    turns = padded // TURN
    last = ffn - (turns - 1) * TURN

    def w_piece(src, dst, idx, at, count):
        return pltpu.make_async_copy(src.at[pl.ds(at * TURN, count)], dst.at[pl.ds(at * TURN, count)], w_sem.at[idx, at])

    def w_both(at, count):
        return [w_piece(wg_hbm, wg_rows, 0, at, count), w_piece(wu_hbm, wu_rows, 1, at, count)]

    down_copy = pltpu.make_async_copy(wd_hbm, wd, d_sem)

    def start_piece(at, carry):
        for copy in w_both(at, TURN):
            copy.start()
        return carry

    lax.fori_loop(0, turns - 1, start_piece, 0)
    for copy in w_both(turns - 1, last):
        copy.start()
    down_copy.start()

    barrier = pltpu.get_barrier_semaphore()
    pl.semaphore_signal(barrier, inc=1, device_id={'tp': partner}, device_id_type=MESH)
    pl.semaphore_signal(barrier, inc=1, device_id={'tp': dev_m}, device_id_type=MESH)

    @pl.when(is_int)
    def _():
        pl.semaphore_signal(barrier, inc=1, device_id={'tp': dev_e}, device_id_type=MESH)
        pl.semaphore_wait(barrier, 3)

    @pl.when(is_end)
    def _():
        pl.semaphore_wait(barrier, 2)

    def remote(src, dst, send_sem, recv_sem, dev):
        return pltpu.make_async_remote_copy(src_ref=src, dst_ref=dst, send_sem=send_sem, recv_sem=recv_sem, device_id={'tp': dev}, device_id_type=MESH)

    def ag_copy(src, chip, k, send_sem, dev):
        return remote(src, g_all.at[chip, 0, pl.ds(k * sub, sub)], send_sem.at[chip, k], ag_recv.at[chip, k], dev)

    def ag_d2d(src, chip, k):
        return remote(src, g_all.at[chip, 1, pl.ds(k * sub, sub)], ag_send_d.at[chip, k], ag_recv_d.at[chip, k], partner)

    for k in range(NSUB):
        piece = g_ref.at[pl.ds(k * sub, sub)]
        ag_copy(piece, z, k, ag_send_m, dev_m).start()

        @pl.when(is_int)
        def _():
            ag_copy(piece, z, k, ag_send_e, dev_e).start()

        ag_d2d(piece, z, k).start()
    g_all[z, 0] = g_ref[...]

    def landed(chip, k):
        return g_all.at[chip, 0, pl.ds(k * sub, sub)]

    def arrive(chip, k, send_sem, dev):
        src = landed(chip, k)
        ag_copy(src, chip, k, ag_send_d, dev_m).wait_recv()
        if dev is not None:
            ag_copy(src, chip, k, send_sem, dev).start()
        ag_d2d(src, chip, k).start()

    def both(chip):
        for k in range(NSUB):
            ag_d2d(landed(chip, k), chip, k).wait_recv()

    def rd_copy(chip, part):
        span = pl.ds(part * (width // HALVES), width // HALVES)
        return remote(psend.at[chip, :, span], precv.at[chip, :, span], rd_send.at[chip, part], rd_recv.at[chip, part], partner)

    def rd_wait(chip):
        for part in range(HALVES):
            rd_copy(chip, part).wait_recv()

    def rs_copy(chip, k, dst, recv_sem, dev):
        span = pl.ds(k * rsub, rsub)
        return remote(rsend.at[chip, span], dst.at[chip, span], rs_send.at[chip, k], recv_sem.at[chip, k], dev)

    def rs_base(chip, k):
        span = pl.ds(k * rsub, rsub)
        return pown[chip, span] + precv[chip, span].astype(jnp.float32)

    def end_send(chip):
        rd_wait(chip)
        for k in range(NRS):
            rsend[chip, pl.ds(k * rsub, rsub)] = rs_base(chip, k).astype(jnp.bfloat16)
            rs_copy(chip, k, rrecv_e, rs_recv_e, dev_m).start()

    def hook(step, strip):
        def at(role, want_step, want_strip, fn):
            if strip == want_strip:
                pl.when(jnp.logical_and(role, step == want_step))(fn)

        at(is_int, 0, 1, lambda: arrive(mir(0), 0, ag_send_e, dev_e))
        at(is_int, 1, 0, lambda: arrive(mir(0), 1, ag_send_e, dev_e))
        at(is_end, 0, 0, lambda: arrive(mir(1), 0, None, None))
        at(is_end, 1, 0, lambda: end_send(mir(2)))
        at(is_end, 1, 1, lambda: arrive(mir(0), 0, None, None))
        at(is_end, 2, 0, lambda: end_send(mir(1)))
        at(is_end, 3, 0, lambda: end_send(mir(0)))

    def swiglu(lhs, span):
        gate = jnp.dot(lhs, wg[:, span], preferred_element_type=jnp.float32)
        up = jnp.dot(lhs, wu[:, span], preferred_element_type=jnp.float32)
        return (gate / (1.0 + jnp.exp(-gate)) * up).astype(jnp.bfloat16)

    def first_arrivals(k):
        @pl.when(is_int)
        def _():
            arrive(mir(3), k, ag_send_m, dev_m)
            arrive(mir(1), k, ag_send_e, dev_e)

        @pl.when(is_end)
        def _():
            arrive(mir(2), k, None, None)

    def turn(at, carry):
        span = pl.ds(pl.multiple_of(at * TURN, TURN), TURN)
        for copy in w_both(at, TURN):
            copy.wait()
        wg[:, span] = wg_rows[span].T
        wu[:, span] = wu_rows[span].T
        pl.when(at == turns // 2)(lambda: first_arrivals(0))
        return carry

    lax.fori_loop(0, turns - 1, turn, 0)
    for copy in w_both(turns - 1, last):
        copy.wait()
    tail = slice((turns - 1) * TURN, padded)
    for src in (wg_rows, wu_rows):
        src[ffn:] = jnp.zeros((padded - ffn, width), jnp.bfloat16)
    wg[:, tail] = wg_rows[tail].T
    wu[:, tail] = wu_rows[tail].T
    first_arrivals(1)


    def one_step(step, carry):
        chip = mir(jnp.where(is_end, lax.rem(6 - step, 4), jnp.where(step == 0, 2, jnp.where(step == 1, 3, 3 - step))))

        @pl.when(jnp.logical_and(step == 1, is_end))
        def _():
            arrive(mir(1), 1, None, None)

        @pl.when(jnp.logical_and(step == 2, is_end))
        def _():
            arrive(mir(0), 1, None, None)

        both(chip)

        for strip, at in enumerate(range(0, padded, STRIP)):
            span = slice(at, min(at + STRIP, padded))
            act[:, span] = swiglu(g_all[chip].reshape(2 * rows, width), span)
            hook(step, strip)

        @pl.when(step == 0)
        def _():
            down_copy.wait()

        for part in range(HALVES):
            wide = width // HALVES
            span = slice(part * wide, (part + 1) * wide)
            down = jnp.dot(act[:, :ffn], wd[:, span], preferred_element_type=jnp.float32)
            psend[chip, :, span] = down[rows:].astype(jnp.bfloat16)
            pown[chip, :, span] = down[:rows]
            rd_copy(chip, part).start()

        return carry

    lax.fori_loop(0, 4, one_step, 0)

    @pl.when(is_end)
    def _():
        rd_wait(z)
        base = pown[z] + precv[z].astype(jnp.float32) + resid_ref[...].astype(jnp.float32)
        pown[z] = base
        for k in range(NRS):
            span = pl.ds(k * rsub, rsub)
            rs_copy(z, k, rrecv_m, rs_recv_m, dev_m).wait_recv()
            out_ref[span] = (pown[z, span] + rrecv_m[z, span].astype(jnp.float32)).astype(jnp.bfloat16)

    @pl.when(is_int)
    def _():
        def pass_on(chip, dst_in, sem_in, dst_out, sem_out, dev):
            rd_wait(chip)
            for k in range(NRS):
                span = pl.ds(k * rsub, rsub)
                rs_copy(chip, k, dst_in, sem_in, dev_m).wait_recv()
                rsend[chip, span] = (rs_base(chip, k) + dst_in[chip, span].astype(jnp.float32)).astype(jnp.bfloat16)
                rs_copy(chip, k, dst_out, sem_out, dev).start()

        def own_send(chip):
            pass_on(chip, rrecv_e, rs_recv_e, rrecv_m, rs_recv_m, dev_m)

        own_send(mir(1))
        rd_wait(z)
        for k in range(NRS):
            rs_copy(z, k, rrecv_e, rs_recv_e, dev_m).wait_recv()
        pown[z] = pown[z] + precv[z].astype(jnp.float32) + resid_ref[...].astype(jnp.float32) + rrecv_e[z].astype(jnp.float32)
        own_send(mir(0))
        for k in range(NRS):
            span = pl.ds(k * rsub, rsub)
            rs_copy(z, k, rrecv_m, rs_recv_m, dev_m).wait_recv()
            out_ref[span] = (pown[z, span] + rrecv_m[z, span].astype(jnp.float32)).astype(jnp.bfloat16)
        pass_on(mir(3), rrecv_m, rs_recv_m, rrecv_m, rs_recv_m, dev_e)

    for k in range(NSUB):
        for chip in range(4):
            ag_d2d(landed(chip, k), chip, k).wait_send()
        ag_copy(landed(z, k), z, k, ag_send_m, dev_m).wait_send()

        @pl.when(is_int)
        def _():
            ag_copy(landed(z, k), z, k, ag_send_e, dev_e).wait_send()
            ag_copy(landed(mir(3), k), mir(3), k, ag_send_m, dev_m).wait_send()
            ag_copy(landed(mir(1), k), mir(1), k, ag_send_e, dev_e).wait_send()
            ag_copy(landed(mir(0), k), mir(0), k, ag_send_e, dev_e).wait_send()

    for chip in range(4):
        for part in range(HALVES):
            rd_copy(chip, part).wait_send()

        @pl.when(chip != z)
        def _():
            for k in range(NRS):
                rs_copy(chip, k, rrecv_m, rs_recv_m, dev_m).wait_send()


def mlp_block(mlp_in, resid, w_gate_t, w_up_t, w_down):
    rows, width = mlp_in.shape
    ffn = w_gate_t.shape[0]
    padded = -(-ffn // TURN) * TURN
    bf16, f32 = jnp.bfloat16, jnp.float32
    vmem = pl.BlockSpec(memory_space=pltpu.VMEM)
    hbm = pl.BlockSpec(memory_space=pl.ANY)
    dma = pltpu.SemaphoreType.DMA
    flops = 3 * 2 * 8 * rows * width * ffn
    return pl.pallas_call(
        mlp_kernel,
        out_shape=jax.ShapeDtypeStruct((rows, width), bf16),
        in_specs=[vmem, vmem, hbm, hbm, hbm],
        out_specs=vmem,
        scratch_shapes=[
            pltpu.VMEM((4, 2, rows, width), bf16),
            pltpu.VMEM((padded, width), bf16),
            pltpu.VMEM((padded, width), bf16),
            pltpu.VMEM((width, padded), bf16),
            pltpu.VMEM((width, padded), bf16),
            pltpu.VMEM((ffn, width), bf16),
            pltpu.VMEM((2 * rows, padded), bf16),
            pltpu.VMEM((4, rows, width), f32),
            pltpu.VMEM((4, rows, width), bf16),
            pltpu.VMEM((4, rows, width), bf16),
            pltpu.VMEM((4, rows, width), bf16),
            pltpu.VMEM((4, rows, width), bf16),
            pltpu.VMEM((4, rows, width), bf16),
            dma((2, padded // TURN)),
            dma,
            dma((4, NSUB)), dma((4, NSUB)), dma((4, NSUB)), dma((4, NSUB)), dma((4, NSUB)),
            dma((4, HALVES)), dma((4, HALVES)),
            dma((4, NRS)), dma((4, NRS)), dma((4, NRS)),
        ],
        compiler_params=pltpu.CompilerParams(collective_id=0, has_side_effects=True, vmem_limit_bytes=60 * 1024 * 1024),
        cost_estimate=pl.CostEstimate(flops=flops, bytes_accessed=3 * 2 * ffn * width, transcendentals=8 * rows * ffn),
        name='mlp_exchange',
    )(mlp_in, resid, w_gate_t, w_up_t, w_down)


def solution(mesh):
    rows_spec = P(('dp', 'tp'), None)
    cache_spec = P(('dp', 'tp'), None, None)
    whole = P()
    in_specs = (rows_spec, cache_spec, cache_spec, P(('dp', 'tp')), whole, whole, whole, whole, whole, whole, whole, whole, P(None, 'tp'), P(None, 'tp'), P('tp', None))
    out_specs = (rows_spec, rows_spec, rows_spec)

    def device_step(hidden, cache_lat, cache_rope, seq_lens, attn_norm, w_query, w_kv_down, kv_norm, w_key_up, w_val_up, w_out, mlp_norm, w_gate, w_up, w_down):
        resid, mlp_in, lat_new, rope_new = attention_block(hidden, cache_lat, cache_rope, seq_lens, attn_norm, w_query, w_kv_down, kv_norm, w_key_up, w_val_up, w_out, mlp_norm)
        out_hidden = mlp_block(mlp_in, resid, w_gate.T, w_up.T, w_down)
        return out_hidden, lat_new, rope_new

    return jax.shard_map(device_step, mesh=mesh, in_specs=in_specs, out_specs=out_specs, check_vma=False)
```
